32 devices in a mesh: data: 32 (over z, y, x, core).
Axes of the slice: x: 2, y: 2, z: 4, core: 2. Of those that a mesh axis runs over, the one named last changes fastest.
Arguments:
- w_in: float32 [16, 512, 2048], replicated
- w_out: float32 [16, 2048, 512], replicated
- mom_in: float32 [16, 512, 2048], replicated
- mom_out: float32 [16, 2048, 512], replicated
- x_first: bfloat16 [2048, 512], P('data')
- y_first: bfloat16 [2048, 512], P('data')
- x_second: bfloat16 [2048, 512], P('data')
- y_second: bfloat16 [2048, 512], P('data')
Outputs:
- output 1: float32 [16, 512, 2048], replicated
- output 2: float32 [16, 2048, 512], replicated
- output 3: float32 [16, 512, 2048], replicated
- output 4: float32 [16, 2048, 512], replicated
- output 5: float32 [2048], P('data')
- output 6: float32 [2048, 512], P('data')
All inputs are finite; a program needn't handle non-finite values.
Results may differ from the reference program's by a relative error of at most 0.00803043.
Values are sent between devices in bfloat16 or wider.
A program may use at most 2.25 GiB of HBM per device.

```python
import jax
import jax.numpy as jnp
from jax import lax

MODEL_DIM = 512
HIDDEN_DIM = 2048
NUM_LAYERS = 16
TOK_DEV = 64
GROUP_SIZE = 32

LR_SCALE = 1.0
MOMENTUM = 0.9


def setup_inputs(seed: int = 0) -> dict:
    base_key = jax.random.key(seed)
    sub_keys = jax.random.split(base_key, 16)
    batch_rows = TOK_DEV * GROUP_SIZE
    shape_in = (NUM_LAYERS, MODEL_DIM, HIDDEN_DIM)
    shape_out = (NUM_LAYERS, HIDDEN_DIM, MODEL_DIM)
    w_in = jax.random.normal(sub_keys[0], shape_in, jnp.float32) * MODEL_DIM ** -0.5
    w_out = jax.random.normal(sub_keys[1], shape_out, jnp.float32) * (HIDDEN_DIM * NUM_LAYERS) ** -0.5
    mom_in = jax.random.normal(sub_keys[2], shape_in, jnp.float32) * (0.1 * NUM_LAYERS * MODEL_DIM ** -0.5)
    col_part = jax.random.normal(sub_keys[3], (NUM_LAYERS, 1, MODEL_DIM), jnp.float32)
    mom_out = (col_part + jax.random.normal(sub_keys[4], shape_out, jnp.float32)) / HIDDEN_DIM

    def draw_batch(key_list):
        x_mean = 0.7 * jax.random.normal(key_list[0], (1, MODEL_DIM), jnp.float32)
        x_vals = jax.random.normal(key_list[1], (batch_rows, MODEL_DIM), jnp.float32) + x_mean
        shared_off = jax.random.normal(key_list[2], (1, 1, MODEL_DIM), jnp.float32)
        dev_off = jax.random.normal(key_list[3], (GROUP_SIZE, 1, MODEL_DIM), jnp.float32)
        noise_part = 0.5 * jax.random.normal(key_list[4], (GROUP_SIZE, TOK_DEV, MODEL_DIM), jnp.float32)
        y_vals = (noise_part + shared_off + dev_off).reshape(batch_rows, MODEL_DIM)
        return x_vals.astype(jnp.bfloat16), y_vals.astype(jnp.bfloat16)

    x_first, y_first = draw_batch(sub_keys[5:10])
    x_second, y_second = draw_batch(sub_keys[10:15])
    return {"w_in": w_in, "w_out": w_out, "mom_in": mom_in, "mom_out": mom_out, "x_first": x_first, "y_first": y_first, "x_second": x_second, "y_second": y_second}


def forward_stack(w_in_bf, w_out_bf, h_start):
    def layer_step(h_cur, weights):
        w_in_l, w_out_l = weights
        h_bf = h_cur.astype(jnp.bfloat16)
        pre_act = jnp.dot(h_bf, w_in_l, preferred_element_type=jnp.float32)
        act_bf = jax.nn.gelu(pre_act).astype(jnp.bfloat16)
        h_next = h_cur + jnp.dot(act_bf, w_out_l, preferred_element_type=jnp.float32)
        return h_next, (h_bf, pre_act, act_bf)
    return lax.scan(layer_step, h_start, (w_in_bf, w_out_bf))


def device_grads(w_in_bf, w_out_bf, x_rows, y_rows):
    h_last, saved_acts = forward_stack(w_in_bf, w_out_bf, x_rows.astype(jnp.float32))
    inv_scale = 1.0 / (TOK_DEV * GROUP_SIZE * MODEL_DIM)
    err_last = (h_last - y_rows.astype(jnp.float32)) * inv_scale

    def back_step(err_row, layer_data):
        w_in_l, w_out_l, h_bf, pre_act, act_bf = layer_data
        err_bf = err_row.astype(jnp.bfloat16)
        grad_out = jnp.dot(act_bf.T, err_bf, preferred_element_type=jnp.float32)
        d_act = jnp.dot(err_bf, w_out_l.T, preferred_element_type=jnp.float32)
        gelu_back = jax.vjp(jax.nn.gelu, pre_act)[1]
        d_pre = gelu_back(d_act)[0].astype(jnp.bfloat16)
        grad_in = jnp.dot(h_bf.T, d_pre, preferred_element_type=jnp.float32)
        err_prev = err_row + jnp.dot(d_pre, w_in_l.T, preferred_element_type=jnp.float32)
        return err_prev, (grad_in.astype(jnp.bfloat16), grad_out.astype(jnp.bfloat16))

    err_first, grads = lax.scan(back_step, err_last, (w_in_bf, w_out_bf, saved_acts[0], saved_acts[1], saved_acts[2]), reverse=True)
    return grads


def reference(w_in, w_out, mom_in, mom_out, x_first, y_first, x_second, y_second):
    w_in_bf = w_in.astype(jnp.bfloat16)
    w_out_bf = w_out.astype(jnp.bfloat16)
    x_blocks = x_first.reshape(GROUP_SIZE, TOK_DEV, MODEL_DIM)
    y_blocks = y_first.reshape(GROUP_SIZE, TOK_DEV, MODEL_DIM)

    def add_device(grad_sums, block_pair):
        grad_in, grad_out = device_grads(w_in_bf, w_out_bf, block_pair[0], block_pair[1])
        return (grad_sums[0] + grad_in.astype(jnp.float32), grad_sums[1] + grad_out.astype(jnp.float32)), None

    zero_sums = (jnp.zeros(w_in.shape, jnp.float32), jnp.zeros(w_out.shape, jnp.float32))
    grad_sums, unused = lax.scan(add_device, zero_sums, (x_blocks, y_blocks))
    step_size = LR_SCALE / NUM_LAYERS
    mom_in_new = MOMENTUM * mom_in + grad_sums[0]
    mom_out_new = MOMENTUM * mom_out + grad_sums[1]
    w_in_new = w_in - step_size * mom_in_new
    w_out_new = w_out - step_size * mom_out_new
    new_in_bf = w_in_new.astype(jnp.bfloat16)
    new_out_bf = w_out_new.astype(jnp.bfloat16)

    def next_forward(x_rows):
        h_last, saved_acts = forward_stack(new_in_bf, new_out_bf, x_rows.astype(jnp.float32))
        return h_last

    h_blocks = lax.map(next_forward, x_second.reshape(GROUP_SIZE, TOK_DEV, MODEL_DIM))
    h_final = h_blocks.reshape(GROUP_SIZE * TOK_DEV, MODEL_DIM)
    row_diff = h_final - y_second.astype(jnp.float32)
    loss_rows = jnp.sum(row_diff * row_diff, axis=-1) / (2 * MODEL_DIM)
    return (w_in_new, w_out_new, mom_in_new, mom_out_new, loss_rows, h_final)
```

```python
import functools

import jax
import jax.numpy as jnp
from jax import lax
from jax.experimental import pallas as pl
from jax.experimental.pallas import tpu as pltpu
from jax.sharding import PartitionSpec as P

LR_SCALE = 1.0
MOMENTUM = 0.9
F32 = jnp.float32
BF16 = jnp.bfloat16
MESH = pl.DeviceIdType.MESH
GELU_C = 0.7978845608028654
GELU_K = 0.044715
SLOTS = 4
PIECES = 4
VMEM_LIMIT = 62 * 1024 * 1024

NN = (((1,), (0,)), ((), ()))
NT = (((1,), (1,)), ((), ()))
TN = (((0,), (0,)), ((), ()))


def mm(a, b, dims=NN):
    return lax.dot_general(a, b, dims, preferred_element_type=F32)


def gelu(z):
    t = jnp.tanh(GELU_C * (z + GELU_K * (z * z * z)))
    return z * (0.5 * (1.0 + t))


def gelu_grad(z):
    zz = z * z
    t = jnp.tanh(GELU_C * (z + GELU_K * (zz * z)))
    cdf = 0.5 * (1.0 + t)
    slope = cdf + (0.5 * z) * (1.0 - t * t) * (GELU_C * (1.0 + (3.0 * GELU_K) * zz))
    return z * cdf, slope


def grads_kernel(dims, w1_hbm, w2_hbm, x_ref, y_ref, *rest):
    n_dev, layers, rows, d, hid = dims
    chips = n_dev // 2
    hc = hid // 2
    piece = hc // PIECES
    g_refs = rest[:PIECES]
    (wb1, wb2, z_all, hb, eb, hcur, rh, re, ow1, ow2, zq, aa, ss, acc1, acc2,
     w1_sem, w2_sem, hs_sem, hr_sem, es_sem, er_sem, px_send, px_recv) = rest[PIECES:]

    me = lax.axis_index("data")
    chip = me // 2
    core = me % 2
    partner = chip * 2 + (1 - core)

    def greet(c, carry):
        @pl.when(c != chip)
        def _():
            pl.semaphore_signal(barrier, inc=1, device_id=(2 * c + core,), device_id_type=MESH)
        return carry

    barrier = pltpu.get_barrier_semaphore()
    lax.fori_loop(0, chips, greet, 0)
    pl.semaphore_signal(barrier, inc=1, device_id=(partner,), device_id_type=MESH)

    def w1_copy(l, j, slot):
        return pltpu.make_async_copy(w1_hbm.at[l, :, pl.ds(pl.multiple_of(j * hc, 128), hc)], wb1.at[slot], w1_sem.at[slot])

    def w2_copy(l, j, slot):
        return pltpu.make_async_copy(w2_hbm.at[l, pl.ds(pl.multiple_of(j * hc, 128), hc), :], wb2.at[slot], w2_sem.at[slot])

    def fetch(l, j, slot):
        w1_copy(l, j, slot).start()
        w2_copy(l, j, slot).start()

    def arrived(l, j, slot):
        w1_copy(l, j, slot).wait()
        w2_copy(l, j, slot).wait()

    for i in range(SLOTS):
        fetch(i // 2, i % 2, i)
    pl.semaphore_wait(barrier, chips)

    def h_copy(l):
        return pltpu.make_async_remote_copy(
            src_ref=hb.at[l], dst_ref=rh.at[core * chips + chip], send_sem=hs_sem.at[l], recv_sem=hr_sem.at[chip],
            device_id=(2 * l + core,), device_id_type=MESH)

    def e_copy(l):
        return pltpu.make_async_remote_copy(
            src_ref=eb.at[l], dst_ref=re.at[core * chips + chip], send_sem=es_sem.at[l], recv_sem=er_sem.at[chip],
            device_id=(2 * l + core,), device_id_type=MESH)

    def h_arrival(c):
        return pltpu.make_async_remote_copy(
            src_ref=hb.at[0], dst_ref=rh.at[core * chips + c], send_sem=hs_sem.at[0], recv_sem=hr_sem.at[c],
            device_id=(me,), device_id_type=MESH)

    def e_arrival(c):
        return pltpu.make_async_remote_copy(
            src_ref=eb.at[0], dst_ref=re.at[core * chips + c], send_sem=es_sem.at[0], recv_sem=er_sem.at[c],
            device_id=(me,), device_id_type=MESH)

    def send_h(l):
        @pl.when(l != chip)
        def _():
            h_copy(l).start()

        @pl.when(l == chip)
        def _():
            rh[core * chips + chip] = hb[l]

    def send_e(l):
        @pl.when(l != chip)
        def _():
            e_copy(l).start()

        @pl.when(l == chip)
        def _():
            re[core * chips + chip] = eb[l]

    n_fwd = 2 * layers
    n_bwd = 2 * (layers - 1)
    hcur[...] = x_ref[...].astype(F32)

    def forward(i, carry):
        l, j, slot = i // 2, i % 2, i % SLOTS
        arrived(l, j, slot)

        @pl.when(j == 0)
        def _():
            hb[l] = hcur[...].astype(BF16)

        z = mm(hb[l], wb1[slot].astype(BF16))
        z_all[i] = z
        hcur[...] += mm(gelu(z).astype(BF16), wb2[slot].astype(BF16))

        nxt = i + SLOTS

        @pl.when(nxt < n_fwd)
        def _():
            fetch(nxt // 2, nxt % 2, slot)

        @pl.when(nxt >= n_fwd)
        def _():
            fetch(layers - 1 - (nxt - n_fwd) // 2, nxt % 2, slot)

        @pl.when(j == 1)
        def _():
            send_h(l)
        return carry

    lax.fori_loop(0, n_fwd, forward, 0)

    scale = 1.0 / (rows * n_dev * d)
    hcur[...] = (hcur[...] - y_ref[...].astype(F32)) * scale

    h_swap = pltpu.make_async_remote_copy(
        src_ref=rh.at[pl.ds(core * chips, chips)], dst_ref=rh.at[pl.ds(core * chips, chips)],
        send_sem=px_send.at[0], recv_sem=px_recv.at[0], device_id=(partner,), device_id_type=MESH)
    e_swap = pltpu.make_async_remote_copy(
        src_ref=re.at[pl.ds(core * chips, chips)], dst_ref=re.at[pl.ds(core * chips, chips)],
        send_sem=px_send.at[1], recv_sem=px_recv.at[1], device_id=(partner,), device_id_type=MESH)

    def backward(i, carry):
        l, j, slot = layers - 1 - i // 2, i % 2, i % SLOTS
        arrived(l, j, slot)

        @pl.when(j == 0)
        def _():
            eb[l] = hcur[...].astype(BF16)

        q = mm(eb[l], wb2[slot].astype(BF16), NT)
        slope = gelu_grad(z_all[2 * l + j])[1]
        hcur[...] += mm((slope * q).astype(BF16), wb1[slot].astype(BF16), NT)

        nxt = i + SLOTS

        @pl.when(nxt < n_bwd)
        def _():
            fetch(layers - 1 - nxt // 2, nxt % 2, slot)

        @pl.when(nxt == n_bwd)
        def _():
            fetch(chip, core, slot)

        @pl.when(j == 1)
        def _():
            send_e(l)
        return carry

    lax.fori_loop(0, n_bwd, backward, 0)
    eb[0] = hcur[...].astype(BF16)

    own_slot = n_bwd % SLOTS
    arrived(chip, core, own_slot)
    ow1[...] = wb1[own_slot].astype(BF16)
    ow2[...] = wb2[own_slot].astype(BF16)
    acc1[...] = jnp.zeros_like(acc1)
    acc2[...] = jnp.zeros_like(acc2)
    send_e(0)

    def h_in(c, carry):
        @pl.when(c != chip)
        def _():
            h_arrival(c).wait_recv()
        return carry

    def e_in(c, carry):
        @pl.when(c != chip)
        def _():
            e_arrival(c).wait_recv()
        return carry

    lax.fori_loop(0, chips, h_in, 0)
    h_swap.start()
    lax.fori_loop(0, chips, e_in, 0)
    e_swap.start()

    group = 4
    half_groups = chips // group
    nb = hc // piece

    def owner(gi, carry):
        half = (core + gi // half_groups) % 2

        @pl.when(gi == half_groups)
        def _():
            h_swap.wait_recv()
            e_swap.wait_recv()

        base = half * chips + (gi % half_groups) * group
        hg = rh[pl.ds(base, group)].reshape(group * rows, d)
        eg = re[pl.ds(base, group)].reshape(group * rows, d)
        for n in range(nb):
            cols = slice(n * piece, (n + 1) * piece)
            z = mm(hg, ow1[:, cols])
            q = mm(eg, ow2[cols, :], NT)
            a, slope = gelu_grad(z)
            aa[n] = a.astype(BF16).reshape(group, rows, piece)
            ss[n] = (slope * q).astype(BF16).reshape(group, rows, piece)

        def products(n, c2):
            for b in range(group):
                h_b = rh[base + b]
                e_b = re[base + b]
                acc1[n] += mm(h_b, ss[n, b], TN).astype(BF16).astype(F32)
                acc2[n] += mm(aa[n, b], e_b, TN).astype(BF16).astype(F32)
            return c2

        lax.fori_loop(0, nb, products, 0)
        return carry

    lax.fori_loop(0, 2 * half_groups, owner, 0)

    for n in range(PIECES):
        for cb in range(piece // 128):
            g_refs[n][cb * d:(cb + 1) * d, :] = acc1[n, :, cb * 128:(cb + 1) * 128].astype(BF16)
        off = (piece // 128) * d
        for lb in range(d // 128):
            g_refs[n][off + lb * piece:off + (lb + 1) * piece, :] = acc2[n, :, lb * 128:(lb + 1) * 128].astype(BF16)

    def sent(l, carry):
        @pl.when(l != chip)
        def _():
            h_copy(l).wait_send()
            e_copy(l).wait_send()
        return carry

    lax.fori_loop(0, layers, sent, 0)
    h_swap.wait_send()
    e_swap.wait_send()


def local_grads(w_in, w_out, x, y, n_dev):
    layers, d, hid = w_in.shape
    rows = x.shape[0]
    hc = hid // 2
    piece = hc // PIECES
    g_rows = (piece // 128) * d + (d // 128) * piece
    dims = (n_dev, layers, rows, d, hid)
    flops = 2 * rows * d * hid * layers * 4 + 2 * rows * n_dev * d * hc * 4
    return pl.pallas_call(
        functools.partial(grads_kernel, dims),
        out_shape=[jax.ShapeDtypeStruct((g_rows, 128), BF16)] * PIECES,
        in_specs=[pl.BlockSpec(memory_space=pl.ANY)] * 2 + [pl.BlockSpec(memory_space=pltpu.VMEM)] * 2,
        out_specs=[pl.BlockSpec(memory_space=pltpu.VMEM)] * PIECES,
        scratch_shapes=[
            pltpu.VMEM((SLOTS, d, hc), F32),
            pltpu.VMEM((SLOTS, hc, d), F32),
            pltpu.VMEM((2 * layers, rows, hc), F32),
            pltpu.VMEM((layers, rows, d), BF16),
            pltpu.VMEM((layers, rows, d), BF16),
            pltpu.VMEM((rows, d), F32),
            pltpu.VMEM((n_dev, rows, d), BF16),
            pltpu.VMEM((n_dev, rows, d), BF16),
            pltpu.VMEM((d, hc), BF16),
            pltpu.VMEM((hc, d), BF16),
            pltpu.VMEM((8, 128), F32),
            pltpu.VMEM((PIECES, 4, rows, piece), BF16),
            pltpu.VMEM((PIECES, 4, rows, piece), BF16),
            pltpu.VMEM((PIECES, d, piece), F32),
            pltpu.VMEM((PIECES, piece, d), F32),
            pltpu.SemaphoreType.DMA((SLOTS,)),
            pltpu.SemaphoreType.DMA((SLOTS,)),
            pltpu.SemaphoreType.DMA((layers,)),
            pltpu.SemaphoreType.DMA((layers,)),
            pltpu.SemaphoreType.DMA((layers,)),
            pltpu.SemaphoreType.DMA((layers,)),
            pltpu.SemaphoreType.DMA((2,)),
            pltpu.SemaphoreType.DMA((2,)),
        ],
        compiler_params=pltpu.CompilerParams(collective_id=0, has_side_effects=True, vmem_limit_bytes=VMEM_LIMIT),
        cost_estimate=pl.CostEstimate(flops=flops, bytes_accessed=4 * w_in.size * 4, transcendentals=0),
        name="local_grads",
    )(w_in, w_out, x, y)


def update_kernel(first, last, dims, *refs):
    layers, rows, d, hid, piece = dims
    step_size = LR_SCALE / layers
    w1, m1, w2, m2, g = refs[:5]
    refs = refs[5:]
    if not first:
        refs = refs[4:]
    if last:
        side = refs[:2 * (PIECES - 1)]
        x_ref, y_ref = refs[2 * (PIECES - 1):2 * PIECES]
        w1o, w2o, m1o, m2o, loss_ref, h_out, nb1, nb2, h_ref, hb_ref = refs[2 * PIECES:]
    else:
        w1o, w2o, m1o, m2o, nb1, nb2 = refs
    lead = () if last else (0,)

    for cb in range(piece // 128):
        cols = slice(cb * 128, (cb + 1) * 128)
        mn = MOMENTUM * m1[0, :, cols] + g[0, cb * d:(cb + 1) * d, :].astype(F32)
        wn = w1[0, :, cols] - step_size * mn
        m1o[0, :, cols] = mn
        w1o[0, :, cols] = wn
        nb1[(*lead, slice(None), cols)] = wn.astype(BF16)
    off = (piece // 128) * d
    for lb in range(d // 128):
        cols = slice(lb * 128, (lb + 1) * 128)
        mn = MOMENTUM * m2[0, :, cols] + g[0, off + lb * piece:off + (lb + 1) * piece, :].astype(F32)
        wn = w2[0, :, cols] - step_size * mn
        m2o[0, :, cols] = mn
        w2o[0, :, cols] = wn
        nb2[(*lead, slice(None), cols)] = wn.astype(BF16)
    if not last:
        return

    l, c = pl.program_id(0), pl.program_id(1)

    @pl.when(jnp.logical_and(l == 0, c == 0))
    def _():
        h_ref[...] = x_ref[...].astype(F32)

    @pl.when(c == 0)
    def _():
        hb_ref[...] = h_ref[...].astype(BF16)

    total = h_ref[...]
    for p in range(PIECES):
        a1 = side[2 * p][0] if p < PIECES - 1 else nb1[...]
        a2 = side[2 * p + 1][0] if p < PIECES - 1 else nb2[...]
        z = mm(hb_ref[...], a1)
        total += mm(gelu(z).astype(BF16), a2)
    h_ref[...] = total

    @pl.when(jnp.logical_and(l == layers - 1, c == 1))
    def _():
        h_out[...] = h_ref[...]
        diff = h_ref[...] - y_ref[...].astype(F32)
        loss_ref[...] = jnp.sum(diff * diff, axis=-1, keepdims=True) / (2 * d)


def update(p, w_in, m_in, w_out, m_out, g_all, prev, side, x, y):
    layers, d, hid = w_in.shape
    rows = x.shape[0]
    piece = hid // 2 // PIECES
    first, last = p == 0, p == PIECES - 1
    in_spec = pl.BlockSpec((1, d, piece), lambda l, c: (l, 0, c * PIECES + p))
    out_spec = pl.BlockSpec((1, piece, d), lambda l, c: (l, c * PIECES + p, 0))
    g_spec = pl.BlockSpec((1, g_all.shape[1], 128), lambda l, c: (2 * l + c, 0, 0))
    any_spec = pl.BlockSpec(memory_space=pl.ANY)
    s1_spec = pl.BlockSpec((1, d, piece), lambda l, c: (2 * l + c, 0, 0))
    s2_spec = pl.BlockSpec((1, piece, d), lambda l, c: (2 * l + c, 0, 0))
    whole = pl.BlockSpec((rows, d), lambda l, c: (0, 0))
    in_specs = [in_spec, in_spec, out_spec, out_spec, g_spec]
    args = [w_in, m_in, w_out, m_out, g_all]
    out_specs = [in_spec, out_spec, in_spec, out_spec]
    out_shape = [jax.ShapeDtypeStruct(a.shape, F32) for a in (w_in, w_out, m_in, m_out)]
    aliases = {}
    scratch = []
    if not first:
        aliases = {5 + i: i for i in range(4)}
        in_specs += [any_spec] * 4
        args += prev
    if last:
        in_specs += [s1_spec, s2_spec] * (PIECES - 1) + [whole, whole]
        args += side + [x, y]
        out_specs += [pl.BlockSpec((rows, 1), lambda l, c: (0, 0)), whole]
        out_shape += [jax.ShapeDtypeStruct((rows, 1), F32), jax.ShapeDtypeStruct((rows, d), F32)]
        scratch = [pltpu.VMEM((d, piece), BF16), pltpu.VMEM((piece, d), BF16), pltpu.VMEM((rows, d), F32), pltpu.VMEM((rows, d), BF16)]
    else:
        out_specs += [s1_spec, s2_spec]
        out_shape += [jax.ShapeDtypeStruct((2 * layers, d, piece), BF16), jax.ShapeDtypeStruct((2 * layers, piece, d), BF16)]
    n_el = 2 * w_in.size // PIECES
    return pl.pallas_call(
        functools.partial(update_kernel, first, last, (layers, rows, d, hid, piece)),
        grid=(layers, 2),
        in_specs=in_specs,
        out_specs=out_specs,
        out_shape=out_shape,
        scratch_shapes=scratch,
        input_output_aliases=aliases,
        compiler_params=pltpu.CompilerParams(dimension_semantics=("arbitrary", "arbitrary"), vmem_limit_bytes=VMEM_LIMIT),
        cost_estimate=pl.CostEstimate(flops=400 * n_el, bytes_accessed=20 * n_el, transcendentals=0),
        name=f"update_{p}",
    )(*args)


def solution(mesh):
    n_dev = mesh.shape["data"]
    rows_spec = P("data", None)

    def local_steps(w_in, w_out, mom_in, mom_out, x_first, y_first, x_second, y_second):
        pieces = local_grads(w_in, w_out, x_first, y_first, n_dev)
        gathered = [lax.all_gather(g, "data", axis=0) for g in pieces]
        prev, side = [], []
        for p in range(PIECES):
            outs = update(p, w_in, mom_in, w_out, mom_out, gathered[p], prev, side, x_second, y_second)
            prev = list(outs[:4])
            side = side + list(outs[4:])
        loss, h_final = outs[4:]
        w_in_new, w_out_new, mom_in_new, mom_out_new = prev
        return w_in_new, w_out_new, mom_in_new, mom_out_new, loss.reshape(-1), h_final

    return jax.shard_map(
        local_steps, mesh=mesh,
        in_specs=(P(), P(), P(), P(), rows_spec, rows_spec, rows_spec, rows_spec),
        out_specs=(P(), P(), P(), P(), P("data"), rows_spec), check_vma=False)
```

```python
import functools

import jax
import jax.numpy as jnp
from jax import lax
from jax.experimental import pallas as pl
from jax.experimental.pallas import tpu as pltpu
from jax.sharding import PartitionSpec as P

LR_SCALE = 1.0
MOMENTUM = 0.9
F32 = jnp.float32
BF16 = jnp.bfloat16
MESH = pl.DeviceIdType.MESH
GELU_C = 0.7978845608028654
GELU_K = 0.044715
SLOTS = 4
QUARTERS = 4
ROUTES = ((0, 2, 1), (1, 2, 0), (2, 0, 1), (2, 1, 0))
VMEM_LIMIT = 62 * 1024 * 1024

NN = (((1,), (0,)), ((), ()))
NT = (((1,), (1,)), ((), ()))
TN = (((0,), (0,)), ((), ()))


def mm(a, b, dims=NN):
    return lax.dot_general(a, b, dims, preferred_element_type=F32)


def gelu(z):
    t = jnp.tanh(GELU_C * (z + GELU_K * (z * z * z)))
    return z * (0.5 * (1.0 + t))


def gelu_grad(z):
    zz = z * z
    t = jnp.tanh(GELU_C * (z + GELU_K * (zz * z)))
    cdf = 0.5 * (1.0 + t)
    slope = cdf + (0.5 * z) * (1.0 - t * t) * (GELU_C * (1.0 + (3.0 * GELU_K) * zz))
    return z * cdf, slope


def grads_kernel(dims, w1_hbm, w2_hbm, x_ref, y_ref, *rest):
    n_dev, layers, rows, d, hid = dims
    chips = n_dev // 2
    hc = hid // 2
    piece = hc // QUARTERS
    (g_all, wb1, wb2, z_all, hb, eb, hcur, rh, re, ow1, ow2, aa, ss, acc1, acc2, own,
     w1_sem, w2_sem, hs_sem, hr_sem, es_sem, er_sem, px_send, px_recv,
     sp_send, sp_recv, tw_send, tw_recv, own_sem) = rest

    me = lax.axis_index("data")
    chip = me // 2
    core = me % 2
    partner = chip * 2 + (1 - core)

    cx, cy, cz = chip % 2, (chip // 2) % 2, chip // 4

    def greet(c, carry):
        @pl.when(c != chip)
        def _():
            pl.semaphore_signal(barrier, inc=1, device_id=(2 * c + core,), device_id_type=MESH)
        return carry

    barrier = pltpu.get_barrier_semaphore()
    lax.fori_loop(0, chips, greet, 0)
    pl.semaphore_signal(barrier, inc=1, device_id=(partner,), device_id_type=MESH)

    def w1_copy(l, j, slot):
        return pltpu.make_async_copy(w1_hbm.at[l, :, pl.ds(pl.multiple_of(j * hc, 128), hc)], wb1.at[slot], w1_sem.at[slot])

    def w2_copy(l, j, slot):
        return pltpu.make_async_copy(w2_hbm.at[l, pl.ds(pl.multiple_of(j * hc, 128), hc), :], wb2.at[slot], w2_sem.at[slot])

    def fetch(l, j, slot):
        w1_copy(l, j, slot).start()
        w2_copy(l, j, slot).start()

    def arrived(l, j, slot):
        w1_copy(l, j, slot).wait()
        w2_copy(l, j, slot).wait()

    for i in range(SLOTS):
        fetch(i // 2, i % 2, i)
    pl.semaphore_wait(barrier, chips)

    def h_copy(l):
        return pltpu.make_async_remote_copy(
            src_ref=hb.at[l], dst_ref=rh.at[core * chips + chip], send_sem=hs_sem.at[l], recv_sem=hr_sem.at[chip],
            device_id=(2 * l + core,), device_id_type=MESH)

    def e_copy(l):
        return pltpu.make_async_remote_copy(
            src_ref=eb.at[l], dst_ref=re.at[core * chips + chip], send_sem=es_sem.at[l], recv_sem=er_sem.at[chip],
            device_id=(2 * l + core,), device_id_type=MESH)

    def h_arrival(c):
        return pltpu.make_async_remote_copy(
            src_ref=hb.at[0], dst_ref=rh.at[core * chips + c], send_sem=hs_sem.at[0], recv_sem=hr_sem.at[c],
            device_id=(me,), device_id_type=MESH)

    def e_arrival(c):
        return pltpu.make_async_remote_copy(
            src_ref=eb.at[0], dst_ref=re.at[core * chips + c], send_sem=es_sem.at[0], recv_sem=er_sem.at[c],
            device_id=(me,), device_id_type=MESH)

    def send_h(l):
        @pl.when(l != chip)
        def _():
            h_copy(l).start()

        @pl.when(l == chip)
        def _():
            rh[core * chips + chip] = hb[l]

    def send_e(l):
        @pl.when(l != chip)
        def _():
            e_copy(l).start()

        @pl.when(l == chip)
        def _():
            re[core * chips + chip] = eb[l]

    n_fwd = 2 * layers
    n_bwd = 2 * (layers - 1)
    hcur[...] = x_ref[...].astype(F32)

    def forward(i, carry):
        l, j, slot = i // 2, i % 2, i % SLOTS
        arrived(l, j, slot)

        @pl.when(j == 0)
        def _():
            hb[l] = hcur[...].astype(BF16)

        z = mm(hb[l], wb1[slot].astype(BF16))
        z_all[i] = z
        hcur[...] += mm(gelu(z).astype(BF16), wb2[slot].astype(BF16))

        nxt = i + SLOTS

        @pl.when(nxt < n_fwd)
        def _():
            fetch(nxt // 2, nxt % 2, slot)

        @pl.when(nxt >= n_fwd)
        def _():
            fetch(layers - 1 - (nxt - n_fwd) // 2, nxt % 2, slot)

        @pl.when(j == 1)
        def _():
            send_h(l)
        return carry

    lax.fori_loop(0, n_fwd, forward, 0)

    scale = 1.0 / (rows * n_dev * d)
    hcur[...] = (hcur[...] - y_ref[...].astype(F32)) * scale

    h_swap = pltpu.make_async_remote_copy(
        src_ref=rh.at[pl.ds(core * chips, chips)], dst_ref=rh.at[pl.ds(core * chips, chips)],
        send_sem=px_send.at[0], recv_sem=px_recv.at[0], device_id=(partner,), device_id_type=MESH)
    e_swap = pltpu.make_async_remote_copy(
        src_ref=re.at[pl.ds(core * chips, chips)], dst_ref=re.at[pl.ds(core * chips, chips)],
        send_sem=px_send.at[1], recv_sem=px_recv.at[1], device_id=(partner,), device_id_type=MESH)

    def backward(i, carry):
        l, j, slot = layers - 1 - i // 2, i % 2, i % SLOTS
        arrived(l, j, slot)

        @pl.when(j == 0)
        def _():
            eb[l] = hcur[...].astype(BF16)

        q = mm(eb[l], wb2[slot].astype(BF16), NT)
        slope = gelu_grad(z_all[2 * l + j])[1]
        hcur[...] += mm((slope * q).astype(BF16), wb1[slot].astype(BF16), NT)

        nxt = i + SLOTS

        @pl.when(nxt < n_bwd)
        def _():
            fetch(layers - 1 - nxt // 2, nxt % 2, slot)

        @pl.when(nxt == n_bwd)
        def _():
            fetch(chip, core, slot)

        @pl.when(j == 1)
        def _():
            send_e(l)
        return carry

    lax.fori_loop(0, n_bwd, backward, 0)
    eb[0] = hcur[...].astype(BF16)

    own_slot = n_bwd % SLOTS
    arrived(chip, core, own_slot)
    ow1[...] = wb1[own_slot].astype(BF16)
    ow2[...] = wb2[own_slot].astype(BF16)
    acc1[...] = jnp.zeros_like(acc1)
    acc2[...] = jnp.zeros_like(acc2)
    send_e(0)

    def h_in(c, carry):
        @pl.when(c != chip)
        def _():
            h_arrival(c).wait_recv()
        return carry

    def e_in(c, carry):
        @pl.when(c != chip)
        def _():
            e_arrival(c).wait_recv()
        return carry

    lax.fori_loop(0, chips, h_in, 0)
    h_swap.start()
    lax.fori_loop(0, chips, e_in, 0)
    e_swap.start()

    group = 4
    half_groups = chips // group

    def owner(gi, carry):
        half = (core + gi // half_groups) % 2

        @pl.when(gi == half_groups)
        def _():
            h_swap.wait_recv()
            e_swap.wait_recv()

        base = half * chips + (gi % half_groups) * group
        hg = rh[pl.ds(base, group)].reshape(group * rows, d)
        eg = re[pl.ds(base, group)].reshape(group * rows, d)
        for n in range(QUARTERS):
            cols = slice(n * piece, (n + 1) * piece)
            z = mm(hg, ow1[:, cols])
            q = mm(eg, ow2[cols, :], NT)
            a, slope = gelu_grad(z)
            aa[n, pl.ds(base, group)] = a.astype(BF16).reshape(group, rows, piece)
            ss[n, pl.ds(base, group)] = (slope * q).astype(BF16).reshape(group, rows, piece)
        return carry

    lax.fori_loop(0, 2 * half_groups, owner, 0)

    def place(src, n):
        return g_all.at[2 * src + core, n]

    hops = {"x": chip + 1 - 2 * cx, "y": chip + 2 - 4 * cy, "up": chip + 4, "down": chip - 4}
    exists = {"x": None, "y": None, "up": cz < 3, "down": cz > 0}
    kinds = ("x", "y", "up", "down")

    def sends(n, rel):
        order = ROUTES[n]
        last = max([i for i in range(3) if rel[order[i]]], default=-1)
        out = []
        if last >= 0 and order[last] == 2:
            out.append("down" if rel[2] > 0 else "up")
        for i in range(last + 1, 3):
            out += {0: ["x"], 1: ["y"], 2: ["up", "down"]}[order[i]]
        return out

    def source(rel):
        sx = 1 - cx if rel[0] else cx
        sy = 1 - cy if rel[1] else cy
        return (cz + rel[2]) * 4 + sy * 2 + sx

    def hop_copy(n, rel, kind):
        src = source(rel)
        block = place(src, n) if any(rel) else own.at[n]
        return pltpu.make_async_remote_copy(
            src_ref=block, dst_ref=place(src, n), send_sem=sp_send.at[n, kinds.index(kind), src],
            recv_sem=sp_recv.at[n, src], device_id=(2 * hops[kind] + core,), device_id_type=MESH)

    def twin_copy(n, rel):
        src = source(rel)
        block = place(src, n) if any(rel) else own.at[n]
        return pltpu.make_async_remote_copy(
            src_ref=block, dst_ref=place(src, n), send_sem=tw_send.at[n, src], recv_sem=tw_recv.at[n, src],
            device_id=(partner,), device_id_type=MESH)

    def guarded(cond, fn):
        if cond is None:
            fn()
        else:
            pl.when(cond)(fn)

    def valid(rel):
        if rel[2] > 0:
            return cz <= 3 - rel[2]
        return cz >= -rel[2] if rel[2] < 0 else None

    def forward_block(n, rel):
        def act():
            if any(rel):
                hop_copy(n, rel, "x").wait_recv()
            for kind in sends(n, rel):
                guarded(exists[kind], hop_copy(n, rel, kind).start)
            twin_copy(n, rel).start()
        guarded(valid(rel), act)

    def drain_block(n, rel):
        def act():
            for kind in sends(n, rel):
                guarded(exists[kind], hop_copy(n, rel, kind).wait_send)
            twin_copy(n, rel).wait_send()
        guarded(valid(rel), act)

    rels = [(rx, ry, dz) for rx in (0, 1) for ry in (0, 1) for dz in (-3, -2, -1, 0, 1, 2, 3)]
    steps = sorted(((n, rel) for n in range(QUARTERS) for rel in rels),
                   key=lambda t: (t[1][0] + t[1][1] + abs(t[1][2]), t[0]))
    steps = [t for t in steps if any(t[1])]
    here = (0, 0, 0)

    for n in range(QUARTERS):
        acc1[...] = jnp.zeros_like(acc1)
        acc2[...] = jnp.zeros_like(acc2)

        def products(gi, carry):
            for b in range(group):
                k = gi * group + b
                acc1[...] += mm(rh[k], ss[n, k], TN).astype(BF16).astype(F32)
                acc2[...] += mm(aa[n, k], re[k], TN).astype(BF16).astype(F32)
            return carry

        lax.fori_loop(0, 2 * half_groups, products, 0)
        for cb in range(piece // 128):
            own[n, cb * d:(cb + 1) * d, :] = acc1[:, cb * 128:(cb + 1) * 128].astype(BF16)
        off = (piece // 128) * d
        for lb in range(d // 128):
            own[n, off + lb * piece:off + (lb + 1) * piece, :] = acc2[:, lb * 128:(lb + 1) * 128].astype(BF16)
        pltpu.make_async_copy(own.at[n], g_all.at[me, n], own_sem.at[n]).start()
        forward_block(n, here)

    for n, rel in steps:
        forward_block(n, rel)

    def sent(l, carry):
        @pl.when(l != chip)
        def _():
            h_copy(l).wait_send()
            e_copy(l).wait_send()
        return carry

    lax.fori_loop(0, layers, sent, 0)
    h_swap.wait_send()
    e_swap.wait_send()
    for n in range(QUARTERS):
        pltpu.make_async_copy(own.at[n], g_all.at[me, n], own_sem.at[n]).wait()
        drain_block(n, here)
    for n, rel in steps:
        drain_block(n, rel)

    def twin_in(i, carry):
        n, src = i // chips, i % chips
        pltpu.make_async_remote_copy(
            src_ref=place(src, n), dst_ref=g_all.at[2 * src + 1 - core, n], send_sem=tw_send.at[n, src],
            recv_sem=tw_recv.at[n, src], device_id=(me,), device_id_type=MESH).wait_recv()
        return carry

    lax.fori_loop(0, QUARTERS * chips, twin_in, 0)


def local_grads(w_in, w_out, x, y, n_dev):
    layers, d, hid = w_in.shape
    rows = x.shape[0]
    hc = hid // 2
    piece = hc // QUARTERS
    g_rows = (piece // 128) * d + (d // 128) * piece
    dims = (n_dev, layers, rows, d, hid)
    flops = 2 * rows * d * hid * layers * 4 + 2 * rows * n_dev * d * hc * 4
    return pl.pallas_call(
        functools.partial(grads_kernel, dims),
        out_shape=jax.ShapeDtypeStruct((n_dev, QUARTERS, g_rows, 128), BF16),
        in_specs=[pl.BlockSpec(memory_space=pl.ANY)] * 2 + [pl.BlockSpec(memory_space=pltpu.VMEM)] * 2,
        out_specs=pl.BlockSpec(memory_space=pl.ANY),
        scratch_shapes=[
            pltpu.VMEM((SLOTS, d, hc), F32),
            pltpu.VMEM((SLOTS, hc, d), F32),
            pltpu.VMEM((2 * layers, rows, hc), F32),
            pltpu.VMEM((layers, rows, d), BF16),
            pltpu.VMEM((layers, rows, d), BF16),
            pltpu.VMEM((rows, d), F32),
            pltpu.VMEM((n_dev, rows, d), BF16),
            pltpu.VMEM((n_dev, rows, d), BF16),
            pltpu.VMEM((d, hc), BF16),
            pltpu.VMEM((hc, d), BF16),
            pltpu.VMEM((QUARTERS, n_dev, rows, piece), BF16),
            pltpu.VMEM((QUARTERS, n_dev, rows, piece), BF16),
            pltpu.VMEM((d, piece), F32),
            pltpu.VMEM((piece, d), F32),
            pltpu.VMEM((QUARTERS, g_rows, 128), BF16),
            pltpu.SemaphoreType.DMA((SLOTS,)),
            pltpu.SemaphoreType.DMA((SLOTS,)),
            pltpu.SemaphoreType.DMA((layers,)),
            pltpu.SemaphoreType.DMA((layers,)),
            pltpu.SemaphoreType.DMA((layers,)),
            pltpu.SemaphoreType.DMA((layers,)),
            pltpu.SemaphoreType.DMA((2,)),
            pltpu.SemaphoreType.DMA((2,)),
            pltpu.SemaphoreType.DMA((QUARTERS, 4, n_dev // 2)),
            pltpu.SemaphoreType.DMA((QUARTERS, n_dev // 2)),
            pltpu.SemaphoreType.DMA((QUARTERS, n_dev // 2)),
            pltpu.SemaphoreType.DMA((QUARTERS, n_dev // 2)),
            pltpu.SemaphoreType.DMA((QUARTERS,)),
        ],
        compiler_params=pltpu.CompilerParams(collective_id=0, has_side_effects=True, vmem_limit_bytes=VMEM_LIMIT),
        cost_estimate=pl.CostEstimate(flops=flops, bytes_accessed=4 * w_in.size * 4, transcendentals=0),
        name="local_grads",
    )(w_in, w_out, x, y)


def update_kernel(dims, w1, m1, w2, m2, g, x_ref, y_ref, w1o, w2o, m1o, m2o, loss_ref, h_out, nb1, nb2, h_ref, hb_ref):
    layers, rows, d, hid = dims
    piece = hid // 2 // QUARTERS
    step_size = LR_SCALE / layers
    off = (piece // 128) * d
    for n in range(QUARTERS):
        for cb in range(piece // 128):
            cols = slice(n * piece + cb * 128, n * piece + (cb + 1) * 128)
            mn = MOMENTUM * m1[0, :, cols] + g[0, n, cb * d:(cb + 1) * d, :].astype(F32)
            wn = w1[0, :, cols] - step_size * mn
            m1o[0, :, cols] = mn
            w1o[0, :, cols] = wn
            nb1[:, cols] = wn.astype(BF16)
        hid_rows = slice(n * piece, (n + 1) * piece)
        for lb in range(d // 128):
            cols = slice(lb * 128, (lb + 1) * 128)
            mn = MOMENTUM * m2[0, hid_rows, cols] + g[0, n, off + lb * piece:off + (lb + 1) * piece, :].astype(F32)
            wn = w2[0, hid_rows, cols] - step_size * mn
            m2o[0, hid_rows, cols] = mn
            w2o[0, hid_rows, cols] = wn
            nb2[hid_rows, cols] = wn.astype(BF16)

    l, c = pl.program_id(0), pl.program_id(1)

    @pl.when(jnp.logical_and(l == 0, c == 0))
    def _():
        h_ref[...] = x_ref[...].astype(F32)

    @pl.when(c == 0)
    def _():
        hb_ref[...] = h_ref[...].astype(BF16)

    z = mm(hb_ref[...], nb1[...])
    h_ref[...] += mm(gelu(z).astype(BF16), nb2[...])

    @pl.when(jnp.logical_and(l == layers - 1, c == 1))
    def _():
        h_out[...] = h_ref[...]
        diff = h_ref[...] - y_ref[...].astype(F32)
        loss_ref[...] = jnp.sum(diff * diff, axis=-1, keepdims=True) / (2 * d)


def update(w_in, m_in, w_out, m_out, g_all, x, y):
    layers, d, hid = w_in.shape
    rows = x.shape[0]
    hc = hid // 2
    in_spec = pl.BlockSpec((1, d, hc), lambda l, c: (l, 0, c))
    out_spec = pl.BlockSpec((1, hc, d), lambda l, c: (l, c, 0))
    g_spec = pl.BlockSpec((1, *g_all.shape[1:]), lambda l, c: (2 * l + c, 0, 0, 0))
    whole = pl.BlockSpec((rows, d), lambda l, c: (0, 0))
    n_el = 2 * w_in.size
    return pl.pallas_call(
        functools.partial(update_kernel, (layers, rows, d, hid)),
        grid=(layers, 2),
        in_specs=[in_spec, in_spec, out_spec, out_spec, g_spec, whole, whole],
        out_specs=[in_spec, out_spec, in_spec, out_spec, pl.BlockSpec((rows, 1), lambda l, c: (0, 0)), whole],
        out_shape=[jax.ShapeDtypeStruct(a.shape, F32) for a in (w_in, w_out, m_in, m_out)]
        + [jax.ShapeDtypeStruct((rows, 1), F32), jax.ShapeDtypeStruct((rows, d), F32)],
        scratch_shapes=[pltpu.VMEM((d, hc), BF16), pltpu.VMEM((hc, d), BF16), pltpu.VMEM((rows, d), F32), pltpu.VMEM((rows, d), BF16)],
        compiler_params=pltpu.CompilerParams(dimension_semantics=("arbitrary", "arbitrary"), vmem_limit_bytes=VMEM_LIMIT),
        cost_estimate=pl.CostEstimate(flops=4 * rows * d * hid * layers, bytes_accessed=18 * n_el, transcendentals=0),
        name="update",
    )(w_in, m_in, w_out, m_out, g_all, x, y)


def solution(mesh):
    n_dev = mesh.shape["data"]
    rows_spec = P("data", None)

    def local_steps(w_in, w_out, mom_in, mom_out, x_first, y_first, x_second, y_second):
        g_all = local_grads(w_in, w_out, x_first, y_first, n_dev)
        w_in_new, w_out_new, mom_in_new, mom_out_new, loss, h_final = update(w_in, mom_in, w_out, mom_out, g_all, x_second, y_second)
        return w_in_new, w_out_new, mom_in_new, mom_out_new, loss.reshape(-1), h_final

    return jax.shard_map(
        local_steps, mesh=mesh,
        in_specs=(P(), P(), P(), P(), rows_spec, rows_spec, rows_spec, rows_spec),
        out_specs=(P(), P(), P(), P(), P("data"), rows_spec), check_vma=False)
```

```python
import functools

import jax
import jax.numpy as jnp
from jax import lax
from jax.experimental import pallas as pl
from jax.experimental.pallas import tpu as pltpu
from jax.sharding import PartitionSpec as P


LR_SCALE = 1.0
MOMENTUM = 0.9
F32 = jnp.float32
BF16 = jnp.bfloat16
MESH = pl.DeviceIdType.MESH
GELU_C = 0.7978845608028654
GELU_K = 0.044715
SLOTS = 4
QUARTERS = 4
AHEAD = 4
CACHED = 4
FIRST = 1
RELAYS = (
    (100, 10, 1, 1100, 1010, 1001, 2100, 2010, 2001, 10001, 21001, 3100, 3010, 3001, 12001, 23001, 101, 1011, 2,
     10002, 20100, 2101, 3011, 1002, 11010, 21002, 102, 110, 3, 10003, 22100, 1110, 1012, 1003, 13010, 21003, 103,
     2110, 2003, 12003, 3110, 1013, 3003, 23003, 2103, 2002, 12002, 3013, 3002, 23002, 2102, 3012),
    (0, 101, 2, 10000, 1011, 20000, 1000, 2101, 1002, 10002, 3011, 21000, 2000, 100, 2002, 30000, 40002, 11000, 10,
     21002, 3000, 102, 3002, 31000, 41002, 12000, 1010, 22000, 1100, 3, 32000, 40003, 10003, 1012, 2100, 1003,
     21003, 33000, 41003, 12002, 2010, 20100, 103, 2003, 42003, 12003, 1013, 2102, 3003, 23003, 43003, 13000, 110,
     23000, 2103, 42002, 11010, 3013, 23002, 3100, 43002, 3010, 13010, 22100, 1110, 3012, 3110, 2110),
    (1, 102, 3, 10001, 1012, 1001, 2102, 1003, 21001, 10003, 3012, 21003, 2001, 101, 2003, 30001, 40003, 12001,
     1011, 3001, 103, 3003, 23001, 31001, 41003, 12003, 1013, 0, 2101, 20000, 30000, 42003, 10000, 3011, 1000,
     2103, 21000, 31000, 43003, 11000, 10, 2000, 100, 22000, 32000, 12000, 1010, 20100, 3000, 1100, 33000, 11010,
     2010, 23000, 2100, 32001, 13000, 110, 22100, 1110, 33001, 3010, 13010, 23003, 3100, 2110, 3110, 3013),
    (2, 103, 10002, 1013, 1002, 2103, 21002, 3013, 2002, 102, 12002, 1012, 3002, 23002, 2102, 1, 10001, 3012, 1001,
     21001, 101, 0, 10000, 20000, 1011, 1000, 21000, 11000, 100, 10, 20100, 2000, 12000, 1100, 1010, 22000, 11010,
     3000, 2100, 110, 13000, 23000, 2001, 1110, 2010, 22100, 12001, 3001, 3100, 3010, 23001, 13010, 2110, 2101,
     3011, 3110),
)
VMEM_LIMIT = 62 * 1024 * 1024

NN = (((1,), (0,)), ((), ()))
NT = (((1,), (1,)), ((), ()))
TN = (((0,), (0,)), ((), ()))


def mm(a, b, dims=NN):
    return lax.dot_general(a, b, dims, preferred_element_type=F32)


def gelu(z):
    t = jnp.tanh(GELU_C * (z + GELU_K * (z * z * z)))
    return z * (0.5 * (1.0 + t))


def gelu_grad(z):
    zz = z * z
    t = jnp.tanh(GELU_C * (z + GELU_K * (zz * z)))
    cdf = 0.5 * (1.0 + t)
    slope = cdf + (0.5 * z) * (1.0 - t * t) * (GELU_C * (1.0 + (3.0 * GELU_K) * zz))
    return z * cdf, slope


def grads_kernel(dims, w1_hbm, w2_hbm, x_ref, y_ref, *rest):
    n_dev, layers, rows, d, hid = dims
    chips = n_dev // 2
    hc = hid // 2
    piece = hc // QUARTERS
    chips_z = chips // 4
    n_out = 4 * chips_z + 4 * FIRST
    outs, rest = rest[:n_out], rest[n_out:]
    (wb1, wb2, cw1, cw2, z_all, hb, eb, hcur, rh, re, ow1, ow2, aa, ss, acc1, acc2, own,
     w1_sem, w2_sem, hs_sem, hr_sem, es_sem, er_sem, px_send, px_recv,
     sp_send, sp_recv, tw_send, tw_recv, own_sem) = rest

    me = lax.axis_index("data")
    chip = me // 2
    core = me % 2
    partner = chip * 2 + (1 - core)

    cx, cy, cz = chip % 2, (chip // 2) % 2, chip // 4

    def greet(c, carry):
        @pl.when(c != chip)
        def _():
            pl.semaphore_signal(barrier, inc=1, device_id=(2 * c + core,), device_id_type=MESH)

        return carry

    barrier = pltpu.get_barrier_semaphore()
    lax.fori_loop(0, chips, greet, 0)
    pl.semaphore_signal(barrier, inc=1, device_id=(partner,), device_id_type=MESH)

    def w1_copy(l, j, slot):
        return pltpu.make_async_copy(w1_hbm.at[l, :, pl.ds(pl.multiple_of(j * hc, 128), hc)], wb1.at[slot], w1_sem.at[slot])

    def w2_copy(l, j, slot):
        return pltpu.make_async_copy(w2_hbm.at[l, pl.ds(pl.multiple_of(j * hc, 128), hc), :], wb2.at[slot], w2_sem.at[slot])

    def fetch(l, j, slot):
        w1_copy(l, j, slot).start()
        w2_copy(l, j, slot).start()

    def arrived(l, j, slot):
        w1_copy(l, j, slot).wait()
        w2_copy(l, j, slot).wait()

    for i in range(SLOTS):
        fetch(i // 2, i % 2, i)
    pl.semaphore_wait(barrier, chips)

    def h_copy(l):
        return pltpu.make_async_remote_copy(
            src_ref=hb.at[l], dst_ref=rh.at[core * chips + chip], send_sem=hs_sem.at[l], recv_sem=hr_sem.at[chip],
            device_id=(2 * l + core,), device_id_type=MESH)

    def e_copy(l):
        return pltpu.make_async_remote_copy(
            src_ref=eb.at[l], dst_ref=re.at[core * chips + chip], send_sem=es_sem.at[l], recv_sem=er_sem.at[chip],
            device_id=(2 * l + core,), device_id_type=MESH)

    def h_arrival(c):
        return pltpu.make_async_remote_copy(
            src_ref=hb.at[0], dst_ref=rh.at[core * chips + c], send_sem=hs_sem.at[0], recv_sem=hr_sem.at[c],
            device_id=(me,), device_id_type=MESH)

    def e_arrival(c):
        return pltpu.make_async_remote_copy(
            src_ref=eb.at[0], dst_ref=re.at[core * chips + c], send_sem=es_sem.at[0], recv_sem=er_sem.at[c],
            device_id=(me,), device_id_type=MESH)

    def send_h(l):
        @pl.when(l != chip)
        def _():
            h_copy(l).start()

        @pl.when(l == chip)
        def _():
            rh[core * chips + chip] = hb[l]

    def send_e(l):
        @pl.when(l != chip)
        def _():
            e_copy(l).start()

        @pl.when(l == chip)
        def _():
            re[core * chips + chip] = eb[l]

    n_fwd = 2 * layers
    n_bwd = 2 * (layers - 1 - CACHED)
    hcur[...] = x_ref[...].astype(F32)

    def forward(i, carry):
        l, j, slot = i // 2, i % 2, i % SLOTS
        arrived(l, j, slot)

        @pl.when(j == 0)
        def _():
            hb[l] = hcur[...].astype(BF16)

        z = mm(hb[l], wb1[slot].astype(BF16))
        z_all[i] = z
        hcur[...] += mm(gelu(z).astype(BF16), wb2[slot].astype(BF16))

        @pl.when(l >= layers - CACHED)
        def _():
            cw1[i - (n_fwd - 2 * CACHED)] = wb1[slot].astype(BF16)
            cw2[i - (n_fwd - 2 * CACHED)] = wb2[slot].astype(BF16)

        nxt = i + SLOTS

        @pl.when(nxt < n_fwd)
        def _():
            fetch(nxt // 2, nxt % 2, slot)

        @pl.when(nxt >= n_fwd)
        def _():
            fetch(layers - 1 - CACHED - (nxt - n_fwd) // 2, nxt % 2, slot)

        @pl.when(j == 1)
        def _():
            send_h(l)

        return carry

    lax.fori_loop(0, n_fwd, forward, 0)

    scale = 1.0 / (rows * n_dev * d)
    hcur[...] = (hcur[...] - y_ref[...].astype(F32)) * scale

    h_swap = pltpu.make_async_remote_copy(
        src_ref=rh.at[pl.ds(core * chips, chips)], dst_ref=rh.at[pl.ds(core * chips, chips)],
        send_sem=px_send.at[0], recv_sem=px_recv.at[0], device_id=(partner,), device_id_type=MESH)
    e_swap = pltpu.make_async_remote_copy(
        src_ref=re.at[pl.ds(core * chips, chips)], dst_ref=re.at[pl.ds(core * chips, chips)],
        send_sem=px_send.at[1], recv_sem=px_recv.at[1], device_id=(partner,), device_id_type=MESH)

    def error_step(l, j, w1, w2):
        @pl.when(j == 0)
        def _():
            eb[l] = hcur[...].astype(BF16)

        q = mm(eb[l], w2, NT)
        slope = gelu_grad(z_all[2 * l + j])[1]
        hcur[...] += mm((slope * q).astype(BF16), w1, NT)

    def backward_cached(i, carry):
        l, j = layers - 1 - i // 2, i % 2
        kept = 2 * (l - (layers - CACHED)) + j
        error_step(l, j, cw1[kept], cw2[kept])

        @pl.when(j == 1)
        def _():
            send_e(l)

        return carry

    def backward(i, carry):
        l, j, slot = layers - 1 - CACHED - i // 2, i % 2, i % SLOTS
        arrived(l, j, slot)
        error_step(l, j, wb1[slot].astype(BF16), wb2[slot].astype(BF16))
        nxt = i + SLOTS

        @pl.when(nxt < n_bwd)
        def _():
            fetch(layers - 1 - CACHED - nxt // 2, nxt % 2, slot)

        @pl.when(nxt == n_bwd)
        def _():
            fetch(chip, core, slot)

        @pl.when(j == 1)
        def _():
            send_e(l)

        return carry

    lax.fori_loop(0, 2 * CACHED, backward_cached, 0)
    lax.fori_loop(0, n_bwd, backward, 0)
    eb[0] = hcur[...].astype(BF16)

    own_slot = n_bwd % SLOTS
    arrived(chip, core, own_slot)
    ow1[...] = wb1[own_slot].astype(BF16)
    ow2[...] = wb2[own_slot].astype(BF16)
    send_e(0)

    def h_in(c, carry):
        @pl.when(c != chip)
        def _():
            h_arrival(c).wait_recv()

        return carry

    def e_in(c, carry):
        @pl.when(c != chip)
        def _():
            e_arrival(c).wait_recv()

        return carry

    lax.fori_loop(0, chips, h_in, 0)
    h_swap.start()
    lax.fori_loop(0, chips, e_in, 0)
    e_swap.start()

    group = 4
    half_groups = chips // group

    def owner(gi, carry):
        half = (core + gi // half_groups) % 2

        @pl.when(gi == half_groups)
        def _():
            h_swap.wait_recv()
            e_swap.wait_recv()

        base = half * chips + (gi % half_groups) * group
        hg = rh[pl.ds(base, group)].reshape(group * rows, d)
        eg = re[pl.ds(base, group)].reshape(group * rows, d)
        for n in range(QUARTERS):
            cols = slice(n * piece, (n + 1) * piece)
            z = mm(hg, ow1[:, cols])
            q = mm(eg, ow2[cols, :], NT)
            a, slope = gelu_grad(z)
            aa[n, pl.ds(base, group)] = a.astype(BF16).reshape(group, rows, piece)
            ss[n, pl.ds(base, group)] = (slope * q).astype(BF16).reshape(group, rows, piece)
        return carry

    lax.fori_loop(0, 2 * half_groups, owner, 0)

    def place(n, rx, ry, sz, twin):
        sx = 1 - cx if rx else cx
        sy = 1 - cy if ry else cy
        inner, far = (sx, ry) if n % 2 == 0 else (sy, rx)
        at = 4 * chips_z + 4 * sz + 2 * (n % 2) + twin if far else 4 * sz + 2 * (n % 2) + twin
        return outs[at].at[inner, n // 2]

    def source(rx, ry, sz):
        sx = 1 - cx if rx else cx
        sy = 1 - cy if ry else cy
        return sz * 4 + sy * 2 + sx

    hops = (chip + 1 - 2 * cx, chip + 2 - 4 * cy, chip + 4, chip - 4)

    def hop_copy(kind, n, rx, ry, sz, mine):
        src = source(rx, ry, sz)
        there = (n, 1 - rx if kind == 0 else rx, 1 - ry if kind == 1 else ry, sz, 0)
        tx, ty = there[1], there[2]
        inner = (1 - cx if rx else cx) if n % 2 == 0 else (1 - cy if ry else cy)
        far = ty if n % 2 == 0 else tx
        at = 4 * chips_z + 4 * sz + 2 * (n % 2) if far else 4 * sz + 2 * (n % 2)
        return pltpu.make_async_remote_copy(
            src_ref=own.at[n] if mine else place(n, rx, ry, sz, 0), dst_ref=outs[at].at[inner, n // 2],
            send_sem=sp_send.at[n, kind, src], recv_sem=sp_recv.at[n, src],
            device_id=(2 * hops[kind] + core,), device_id_type=MESH)

    def arrival(n, rx, ry, sz):
        return pltpu.make_async_remote_copy(
            src_ref=own.at[n], dst_ref=place(n, rx, ry, sz, 0), send_sem=sp_send.at[n, 0, source(rx, ry, sz)],
            recv_sem=sp_recv.at[n, source(rx, ry, sz)], device_id=(me,), device_id_type=MESH)

    def twin_copy(n, rx, ry, sz, mine):
        src = source(rx, ry, sz)
        return pltpu.make_async_remote_copy(
            src_ref=own.at[n] if mine else place(n, rx, ry, sz, 0), dst_ref=place(n, rx, ry, sz, 1),
            send_sem=tw_send.at[n, src], recv_sem=tw_recv.at[n, src], device_id=(partner,), device_id_type=MESH)

    def own_sends(n, z):
        kinds = [0 if n % 2 == 0 else 1]
        if z < FIRST:
            kinds.append(1 if n % 2 == 0 else 0)
        return kinds + ([2] if z < chips_z - 1 else []) + ([3] if z > 0 else [])

    def at_z(fn):
        for z in range(chips_z):
            pl.when(cz == z)(functools.partial(fn, z))

    def split(code):
        return code // 10000, (code // 1000 % 10, code // 100 % 10, code // 10 % 10, code % 10)

    for n in range(QUARTERS):
        acc1[...] = jnp.zeros_like(acc1)
        acc2[...] = jnp.zeros_like(acc2)

        def products(gi, carry):
            for b in range(group):
                k = gi * group + b
                acc1[...] += mm(rh[k], ss[n, k], TN).astype(BF16).astype(F32)
                acc2[...] += mm(aa[n, k], re[k], TN).astype(BF16).astype(F32)
            return carry

        lax.fori_loop(0, 2 * half_groups, products, 0)
        for cb in range(piece // 128):
            own[n, cb * d:(cb + 1) * d, :] = acc1[:, cb * 128:(cb + 1) * 128].astype(BF16)
        off = (piece // 128) * d
        for lb in range(d // 128):
            own[n, off + lb * piece:off + (lb + 1) * piece, :] = acc2[:, lb * 128:(lb + 1) * 128].astype(BF16)

        def start_own(z, n=n):
            for kind in own_sends(n, z):
                hop_copy(kind, n, 0, 0, z, True).start()
            twin_copy(n, 0, 0, z, True).start()
            pltpu.make_async_copy(own.at[n], place(n, 0, 0, z, 0), own_sem.at[n]).start()

        at_z(start_own)

    def relay(z):
        for code in RELAYS[z]:
            kind, (n, rx, ry, sz) = split(code)
            if kind == 0:
                arrival(n, rx, ry, sz).wait_recv()
                twin_copy(n, rx, ry, sz, False).start()
            else:
                hop_copy(kind - 1, n, rx, ry, sz, False).start()

    at_z(relay)

    def sent(l, carry):
        @pl.when(l != chip)
        def _():
            h_copy(l).wait_send()
            e_copy(l).wait_send()

        return carry

    lax.fori_loop(0, layers, sent, 0)
    h_swap.wait_send()
    e_swap.wait_send()

    def drain(z):
        for n in range(QUARTERS):
            for kind in own_sends(n, z):
                hop_copy(kind, n, 0, 0, z, True).wait_send()
            twin_copy(n, 0, 0, z, True).wait_send()
            pltpu.make_async_copy(own.at[n], place(n, 0, 0, z, 0), own_sem.at[n]).wait()
            twin_copy(n, 0, 0, z, True).wait_recv()
        for code in RELAYS[z]:
            kind, (n, rx, ry, sz) = split(code)
            if kind == 0:
                twin_copy(n, rx, ry, sz, False).wait()
            else:
                hop_copy(kind - 1, n, rx, ry, sz, False).wait_send()

    at_z(drain)


def local_grads(w_in, w_out, x, y, n_dev):
    layers, d, hid = w_in.shape
    rows = x.shape[0]
    hc = hid // 2
    piece = hc // QUARTERS
    g_rows = (piece // 128) * d + (d // 128) * piece
    dims = (n_dev, layers, rows, d, hid)
    n_out = n_dev // 2 + 4 * FIRST
    flops = 2 * rows * d * hid * layers * 4 + 2 * rows * n_dev * d * hc * 4
    return pl.pallas_call(
        functools.partial(grads_kernel, dims),
        out_shape=[jax.ShapeDtypeStruct((2, QUARTERS // 2, g_rows, 128), BF16)] * n_out,
        in_specs=[pl.BlockSpec(memory_space=pl.ANY)] * 2 + [pl.BlockSpec(memory_space=pltpu.VMEM)] * 2,
        out_specs=[pl.BlockSpec(memory_space=pl.ANY)] * n_out,
        scratch_shapes=[
            pltpu.VMEM((SLOTS, d, hc), F32),
            pltpu.VMEM((SLOTS, hc, d), F32),
            pltpu.VMEM((2 * CACHED, d, hc), BF16),
            pltpu.VMEM((2 * CACHED, hc, d), BF16),
            pltpu.VMEM((2 * layers, rows, hc), F32),
            pltpu.VMEM((layers, rows, d), BF16),
            pltpu.VMEM((layers, rows, d), BF16),
            pltpu.VMEM((rows, d), F32),
            pltpu.VMEM((n_dev, rows, d), BF16),
            pltpu.VMEM((n_dev, rows, d), BF16),
            pltpu.VMEM((d, hc), BF16),
            pltpu.VMEM((hc, d), BF16),
            pltpu.VMEM((QUARTERS, n_dev, rows, piece), BF16),
            pltpu.VMEM((QUARTERS, n_dev, rows, piece), BF16),
            pltpu.VMEM((d, piece), F32),
            pltpu.VMEM((piece, d), F32),
            pltpu.VMEM((QUARTERS, g_rows, 128), BF16),
            pltpu.SemaphoreType.DMA((SLOTS,)),
            pltpu.SemaphoreType.DMA((SLOTS,)),
            pltpu.SemaphoreType.DMA((layers,)),
            pltpu.SemaphoreType.DMA((layers,)),
            pltpu.SemaphoreType.DMA((layers,)),
            pltpu.SemaphoreType.DMA((layers,)),
            pltpu.SemaphoreType.DMA((2,)),
            pltpu.SemaphoreType.DMA((2,)),
            pltpu.SemaphoreType.DMA((QUARTERS, 4, n_dev // 2)),
            pltpu.SemaphoreType.DMA((QUARTERS, n_dev // 2)),
            pltpu.SemaphoreType.DMA((QUARTERS, n_dev // 2)),
            pltpu.SemaphoreType.DMA((QUARTERS, n_dev // 2)),
            pltpu.SemaphoreType.DMA((QUARTERS,)),
        ],
        compiler_params=pltpu.CompilerParams(collective_id=0, has_side_effects=True, vmem_limit_bytes=VMEM_LIMIT),
        cost_estimate=pl.CostEstimate(flops=flops, bytes_accessed=4 * w_in.size * 4, transcendentals=0),
        name="local_grads",
    )(w_in, w_out, x, y)


def update_kernel(dims, group, last, *refs):
    layers, _, d, piece = dims
    step_size = LR_SCALE / layers
    chunk = 2 * piece
    steps = 16
    w1, m1, w2, m2, h_in = refs[:5]
    sums = refs[5:13]
    refs = refs[13:]
    if group:
        refs = refs[4:]
    if last:
        y_ref, refs = refs[0], refs[1:]
    w1o, w2o, m1o, m2o, h_out = refs[:5]
    if last:
        loss_ref = refs[5]
    bw1, bm1, bw2, bm2, gbuf, in_sem, out_sem, gsem, nb1, nb2, hb_ref = refs[-11:]
    slots = bw1.shape[0]

    me = lax.axis_index("data")
    chip, core = me // 2, me % 2
    cx, cy = chip % 2, (chip // 2) % 2

    def tile1(ref, t):
        return ref.at[4 * group + t // 4, :, pl.ds(pl.multiple_of((t % 4) * chunk, 128), chunk)]

    def tile2(ref, t):
        return ref.at[4 * group + t // 4, pl.ds(pl.multiple_of((t % 4) * chunk, 8), chunk), :]

    def reads(t, slot):
        return [pltpu.make_async_copy(src, buf.at[slot], in_sem.at[i, slot]) for i, (src, buf) in enumerate(
            ((tile1(w1, t), bw1), (tile1(m1, t), bm1), (tile2(w2, t), bw2), (tile2(m2, t), bm2)))]

    def writes(t, slot):
        return [pltpu.make_async_copy(buf.at[slot], dst, out_sem.at[i, slot]) for i, (dst, buf) in enumerate(
            ((tile1(w1o, t), bw1), (tile1(m1o, t), bm1), (tile2(w2o, t), bw2), (tile2(m2o, t), bm2)))]

    def fetch(t, slot):
        for copy in reads(t, slot):
            copy.start()
        layer, part = t // 4, t % 4
        sx, sy, half, q = layer % 2, layer // 2, part // 2, part % 2
        for par, inner, far in ((0, sx, sy != cy), (1, sy, sx != cx)):
            for is_far in (0, 1):
                for twin in (0, 1):
                    hit = jnp.logical_and(far == bool(is_far), (half != core) == bool(twin))

                    @pl.when(hit)
                    def _(par=par, inner=inner, is_far=is_far, twin=twin):
                        pltpu.make_async_copy(sums[4 * is_far + 2 * par + twin].at[inner, q], gbuf.at[slot, par], gsem.at[par, slot]).start()

    for t in range(AHEAD):
        fetch(t, t)
    h_out[...] = h_in[...].astype(F32)
    off = (piece // 128) * d

    def body(t, carry):
        slot = t % slots

        @pl.when(t % 4 == 0)
        def _():
            hb_ref[...] = h_out[...].astype(BF16)

        for copy in reads(t, slot):
            copy.wait()
        for par in range(2):
            pltpu.make_async_copy(sums[0].at[0, 0], gbuf.at[slot, par], gsem.at[par, slot]).wait()
            for cb in range(piece // 128):
                cols = slice(par * piece + cb * 128, par * piece + (cb + 1) * 128)
                mn = MOMENTUM * bm1[slot, :, cols] + gbuf[slot, par, cb * d:(cb + 1) * d, :].astype(F32)
                wn = bw1[slot, :, cols] - step_size * mn
                bm1[slot, :, cols] = mn
                bw1[slot, :, cols] = wn
                nb1[:, cols] = wn.astype(BF16)
            hid_rows = slice(par * piece, (par + 1) * piece)
            for lb in range(d // 128):
                cols = slice(lb * 128, (lb + 1) * 128)
                mn = MOMENTUM * bm2[slot, hid_rows, cols] + gbuf[slot, par, off + lb * piece:off + (lb + 1) * piece, :].astype(F32)
                wn = bw2[slot, hid_rows, cols] - step_size * mn
                bm2[slot, hid_rows, cols] = mn
                bw2[slot, hid_rows, cols] = wn
                nb2[hid_rows, cols] = wn.astype(BF16)
        for copy in writes(t, slot):
            copy.start()

        @pl.when(t + AHEAD < steps)
        def _():
            nslot = (t + AHEAD) % slots

            @pl.when(t + AHEAD >= slots)
            def _():
                for copy in writes(t + AHEAD - slots, nslot):
                    copy.wait()

            fetch(t + AHEAD, nslot)

        z = mm(hb_ref[...], nb1[...])
        h_out[...] += mm(gelu(z).astype(BF16), nb2[...])
        return carry

    lax.fori_loop(0, steps, body, 0)
    for t in range(steps - slots, steps):
        for copy in writes(t, t % slots):
            copy.wait()
    if last:
        diff = h_out[...] - y_ref[...].astype(F32)
        loss_ref[...] = jnp.sum(diff * diff, axis=-1) / (2 * d)


def update(group, w_in, m_in, w_out, m_out, h, sums, prev, y):
    layers, d, hid = w_in.shape
    rows = h.shape[0]
    piece = hid // 2 // QUARTERS
    chunk = 2 * piece
    last = group == layers // 4 - 1
    whole = pl.BlockSpec(memory_space=pltpu.VMEM)
    any_spec = pl.BlockSpec(memory_space=pl.ANY)
    args = [w_in, m_in, w_out, m_out, h, *sums, *prev] + ([y] if last else [])
    in_specs = [any_spec] * 4 + [whole] + [any_spec] * (8 + len(prev)) + ([whole] if last else [])
    out_specs = [any_spec] * 4 + [whole]
    out_shape = [jax.ShapeDtypeStruct(a.shape, F32) for a in (w_in, w_out, m_in, m_out, h)]
    if last:
        out_specs.append(whole)
        out_shape.append(jax.ShapeDtypeStruct((rows,), F32))
    n_el = 2 * w_in.size // 4
    slots = 7
    return pl.pallas_call(
        functools.partial(update_kernel, (layers, rows, d, piece), group, last),
        in_specs=in_specs,
        out_specs=out_specs,
        out_shape=out_shape,
        scratch_shapes=[
            pltpu.VMEM((slots, d, chunk), F32),
            pltpu.VMEM((slots, d, chunk), F32),
            pltpu.VMEM((slots, chunk, d), F32),
            pltpu.VMEM((slots, chunk, d), F32),
            pltpu.VMEM((slots, 2, *sums[0].shape[2:]), BF16),
            pltpu.SemaphoreType.DMA((4, slots)),
            pltpu.SemaphoreType.DMA((4, slots)),
            pltpu.SemaphoreType.DMA((2, slots)),
            pltpu.VMEM((d, chunk), BF16),
            pltpu.VMEM((chunk, d), BF16),
            pltpu.VMEM((rows, d), BF16),
        ],
        input_output_aliases={13 + i: i for i in range(len(prev))},
        compiler_params=pltpu.CompilerParams(vmem_limit_bytes=VMEM_LIMIT),
        cost_estimate=pl.CostEstimate(flops=5 * 10**10, bytes_accessed=18 * n_el, transcendentals=0),
    )(*args)


def solution(mesh):
    n_dev = mesh.shape["data"]
    rows_spec = P("data", None)
    swap = {axis: [(i, i ^ bit) for i in range(n_dev)] for axis, bit in (("core", 1), ("x", 2), ("y", 4))}

    def send(array, axis):
        return lax.ppermute(array, "data", swap[axis])

    def local_steps(w_in, w_out, mom_in, mom_out, x_first, y_first, x_second, y_second):
        groups = w_in.shape[0] // 4
        sums = local_grads(w_in, w_out, x_first, y_first, n_dev)
        near = [list(sums[4 * g:4 * g + 4]) for g in range(groups)]
        far = [list(sums[4 * (groups + g):4 * (groups + g) + 4]) for g in range(FIRST)]
        for g in range(FIRST, groups):
            from_y = send(near[g][0], "y")
            from_x = send(near[g][2], "x")
            far.append([from_y, send(from_y, "core"), from_x, send(from_x, "core")])
        prev, h = [], x_second
        for g in range(groups):
            outs = update(g, w_in, mom_in, w_out, mom_out, h, near[g] + far[g], prev, y_second)
            prev, h = list(outs[:4]), outs[4]
        w_in_new, w_out_new, mom_in_new, mom_out_new = prev
        return w_in_new, w_out_new, mom_in_new, mom_out_new, outs[5], h

    return jax.shard_map(
        local_steps, mesh=mesh,
        in_specs=(P(), P(), P(), P(), rows_spec, rows_spec, rows_spec, rows_spec),
        out_specs=(P(), P(), P(), P(), P("data"), rows_spec), check_vma=False)
```

```python
import functools

import jax
import jax.numpy as jnp
from jax import lax
from jax.experimental import pallas as pl
from jax.experimental.pallas import tpu as pltpu
from jax.sharding import PartitionSpec as P


LR_SCALE = 1.0
MOMENTUM = 0.9
F32 = jnp.float32
BF16 = jnp.bfloat16
MESH = pl.DeviceIdType.MESH
GELU_C = 0.7978845608028654
GELU_K = 0.044715
SLOTS = 4
QUARTERS = 4
AHEAD = 4
CACHED = 6
FIRST = 1
RELAYS = (
    (
        (30000, 10000, 20000),
        (31000, 11000, 21000),
        (32000,),
        (),
        (100, 10, 1, 10001, 20100, 1100, 1010, 1001, 33000, 12000, 21001, 101, 110, 2, 10002, 22000, 2100, 1011, 1002,
         13000, 21002, 102, 2010, 3, 10003, 23000, 3100, 1012, 1003, 11010, 21003, 103, 3010, 2003, 12003, 22100, 1110,
         1013, 3003, 13010, 23003, 2103, 2110, 2002, 12002, 3110, 3013, 3002, 23002, 2102, 2001, 12001, 3012, 3001,
         23001, 2101, 3011),
    ),
    (
        (30001, 40001, 10001),
        (21001, 31001, 41001),
        (),
        (),
        (0, 101, 2, 10000, 20000, 30000, 40002, 10002, 1011, 1000, 1002, 21000, 100, 31000, 41002, 11000, 10, 21002,
         2000, 3, 102, 32000, 40003, 10003, 1010, 3000, 1003, 21003, 1100, 33000, 41003, 1012, 20100, 2003, 12003, 103,
         32001, 42003, 12000, 1013, 3003, 23003, 2103, 33001, 43003, 11010, 110, 22000, 2002, 2100, 42002, 13000, 3013,
         23000, 3002, 1110, 43002, 12002, 2010, 22100, 3100, 42001, 3010, 13010, 23002, 2102, 43001, 12001, 2110,
         23001, 3110, 3012, 2101, 3011),
    ),
    (
        (30002, 40002, 10002),
        (21002, 31002, 41002),
        (),
        (),
        (1, 102, 3, 10001, 30001, 40003, 10003, 1012, 23002, 1001, 1003, 21001, 101, 31001, 41003, 3012, 0, 2003,
         10000, 20000, 103, 30000, 42003, 1011, 1000, 3003, 11000, 21000, 100, 31000, 43003, 10, 2000, 12000, 20100,
         1100, 32000, 42002, 1010, 11010, 3000, 22000, 2100, 33000, 43002, 13000, 110, 2001, 23000, 1110, 32001, 12003,
         2010, 3001, 22100, 3100, 33001, 3010, 13010, 21003, 2103, 32002, 12001, 2110, 23003, 3110, 33002, 12002, 1013,
         23001, 2101, 3013, 2102, 3011),
    ),
    (
        (40003, 10003),
        (21003, 41003),
        (42003, 12003),
        (),
        (2, 103, 10002, 1013, 23003, 1002, 21002, 102, 43003, 3013, 1, 10001, 2103, 1012, 1001, 21001, 101, 0, 10000,
         20000, 1011, 1000, 21000, 11000, 100, 10, 20100, 2000, 12000, 1100, 1010, 22000, 11010, 3000, 2100, 110,
         13000, 23000, 2001, 1110, 2010, 22100, 12001, 3001, 3100, 3010, 13010, 23001, 2002, 2110, 2101, 12002, 3002,
         23002, 3110, 3011, 3012, 2102),
    ),
)
VMEM_LIMIT = 67043328

NN = (((1,), (0,)), ((), ()))
NT = (((1,), (1,)), ((), ()))
TN = (((0,), (0,)), ((), ()))


def mm(a, b, dims=NN):
    return lax.dot_general(a, b, dims, preferred_element_type=F32)


def gelu(z):
    t = jnp.tanh(GELU_C * (z + GELU_K * (z * z * z)))
    return z * (0.5 * (1.0 + t))


def gelu_grad(z):
    zz = z * z
    t = jnp.tanh(GELU_C * (z + GELU_K * (zz * z)))
    cdf = 0.5 * (1.0 + t)
    slope = cdf + (0.5 * z) * (1.0 - t * t) * (GELU_C * (1.0 + (3.0 * GELU_K) * zz))
    return z * cdf, slope


def grads_kernel(dims, w1_hbm, w2_hbm, x_ref, y_ref, *rest):
    n_dev, layers, rows, d, hid = dims
    chips = n_dev // 2
    hc = hid // 2
    piece = hc // QUARTERS
    chips_z = chips // 4
    n_out = 4 * chips_z + 4 * FIRST
    outs, rest = rest[:n_out], rest[n_out:]
    (wb1, wb2, cw1, cw2, z_all, hb, eb, hcur, rh, re, ow1, ow2, acc1, acc2, own,
     w1_sem, w2_sem, hs_sem, hr_sem, es_sem, er_sem, px_send, px_recv,
     sp_send, sp_recv, tw_send, tw_recv, own_sem) = rest

    me = lax.axis_index("data")
    chip = me // 2
    core = me % 2
    partner = chip * 2 + (1 - core)

    cx, cy, cz = chip % 2, (chip // 2) % 2, chip // 4

    def greet(c, carry):
        @pl.when(c != chip)
        def _():
            pl.semaphore_signal(barrier, inc=1, device_id=(2 * c + core,), device_id_type=MESH)

        return carry

    barrier = pltpu.get_barrier_semaphore()
    lax.fori_loop(0, chips, greet, 0)
    pl.semaphore_signal(barrier, inc=1, device_id=(partner,), device_id_type=MESH)

    def w1_copy(l, j, slot):
        return pltpu.make_async_copy(w1_hbm.at[l, :, pl.ds(pl.multiple_of(j * hc, 128), hc)], wb1.at[slot], w1_sem.at[slot])

    def w2_copy(l, j, slot):
        return pltpu.make_async_copy(w2_hbm.at[l, pl.ds(pl.multiple_of(j * hc, 128), hc), :], wb2.at[slot], w2_sem.at[slot])

    def fetch(l, j, slot):
        w1_copy(l, j, slot).start()
        w2_copy(l, j, slot).start()

    def arrived(l, j, slot):
        w1_copy(l, j, slot).wait()
        w2_copy(l, j, slot).wait()

    for i in range(SLOTS):
        fetch(i // 2, i % 2, i)
    pl.semaphore_wait(barrier, chips)

    def h_copy(l):
        return pltpu.make_async_remote_copy(
            src_ref=hb.at[l], dst_ref=rh.at[core * chips + chip], send_sem=hs_sem.at[l], recv_sem=hr_sem.at[chip],
            device_id=(2 * l + core,), device_id_type=MESH)

    def e_copy(l):
        return pltpu.make_async_remote_copy(
            src_ref=eb.at[l], dst_ref=re.at[core * chips + chip], send_sem=es_sem.at[l], recv_sem=er_sem.at[chip],
            device_id=(2 * l + core,), device_id_type=MESH)

    def h_arrival(c):
        return pltpu.make_async_remote_copy(
            src_ref=hb.at[0], dst_ref=rh.at[core * chips + c], send_sem=hs_sem.at[0], recv_sem=hr_sem.at[c],
            device_id=(me,), device_id_type=MESH)

    def e_arrival(c):
        return pltpu.make_async_remote_copy(
            src_ref=eb.at[0], dst_ref=re.at[core * chips + c], send_sem=es_sem.at[0], recv_sem=er_sem.at[c],
            device_id=(me,), device_id_type=MESH)

    def send_h(l):
        @pl.when(l != chip)
        def _():
            h_copy(l).start()

        @pl.when(l == chip)
        def _():
            rh[core * chips + chip] = hb[l]

    def send_e(l):
        @pl.when(l != chip)
        def _():
            e_copy(l).start()

        @pl.when(l == chip)
        def _():
            re[core * chips + chip] = eb[l]

    n_fwd = 2 * layers
    n_bwd = 2 * (layers - 1 - CACHED)
    hcur[...] = x_ref[...].astype(F32)

    def forward(i, carry):
        l, j, slot = i // 2, i % 2, i % SLOTS
        arrived(l, j, slot)

        @pl.when(j == 0)
        def _():
            hb[l] = hcur[...].astype(BF16)

        z = mm(hb[l], wb1[slot].astype(BF16))
        z_all[i] = z
        hcur[...] += mm(gelu(z).astype(BF16), wb2[slot].astype(BF16))

        @pl.when(l >= layers - CACHED)
        def _():
            cw1[i - (n_fwd - 2 * CACHED)] = wb1[slot].astype(BF16)
            cw2[i - (n_fwd - 2 * CACHED)] = wb2[slot].astype(BF16)

        nxt = i + SLOTS

        @pl.when(nxt < n_fwd)
        def _():
            fetch(nxt // 2, nxt % 2, slot)

        @pl.when(nxt >= n_fwd)
        def _():
            fetch(layers - 1 - CACHED - (nxt - n_fwd) // 2, nxt % 2, slot)

        @pl.when(j == 1)
        def _():
            send_h(l)

        return carry

    lax.fori_loop(0, n_fwd, forward, 0)

    scale = 1.0 / (rows * n_dev * d)
    hcur[...] = (hcur[...] - y_ref[...].astype(F32)) * scale

    h_swap = pltpu.make_async_remote_copy(
        src_ref=rh.at[pl.ds(core * chips, chips)], dst_ref=rh.at[pl.ds(core * chips, chips)],
        send_sem=px_send.at[0], recv_sem=px_recv.at[0], device_id=(partner,), device_id_type=MESH)
    e_swap = pltpu.make_async_remote_copy(
        src_ref=re.at[pl.ds(core * chips, chips)], dst_ref=re.at[pl.ds(core * chips, chips)],
        send_sem=px_send.at[1], recv_sem=px_recv.at[1], device_id=(partner,), device_id_type=MESH)

    def error_step(l, j, w1, w2):
        @pl.when(j == 0)
        def _():
            eb[l] = hcur[...].astype(BF16)

        q = mm(eb[l], w2, NT)
        slope = gelu_grad(z_all[2 * l + j])[1]
        hcur[...] += mm((slope * q).astype(BF16), w1, NT)

    def backward_cached(i, carry):
        l, j = layers - 1 - i // 2, i % 2
        kept = 2 * (l - (layers - CACHED)) + j
        error_step(l, j, cw1[kept], cw2[kept])

        @pl.when(j == 1)
        def _():
            send_e(l)

        return carry

    def backward(i, carry):
        l, j, slot = layers - 1 - CACHED - i // 2, i % 2, i % SLOTS
        arrived(l, j, slot)
        error_step(l, j, wb1[slot].astype(BF16), wb2[slot].astype(BF16))
        nxt = i + SLOTS

        @pl.when(nxt < n_bwd)
        def _():
            fetch(layers - 1 - CACHED - nxt // 2, nxt % 2, slot)

        @pl.when(nxt == n_bwd)
        def _():
            fetch(chip, core, slot)

        @pl.when(j == 1)
        def _():
            send_e(l)

        return carry

    lax.fori_loop(0, 2 * CACHED, backward_cached, 0)
    lax.fori_loop(0, n_bwd, backward, 0)
    eb[0] = hcur[...].astype(BF16)

    own_slot = n_bwd % SLOTS
    arrived(chip, core, own_slot)
    ow1[...] = wb1[own_slot].astype(BF16)
    ow2[...] = wb2[own_slot].astype(BF16)
    send_e(0)

    def h_in(c, carry):
        @pl.when(c != chip)
        def _():
            h_arrival(c).wait_recv()

        return carry

    def e_in(c, carry):
        @pl.when(c != chip)
        def _():
            e_arrival(c).wait_recv()

        return carry

    lax.fori_loop(0, chips, h_in, 0)
    h_swap.start()
    lax.fori_loop(0, chips, e_in, 0)
    e_swap.start()

    def place(n, rx, ry, sz, twin):
        sx = 1 - cx if rx else cx
        sy = 1 - cy if ry else cy
        inner, far = (sx, ry) if n % 2 == 0 else (sy, rx)
        at = 4 * chips_z + 4 * sz + 2 * (n % 2) + twin if far else 4 * sz + 2 * (n % 2) + twin
        return outs[at].at[inner, n // 2]

    def source(rx, ry, sz):
        sx = 1 - cx if rx else cx
        sy = 1 - cy if ry else cy
        return sz * 4 + sy * 2 + sx

    hops = (chip + 1 - 2 * cx, chip + 2 - 4 * cy, chip + 4, chip - 4)

    def hop_copy(kind, n, rx, ry, sz, mine):
        src = source(rx, ry, sz)
        there = (n, 1 - rx if kind == 0 else rx, 1 - ry if kind == 1 else ry, sz, 0)
        tx, ty = there[1], there[2]
        inner = (1 - cx if rx else cx) if n % 2 == 0 else (1 - cy if ry else cy)
        far = ty if n % 2 == 0 else tx
        at = 4 * chips_z + 4 * sz + 2 * (n % 2) if far else 4 * sz + 2 * (n % 2)
        return pltpu.make_async_remote_copy(
            src_ref=own.at[n] if mine else place(n, rx, ry, sz, 0), dst_ref=outs[at].at[inner, n // 2],
            send_sem=sp_send.at[n, kind, src], recv_sem=sp_recv.at[n, src],
            device_id=(2 * hops[kind] + core,), device_id_type=MESH)

    def arrival(n, rx, ry, sz):
        return pltpu.make_async_remote_copy(
            src_ref=own.at[n], dst_ref=place(n, rx, ry, sz, 0), send_sem=sp_send.at[n, 0, source(rx, ry, sz)],
            recv_sem=sp_recv.at[n, source(rx, ry, sz)], device_id=(me,), device_id_type=MESH)

    def twin_copy(n, rx, ry, sz, mine):
        src = source(rx, ry, sz)
        return pltpu.make_async_remote_copy(
            src_ref=own.at[n] if mine else place(n, rx, ry, sz, 0), dst_ref=place(n, rx, ry, sz, 1),
            send_sem=tw_send.at[n, src], recv_sem=tw_recv.at[n, src], device_id=(partner,), device_id_type=MESH)

    def at_z(fn):
        for z in range(chips_z):
            pl.when(cz == z)(functools.partial(fn, z))

    def split(code):
        return code // 10000, (code // 1000 % 10, code // 100 % 10, code // 10 % 10, code % 10)

    def act(z, code):
        kind, block = split(code)
        mine = block[1:] == (0, 0, z)
        if kind:
            hop_copy(kind - 1, *block, mine).start()
        else:
            arrival(*block).wait_recv()
            twin_copy(*block, False).start()

    group = 4
    half_groups = chips // group

    for n in range(QUARTERS):
        cols = slice(n * piece, (n + 1) * piece)
        acc1[...] = jnp.zeros_like(acc1)
        acc2[...] = jnp.zeros_like(acc2)

        def owner(gi, carry, n=n, cols=cols):
            half = (core + gi // half_groups) % 2
            if n == 0:
                @pl.when(gi == half_groups)
                def _():
                    h_swap.wait_recv()
                    e_swap.wait_recv()

            base = half * chips + (gi % half_groups) * group
            hg = rh[pl.ds(base, group)].reshape(group * rows, d)
            eg = re[pl.ds(base, group)].reshape(group * rows, d)
            z = mm(hg, ow1[:, cols])
            q = mm(eg, ow2[cols, :], NT)
            a, slope = gelu_grad(z)
            a = a.astype(BF16)
            s = (slope * q).astype(BF16)
            for b in range(group):
                own_rows = slice(b * rows, (b + 1) * rows)
                acc1[...] += mm(rh[base + b], s[own_rows], TN).astype(BF16).astype(F32)
                acc2[...] += mm(a[own_rows], re[base + b], TN).astype(BF16).astype(F32)
            return carry

        lax.fori_loop(0, 2 * half_groups, owner, 0)
        for cb in range(piece // 128):
            own[n, cb * d:(cb + 1) * d, :] = acc1[:, cb * 128:(cb + 1) * 128].astype(BF16)
        off = (piece // 128) * d
        for lb in range(d // 128):
            own[n, off + lb * piece:off + (lb + 1) * piece, :] = acc2[:, lb * 128:(lb + 1) * 128].astype(BF16)

        def start_own(z, n=n):
            for code in RELAYS[z][n]:
                act(z, code)
            twin_copy(n, 0, 0, z, True).start()
            pltpu.make_async_copy(own.at[n], place(n, 0, 0, z, 0), own_sem.at[n]).start()

        at_z(start_own)

    def relay(z):
        for code in RELAYS[z][QUARTERS]:
            act(z, code)

    at_z(relay)

    def sent(l, carry):
        @pl.when(l != chip)
        def _():
            h_copy(l).wait_send()
            e_copy(l).wait_send()

        return carry

    lax.fori_loop(0, layers, sent, 0)
    h_swap.wait_send()
    e_swap.wait_send()

    def drain(z):
        for n in range(QUARTERS):
            twin_copy(n, 0, 0, z, True).wait()
            pltpu.make_async_copy(own.at[n], place(n, 0, 0, z, 0), own_sem.at[n]).wait()
        for code in sum(RELAYS[z], ()):
            kind, block = split(code)
            if kind:
                hop_copy(kind - 1, *block, block[1:] == (0, 0, z)).wait_send()
            else:
                twin_copy(*block, False).wait()

    at_z(drain)


def local_grads(w_in, w_out, x, y, n_dev):
    layers, d, hid = w_in.shape
    rows = x.shape[0]
    hc = hid // 2
    piece = hc // QUARTERS
    g_rows = (piece // 128) * d + (d // 128) * piece
    dims = (n_dev, layers, rows, d, hid)
    n_out = n_dev // 2 + 4 * FIRST
    flops = 2 * rows * d * hid * layers * 4 + 2 * rows * n_dev * d * hc * 4
    return pl.pallas_call(
        functools.partial(grads_kernel, dims),
        out_shape=[jax.ShapeDtypeStruct((2, QUARTERS // 2, g_rows, 128), BF16)] * n_out,
        in_specs=[pl.BlockSpec(memory_space=pl.ANY)] * 2 + [pl.BlockSpec(memory_space=pltpu.VMEM)] * 2,
        out_specs=[pl.BlockSpec(memory_space=pl.ANY)] * n_out,
        scratch_shapes=[
            pltpu.VMEM((SLOTS, d, hc), F32),
            pltpu.VMEM((SLOTS, hc, d), F32),
            pltpu.VMEM((2 * CACHED, d, hc), BF16),
            pltpu.VMEM((2 * CACHED, hc, d), BF16),
            pltpu.VMEM((2 * layers, rows, hc), F32),
            pltpu.VMEM((layers, rows, d), BF16),
            pltpu.VMEM((layers, rows, d), BF16),
            pltpu.VMEM((rows, d), F32),
            pltpu.VMEM((n_dev, rows, d), BF16),
            pltpu.VMEM((n_dev, rows, d), BF16),
            pltpu.VMEM((d, hc), BF16),
            pltpu.VMEM((hc, d), BF16),
            pltpu.VMEM((d, piece), F32),
            pltpu.VMEM((piece, d), F32),
            pltpu.VMEM((QUARTERS, g_rows, 128), BF16),
            pltpu.SemaphoreType.DMA((SLOTS,)),
            pltpu.SemaphoreType.DMA((SLOTS,)),
            pltpu.SemaphoreType.DMA((layers,)),
            pltpu.SemaphoreType.DMA((layers,)),
            pltpu.SemaphoreType.DMA((layers,)),
            pltpu.SemaphoreType.DMA((layers,)),
            pltpu.SemaphoreType.DMA((2,)),
            pltpu.SemaphoreType.DMA((2,)),
            pltpu.SemaphoreType.DMA((QUARTERS, 4, n_dev // 2)),
            pltpu.SemaphoreType.DMA((QUARTERS, n_dev // 2)),
            pltpu.SemaphoreType.DMA((QUARTERS, n_dev // 2)),
            pltpu.SemaphoreType.DMA((QUARTERS, n_dev // 2)),
            pltpu.SemaphoreType.DMA((QUARTERS,)),
        ],
        compiler_params=pltpu.CompilerParams(collective_id=0, has_side_effects=True, vmem_limit_bytes=VMEM_LIMIT),
        cost_estimate=pl.CostEstimate(flops=flops, bytes_accessed=4 * w_in.size * 4, transcendentals=0),
        name="local_grads",
    )(w_in, w_out, x, y)


def update_kernel(dims, group, last, *refs):
    layers, _, d, piece = dims
    step_size = LR_SCALE / layers
    chunk = 2 * piece
    steps = 16
    w1, m1, w2, m2, h_in = refs[:5]
    sums = refs[5:13]
    refs = refs[13:]
    if group:
        refs = refs[4:]
    if last:
        y_ref, refs = refs[0], refs[1:]
    w1o, w2o, m1o, m2o, h_out = refs[:5]
    if last:
        loss_ref = refs[5]
    bw1, bm1, bw2, bm2, gbuf, in_sem, out_sem, gsem, nb1, nb2, hb_ref = refs[-11:]
    slots = bw1.shape[0]

    me = lax.axis_index("data")
    chip, core = me // 2, me % 2
    cx, cy = chip % 2, (chip // 2) % 2

    def tile1(ref, t):
        return ref.at[4 * group + t // 4, :, pl.ds(pl.multiple_of((t % 4) * chunk, 128), chunk)]

    def tile2(ref, t):
        return ref.at[4 * group + t // 4, pl.ds(pl.multiple_of((t % 4) * chunk, 8), chunk), :]

    def reads(t, slot):
        return [pltpu.make_async_copy(src, buf.at[slot], in_sem.at[i, slot]) for i, (src, buf) in enumerate(
            ((tile1(w1, t), bw1), (tile1(m1, t), bm1), (tile2(w2, t), bw2), (tile2(m2, t), bm2)))]

    def writes(t, slot):
        return [pltpu.make_async_copy(buf.at[slot], dst, out_sem.at[i, slot]) for i, (dst, buf) in enumerate(
            ((tile1(w1o, t), bw1), (tile1(m1o, t), bm1), (tile2(w2o, t), bw2), (tile2(m2o, t), bm2)))]

    def fetch(t, slot):
        for copy in reads(t, slot):
            copy.start()
        layer, part = t // 4, t % 4
        sx, sy, half, q = layer % 2, layer // 2, part // 2, part % 2
        for par, inner, far in ((0, sx, sy != cy), (1, sy, sx != cx)):
            for is_far in (0, 1):
                for twin in (0, 1):
                    hit = jnp.logical_and(far == bool(is_far), (half != core) == bool(twin))

                    @pl.when(hit)
                    def _(par=par, inner=inner, is_far=is_far, twin=twin):
                        pltpu.make_async_copy(sums[4 * is_far + 2 * par + twin].at[inner, q], gbuf.at[slot, par], gsem.at[par, slot]).start()

    for t in range(AHEAD):
        fetch(t, t)
    h_out[...] = h_in[...].astype(F32)
    off = (piece // 128) * d

    def body(t, carry):
        slot = t % slots

        @pl.when(t % 4 == 0)
        def _():
            hb_ref[...] = h_out[...].astype(BF16)

        for copy in reads(t, slot):
            copy.wait()
        for par in range(2):
            pltpu.make_async_copy(sums[0].at[0, 0], gbuf.at[slot, par], gsem.at[par, slot]).wait()
            for cb in range(piece // 128):
                cols = slice(par * piece + cb * 128, par * piece + (cb + 1) * 128)
                mn = MOMENTUM * bm1[slot, :, cols] + gbuf[slot, par, cb * d:(cb + 1) * d, :].astype(F32)
                wn = bw1[slot, :, cols] - step_size * mn
                bm1[slot, :, cols] = mn
                bw1[slot, :, cols] = wn
                nb1[:, cols] = wn.astype(BF16)
            hid_rows = slice(par * piece, (par + 1) * piece)
            for lb in range(d // 128):
                cols = slice(lb * 128, (lb + 1) * 128)
                mn = MOMENTUM * bm2[slot, hid_rows, cols] + gbuf[slot, par, off + lb * piece:off + (lb + 1) * piece, :].astype(F32)
                wn = bw2[slot, hid_rows, cols] - step_size * mn
                bm2[slot, hid_rows, cols] = mn
                bw2[slot, hid_rows, cols] = wn
                nb2[hid_rows, cols] = wn.astype(BF16)
        for copy in writes(t, slot):
            copy.start()

        @pl.when(t + AHEAD < steps)
        def _():
            nslot = (t + AHEAD) % slots

            @pl.when(t + AHEAD >= slots)
            def _():
                for copy in writes(t + AHEAD - slots, nslot):
                    copy.wait()

            fetch(t + AHEAD, nslot)

        z = mm(hb_ref[...], nb1[...])
        h_out[...] += mm(gelu(z).astype(BF16), nb2[...])
        return carry

    lax.fori_loop(0, steps, body, 0)
    for t in range(steps - slots, steps):
        for copy in writes(t, t % slots):
            copy.wait()
    if last:
        diff = h_out[...] - y_ref[...].astype(F32)
        loss_ref[...] = jnp.sum(diff * diff, axis=-1) / (2 * d)


def update(group, w_in, m_in, w_out, m_out, h, sums, prev, y):
    layers, d, hid = w_in.shape
    rows = h.shape[0]
    piece = hid // 2 // QUARTERS
    chunk = 2 * piece
    last = group == layers // 4 - 1
    whole = pl.BlockSpec(memory_space=pltpu.VMEM)
    any_spec = pl.BlockSpec(memory_space=pl.ANY)
    args = [w_in, m_in, w_out, m_out, h, *sums, *prev] + ([y] if last else [])
    in_specs = [any_spec] * 4 + [whole] + [any_spec] * (8 + len(prev)) + ([whole] if last else [])
    out_specs = [any_spec] * 4 + [whole]
    out_shape = [jax.ShapeDtypeStruct(a.shape, F32) for a in (w_in, w_out, m_in, m_out, h)]
    if last:
        out_specs.append(whole)
        out_shape.append(jax.ShapeDtypeStruct((rows,), F32))
    n_el = 2 * w_in.size // 4
    slots = 7
    return pl.pallas_call(
        functools.partial(update_kernel, (layers, rows, d, piece), group, last),
        in_specs=in_specs,
        out_specs=out_specs,
        out_shape=out_shape,
        scratch_shapes=[
            pltpu.VMEM((slots, d, chunk), F32),
            pltpu.VMEM((slots, d, chunk), F32),
            pltpu.VMEM((slots, chunk, d), F32),
            pltpu.VMEM((slots, chunk, d), F32),
            pltpu.VMEM((slots, 2, *sums[0].shape[2:]), BF16),
            pltpu.SemaphoreType.DMA((4, slots)),
            pltpu.SemaphoreType.DMA((4, slots)),
            pltpu.SemaphoreType.DMA((2, slots)),
            pltpu.VMEM((d, chunk), BF16),
            pltpu.VMEM((chunk, d), BF16),
            pltpu.VMEM((rows, d), BF16),
        ],
        input_output_aliases={13 + i: i for i in range(len(prev))},
        compiler_params=pltpu.CompilerParams(vmem_limit_bytes=VMEM_LIMIT),
        cost_estimate=pl.CostEstimate(flops=5 * 10**10, bytes_accessed=18 * n_el, transcendentals=0),
    )(*args)


def solution(mesh):
    n_dev = mesh.shape["data"]
    rows_spec = P("data", None)
    swap = {axis: [(i, i ^ bit) for i in range(n_dev)] for axis, bit in (("core", 1), ("x", 2), ("y", 4))}

    def send(array, axis):
        return lax.ppermute(array, "data", swap[axis])

    def local_steps(w_in, w_out, mom_in, mom_out, x_first, y_first, x_second, y_second):
        groups = w_in.shape[0] // 4
        sums = local_grads(w_in, w_out, x_first, y_first, n_dev)
        near = [list(sums[4 * g:4 * g + 4]) for g in range(groups)]
        far = [list(sums[4 * (groups + g):4 * (groups + g) + 4]) for g in range(FIRST)]
        for g in range(FIRST, groups):
            from_y = send(near[g][0], "y")
            from_x = send(near[g][2], "x")
            far.append([from_y, send(from_y, "core"), from_x, send(from_x, "core")])
        prev, h = [], x_second
        for g in range(groups):
            outs = update(g, w_in, mom_in, w_out, mom_out, h, near[g] + far[g], prev, y_second)
            prev, h = list(outs[:4]), outs[4]
        w_in_new, w_out_new, mom_in_new, mom_out_new = prev
        return w_in_new, w_out_new, mom_in_new, mom_out_new, outs[5], h

    return jax.shard_map(
        local_steps, mesh=mesh,
        in_specs=(P(), P(), P(), P(), rows_spec, rows_spec, rows_spec, rows_spec),
        out_specs=(P(), P(), P(), P(), P("data"), rows_spec), check_vma=False)
```

```python
import functools

import jax
import jax.numpy as jnp
from jax import lax
from jax.experimental import pallas as pl
from jax.experimental.pallas import tpu as pltpu
from jax.sharding import PartitionSpec as P


LR_SCALE = 1.0
MOMENTUM = 0.9
F32 = jnp.float32
BF16 = jnp.bfloat16
MESH = pl.DeviceIdType.MESH
GELU_C = 0.7978845608028654
GELU_K = 0.044715
SLOTS = 4
QUARTERS = 4
AHEAD = 4
TILES = 16
HEAD = 15
CACHED = 6
FIRST = 1
RELAYS = (
    (
        (30000, 10000, 20000),
        (31000, 11000, 21000),
        (32000, 22000),
        (),
        (100, 10, 1, 10001, 1100, 1010, 1001, 33000, 21001, 12000, 101, 2010, 2, 20100, 10002, 2100, 1011, 1002, 21002,
         13000, 102, 110, 3, 23000, 10003, 3100, 1012, 1003, 21003, 11010, 103, 3010, 2003, 22100, 12003, 1110, 1013,
         3003, 23003, 13010, 2103, 2110, 2002, 12002, 3110, 3013, 3002, 23002, 2102, 2001, 12001, 3012, 3001, 23001,
         2101, 3011),
    ),
    (
        (30001, 40001, 10001),
        (21001, 31001, 41001),
        (12001,),
        (),
        (0, 101, 2, 20000, 30000, 40002, 10000, 1011, 1000, 1002, 21000, 31000, 41002, 2101, 10002, 10, 21002, 2000, 3,
         32000, 40003, 100, 10003, 1010, 3000, 1003, 21003, 33000, 41003, 102, 11000, 1012, 22000, 2003, 32001, 42003,
         103, 12003, 1013, 3003, 23003, 33001, 43003, 1100, 12000, 2010, 20100, 2002, 42002, 2103, 11010, 3013, 23000,
         3002, 43002, 2100, 13000, 110, 23002, 42001, 1110, 12002, 3010, 22100, 43001, 3100, 13010, 3012, 23001, 2102,
         2110, 3110, 3011),
    ),
    (
        (30002, 40002, 10002),
        (21002, 31002, 41002),
        (12002,),
        (),
        (1, 102, 3, 30001, 40003, 10001, 23002, 1012, 1001, 1003, 31001, 41003, 21001, 2102, 10003, 0, 3012, 2003,
         30000, 42003, 20000, 101, 10000, 1000, 1011, 3003, 31000, 43003, 21000, 103, 11000, 2000, 10, 32000, 42002,
         22000, 100, 12000, 3000, 1010, 33000, 43002, 20100, 1100, 13000, 2001, 2010, 32001, 23000, 2100, 11010, 3001,
         110, 33001, 22100, 3100, 12003, 3010, 32002, 21003, 1110, 13010, 2110, 33002, 23003, 2103, 12001, 1013, 23001,
         3110, 3013, 2101, 3011),
    ),
    (
        (40003, 10003),
        (21003, 41003),
        (12003, 42003),
        (),
        (2, 103, 10002, 23003, 1013, 1002, 43003, 21002, 2103, 1, 3013, 10001, 102, 1001, 1012, 21001, 101, 0, 10000,
         20000, 1011, 1000, 21000, 11000, 100, 10, 20100, 2000, 12000, 1100, 1010, 22000, 11010, 3000, 2100, 110,
         13000, 23000, 2001, 1110, 2010, 22100, 12001, 3001, 3100, 3010, 13010, 23001, 2002, 2110, 2101, 12002, 3002,
         23002, 3110, 3011, 3012, 2102),
    ),
)
VMEM_LIMIT = 67043328

NN = (((1,), (0,)), ((), ()))
NT = (((1,), (1,)), ((), ()))
TN = (((0,), (0,)), ((), ()))


def mm(a, b, dims=NN):
    return lax.dot_general(a, b, dims, preferred_element_type=F32)


def gelu(z):
    t = jnp.tanh(GELU_C * (z + GELU_K * (z * z * z)))
    return z * (0.5 * (1.0 + t))


def gelu_grad(z):
    zz = z * z
    t = jnp.tanh(GELU_C * (z + GELU_K * (zz * z)))
    cdf = 0.5 * (1.0 + t)
    slope = cdf + (0.5 * z) * (1.0 - t * t) * (GELU_C * (1.0 + (3.0 * GELU_K) * zz))
    return z * cdf, slope


def grads_kernel(dims, w1_hbm, w2_hbm, x_ref, y_ref, *rest):
    n_dev, layers, rows, d, hid = dims
    chips = n_dev // 2
    hc = hid // 2
    piece = hc // QUARTERS
    chips_z = chips // 4
    n_out = 4 * chips_z + 4 * FIRST
    outs, rest = rest[:n_out], rest[n_out:]
    (wb1, wb2, cw1, cw2, z_all, hb, eb, hcur, rh, re, ow1, ow2, acc1, acc2, own,
     w1_sem, w2_sem, hs_sem, hr_sem, es_sem, er_sem, px_send, px_recv,
     sp_send, sp_recv, tw_send, tw_recv, own_sem) = rest

    me = lax.axis_index("data")
    chip = me // 2
    core = me % 2
    partner = chip * 2 + (1 - core)

    cx, cy, cz = chip % 2, (chip // 2) % 2, chip // 4

    def greet(c, carry):
        @pl.when(c != chip)
        def _():
            pl.semaphore_signal(barrier, inc=1, device_id=(2 * c + core,), device_id_type=MESH)

        return carry

    barrier = pltpu.get_barrier_semaphore()
    lax.fori_loop(0, chips, greet, 0)
    pl.semaphore_signal(barrier, inc=1, device_id=(partner,), device_id_type=MESH)

    def w1_copy(l, j, slot):
        return pltpu.make_async_copy(w1_hbm.at[l, :, pl.ds(pl.multiple_of(j * hc, 128), hc)], wb1.at[slot], w1_sem.at[slot])

    def w2_copy(l, j, slot):
        return pltpu.make_async_copy(w2_hbm.at[l, pl.ds(pl.multiple_of(j * hc, 128), hc), :], wb2.at[slot], w2_sem.at[slot])

    def fetch(l, j, slot):
        w1_copy(l, j, slot).start()
        w2_copy(l, j, slot).start()

    def arrived(l, j, slot):
        w1_copy(l, j, slot).wait()
        w2_copy(l, j, slot).wait()

    for i in range(SLOTS):
        fetch(i // 2, i % 2, i)
    pl.semaphore_wait(barrier, chips)

    def h_copy(l):
        return pltpu.make_async_remote_copy(
            src_ref=hb.at[l], dst_ref=rh.at[core * chips + chip], send_sem=hs_sem.at[l], recv_sem=hr_sem.at[chip],
            device_id=(2 * l + core,), device_id_type=MESH)

    def e_copy(l):
        return pltpu.make_async_remote_copy(
            src_ref=eb.at[l], dst_ref=re.at[core * chips + chip], send_sem=es_sem.at[l], recv_sem=er_sem.at[chip],
            device_id=(2 * l + core,), device_id_type=MESH)

    def h_arrival(c):
        return pltpu.make_async_remote_copy(
            src_ref=hb.at[0], dst_ref=rh.at[core * chips + c], send_sem=hs_sem.at[0], recv_sem=hr_sem.at[c],
            device_id=(me,), device_id_type=MESH)

    def e_arrival(c):
        return pltpu.make_async_remote_copy(
            src_ref=eb.at[0], dst_ref=re.at[core * chips + c], send_sem=es_sem.at[0], recv_sem=er_sem.at[c],
            device_id=(me,), device_id_type=MESH)

    def send_h(l):
        @pl.when(l != chip)
        def _():
            h_copy(l).start()

        @pl.when(l == chip)
        def _():
            rh[core * chips + chip] = hb[l]

    def send_e(l):
        @pl.when(l != chip)
        def _():
            e_copy(l).start()

        @pl.when(l == chip)
        def _():
            re[core * chips + chip] = eb[l]

    n_fwd = 2 * layers
    n_bwd = 2 * (layers - 1 - CACHED)
    hcur[...] = x_ref[...].astype(F32)

    def forward(i, carry):
        l, j, slot = i // 2, i % 2, i % SLOTS
        arrived(l, j, slot)

        @pl.when(j == 0)
        def _():
            hb[l] = hcur[...].astype(BF16)

        z = mm(hb[l], wb1[slot].astype(BF16))
        z_all[i] = z
        hcur[...] += mm(gelu(z).astype(BF16), wb2[slot].astype(BF16))

        @pl.when(l >= layers - CACHED)
        def _():
            cw1[i - (n_fwd - 2 * CACHED)] = wb1[slot].astype(BF16)
            cw2[i - (n_fwd - 2 * CACHED)] = wb2[slot].astype(BF16)

        nxt = i + SLOTS

        @pl.when(nxt < n_fwd)
        def _():
            fetch(nxt // 2, nxt % 2, slot)

        @pl.when(nxt >= n_fwd)
        def _():
            fetch(layers - 1 - CACHED - (nxt - n_fwd) // 2, nxt % 2, slot)

        @pl.when(j == 1)
        def _():
            send_h(l)

        return carry

    lax.fori_loop(0, n_fwd, forward, 0)

    scale = 1.0 / (rows * n_dev * d)
    hcur[...] = (hcur[...] - y_ref[...].astype(F32)) * scale

    h_swap = pltpu.make_async_remote_copy(
        src_ref=rh.at[pl.ds(core * chips, chips)], dst_ref=rh.at[pl.ds(core * chips, chips)],
        send_sem=px_send.at[0], recv_sem=px_recv.at[0], device_id=(partner,), device_id_type=MESH)
    e_swap = pltpu.make_async_remote_copy(
        src_ref=re.at[pl.ds(core * chips, chips)], dst_ref=re.at[pl.ds(core * chips, chips)],
        send_sem=px_send.at[1], recv_sem=px_recv.at[1], device_id=(partner,), device_id_type=MESH)

    def error_step(l, j, w1, w2):
        @pl.when(j == 0)
        def _():
            eb[l] = hcur[...].astype(BF16)

        q = mm(eb[l], w2, NT)
        slope = gelu_grad(z_all[2 * l + j])[1]
        hcur[...] += mm((slope * q).astype(BF16), w1, NT)

    def backward_cached(i, carry):
        l, j = layers - 1 - i // 2, i % 2
        kept = 2 * (l - (layers - CACHED)) + j
        error_step(l, j, cw1[kept], cw2[kept])

        @pl.when(j == 1)
        def _():
            send_e(l)

        return carry

    def backward(i, carry):
        l, j, slot = layers - 1 - CACHED - i // 2, i % 2, i % SLOTS
        arrived(l, j, slot)
        error_step(l, j, wb1[slot].astype(BF16), wb2[slot].astype(BF16))
        nxt = i + SLOTS

        @pl.when(nxt < n_bwd)
        def _():
            fetch(layers - 1 - CACHED - nxt // 2, nxt % 2, slot)

        @pl.when(nxt == n_bwd)
        def _():
            fetch(chip, core, slot)

        @pl.when(j == 1)
        def _():
            send_e(l)

        return carry

    lax.fori_loop(0, 2 * CACHED, backward_cached, 0)
    lax.fori_loop(0, n_bwd, backward, 0)
    eb[0] = hcur[...].astype(BF16)

    own_slot = n_bwd % SLOTS
    arrived(chip, core, own_slot)
    ow1[...] = wb1[own_slot].astype(BF16)
    ow2[...] = wb2[own_slot].astype(BF16)
    send_e(0)

    def h_in(c, carry):
        @pl.when(c != chip)
        def _():
            h_arrival(c).wait_recv()

        return carry

    def e_in(c, carry):
        @pl.when(c != chip)
        def _():
            e_arrival(c).wait_recv()

        return carry

    lax.fori_loop(0, chips, h_in, 0)
    h_swap.start()
    lax.fori_loop(0, chips, e_in, 0)
    e_swap.start()

    def place(n, rx, ry, sz, twin):
        sx = 1 - cx if rx else cx
        sy = 1 - cy if ry else cy
        inner, far = (sx, ry) if n % 2 == 0 else (sy, rx)
        at = 4 * chips_z + 4 * sz + 2 * (n % 2) + twin if far else 4 * sz + 2 * (n % 2) + twin
        return outs[at].at[inner, n // 2]

    def source(rx, ry, sz):
        sx = 1 - cx if rx else cx
        sy = 1 - cy if ry else cy
        return sz * 4 + sy * 2 + sx

    hops = (chip + 1 - 2 * cx, chip + 2 - 4 * cy, chip + 4, chip - 4)

    def hop_copy(kind, n, rx, ry, sz, mine):
        src = source(rx, ry, sz)
        there = (n, 1 - rx if kind == 0 else rx, 1 - ry if kind == 1 else ry, sz, 0)
        tx, ty = there[1], there[2]
        inner = (1 - cx if rx else cx) if n % 2 == 0 else (1 - cy if ry else cy)
        far = ty if n % 2 == 0 else tx
        at = 4 * chips_z + 4 * sz + 2 * (n % 2) if far else 4 * sz + 2 * (n % 2)
        return pltpu.make_async_remote_copy(
            src_ref=own.at[n] if mine else place(n, rx, ry, sz, 0), dst_ref=outs[at].at[inner, n // 2],
            send_sem=sp_send.at[n, kind, src], recv_sem=sp_recv.at[n, src],
            device_id=(2 * hops[kind] + core,), device_id_type=MESH)

    def arrival(n, rx, ry, sz):
        return pltpu.make_async_remote_copy(
            src_ref=own.at[n], dst_ref=place(n, rx, ry, sz, 0), send_sem=sp_send.at[n, 0, source(rx, ry, sz)],
            recv_sem=sp_recv.at[n, source(rx, ry, sz)], device_id=(me,), device_id_type=MESH)

    def twin_copy(n, rx, ry, sz, mine):
        src = source(rx, ry, sz)
        return pltpu.make_async_remote_copy(
            src_ref=own.at[n] if mine else place(n, rx, ry, sz, 0), dst_ref=place(n, rx, ry, sz, 1),
            send_sem=tw_send.at[n, src], recv_sem=tw_recv.at[n, src], device_id=(partner,), device_id_type=MESH)

    def at_z(fn):
        for z in range(chips_z):
            pl.when(cz == z)(functools.partial(fn, z))

    def split(code):
        return code // 10000, (code // 1000 % 10, code // 100 % 10, code // 10 % 10, code % 10)

    def act(z, code):
        kind, block = split(code)
        mine = block[1:] == (0, 0, z)
        if kind:
            hop_copy(kind - 1, *block, mine).start()
        else:
            arrival(*block).wait_recv()
            twin_copy(*block, False).start()

    group = 4
    half_groups = chips // group

    for n in range(QUARTERS):
        cols = slice(n * piece, (n + 1) * piece)
        acc1[...] = jnp.zeros_like(acc1)
        acc2[...] = jnp.zeros_like(acc2)

        def owner(gi, carry, n=n, cols=cols):
            half = (core + gi // half_groups) % 2
            if n == 0:
                @pl.when(gi == half_groups)
                def _():
                    h_swap.wait_recv()
                    e_swap.wait_recv()

            base = half * chips + (gi % half_groups) * group
            hg = rh[pl.ds(base, group)].reshape(group * rows, d)
            eg = re[pl.ds(base, group)].reshape(group * rows, d)
            z = mm(hg, ow1[:, cols])
            q = mm(eg, ow2[cols, :], NT)
            a, slope = gelu_grad(z)
            a = a.astype(BF16)
            s = (slope * q).astype(BF16)
            for b in range(group):
                own_rows = slice(b * rows, (b + 1) * rows)
                acc1[...] += mm(rh[base + b], s[own_rows], TN).astype(BF16).astype(F32)
                acc2[...] += mm(a[own_rows], re[base + b], TN).astype(BF16).astype(F32)
            return carry

        lax.fori_loop(0, 2 * half_groups, owner, 0)
        for cb in range(piece // 128):
            own[n, cb * d:(cb + 1) * d, :] = acc1[:, cb * 128:(cb + 1) * 128].astype(BF16)
        off = (piece // 128) * d
        for lb in range(d // 128):
            own[n, off + lb * piece:off + (lb + 1) * piece, :] = acc2[:, lb * 128:(lb + 1) * 128].astype(BF16)

        def start_own(z, n=n):
            for code in RELAYS[z][n]:
                act(z, code)
            twin_copy(n, 0, 0, z, True).start()
            pltpu.make_async_copy(own.at[n], place(n, 0, 0, z, 0), own_sem.at[n]).start()

        at_z(start_own)

    def relay(z):
        for code in RELAYS[z][QUARTERS]:
            act(z, code)

    at_z(relay)

    def sent(l, carry):
        @pl.when(l != chip)
        def _():
            h_copy(l).wait_send()
            e_copy(l).wait_send()

        return carry

    lax.fori_loop(0, layers, sent, 0)
    h_swap.wait_send()
    e_swap.wait_send()

    def drain(z):
        for n in range(QUARTERS):
            twin_copy(n, 0, 0, z, True).wait()
            pltpu.make_async_copy(own.at[n], place(n, 0, 0, z, 0), own_sem.at[n]).wait()
        for code in sum(RELAYS[z], ()):
            kind, block = split(code)
            if kind:
                hop_copy(kind - 1, *block, block[1:] == (0, 0, z)).wait_send()
            else:
                twin_copy(*block, False).wait()

    at_z(drain)


def local_grads(w_in, w_out, x, y, n_dev):
    layers, d, hid = w_in.shape
    rows = x.shape[0]
    hc = hid // 2
    piece = hc // QUARTERS
    g_rows = (piece // 128) * d + (d // 128) * piece
    dims = (n_dev, layers, rows, d, hid)
    n_out = n_dev // 2 + 4 * FIRST
    flops = 2 * rows * d * hid * layers * 4 + 2 * rows * n_dev * d * hc * 4
    return pl.pallas_call(
        functools.partial(grads_kernel, dims),
        out_shape=[jax.ShapeDtypeStruct((2, QUARTERS // 2, g_rows, 128), BF16)] * n_out,
        in_specs=[pl.BlockSpec(memory_space=pl.ANY)] * 2 + [pl.BlockSpec(memory_space=pltpu.VMEM)] * 2,
        out_specs=[pl.BlockSpec(memory_space=pl.ANY)] * n_out,
        scratch_shapes=[
            pltpu.VMEM((SLOTS, d, hc), F32),
            pltpu.VMEM((SLOTS, hc, d), F32),
            pltpu.VMEM((2 * CACHED, d, hc), BF16),
            pltpu.VMEM((2 * CACHED, hc, d), BF16),
            pltpu.VMEM((2 * layers, rows, hc), F32),
            pltpu.VMEM((layers, rows, d), BF16),
            pltpu.VMEM((layers, rows, d), BF16),
            pltpu.VMEM((rows, d), F32),
            pltpu.VMEM((n_dev, rows, d), BF16),
            pltpu.VMEM((n_dev, rows, d), BF16),
            pltpu.VMEM((d, hc), BF16),
            pltpu.VMEM((hc, d), BF16),
            pltpu.VMEM((d, piece), F32),
            pltpu.VMEM((piece, d), F32),
            pltpu.VMEM((QUARTERS, g_rows, 128), BF16),
            pltpu.SemaphoreType.DMA((SLOTS,)),
            pltpu.SemaphoreType.DMA((SLOTS,)),
            pltpu.SemaphoreType.DMA((layers,)),
            pltpu.SemaphoreType.DMA((layers,)),
            pltpu.SemaphoreType.DMA((layers,)),
            pltpu.SemaphoreType.DMA((layers,)),
            pltpu.SemaphoreType.DMA((2,)),
            pltpu.SemaphoreType.DMA((2,)),
            pltpu.SemaphoreType.DMA((QUARTERS, 4, n_dev // 2)),
            pltpu.SemaphoreType.DMA((QUARTERS, n_dev // 2)),
            pltpu.SemaphoreType.DMA((QUARTERS, n_dev // 2)),
            pltpu.SemaphoreType.DMA((QUARTERS, n_dev // 2)),
            pltpu.SemaphoreType.DMA((QUARTERS,)),
        ],
        compiler_params=pltpu.CompilerParams(collective_id=0, has_side_effects=True, vmem_limit_bytes=VMEM_LIMIT),
        cost_estimate=pl.CostEstimate(flops=flops, bytes_accessed=4 * w_in.size * 4, transcendentals=0),
        name="local_grads",
    )(w_in, w_out, x, y)


def update_kernel(dims, group, first, stop, last, *refs):
    layers, _, d, piece = dims
    step_size = LR_SCALE / layers
    chunk = 2 * piece
    w1, m1, w2, m2, h_in, hb_in = refs[:6]
    sums = refs[6:14]
    refs = refs[14:]
    if group or first:
        refs = refs[4:]
    if last:
        y_ref, refs = refs[0], refs[1:]
    w1o, w2o, m1o, m2o, h_out, hb_ref = refs[:6]
    if last:
        loss_ref = refs[6]
    bw1, bm1, bw2, bm2, gbuf, in_sem, out_sem, gsem, nb1, nb2 = refs[-10:]
    slots = bw1.shape[0]

    me = lax.axis_index("data")
    chip, core = me // 2, me % 2
    cx, cy = chip % 2, (chip // 2) % 2

    def tile1(ref, t):
        return ref.at[4 * group + t // 4, :, pl.ds(pl.multiple_of((t % 4) * chunk, 128), chunk)]

    def tile2(ref, t):
        return ref.at[4 * group + t // 4, pl.ds(pl.multiple_of((t % 4) * chunk, 8), chunk), :]

    def reads(t, slot):
        return [pltpu.make_async_copy(src, buf.at[slot], in_sem.at[i, slot]) for i, (src, buf) in enumerate(
            ((tile1(w1, t), bw1), (tile1(m1, t), bm1), (tile2(w2, t), bw2), (tile2(m2, t), bm2)))]

    def writes(t, slot):
        return [pltpu.make_async_copy(buf.at[slot], dst, out_sem.at[i, slot]) for i, (dst, buf) in enumerate(
            ((tile1(w1o, t), bw1), (tile1(m1o, t), bm1), (tile2(w2o, t), bw2), (tile2(m2o, t), bm2)))]

    def fetch(t, slot):
        for copy in reads(t, slot):
            copy.start()
        layer, part = t // 4, t % 4
        sx, sy, half, q = layer % 2, layer // 2, part // 2, part % 2
        for par, inner, far in ((0, sx, sy != cy), (1, sy, sx != cx)):
            for is_far in (0, 1):
                for twin in (0, 1):
                    hit = jnp.logical_and(far == bool(is_far), (half != core) == bool(twin))

                    @pl.when(hit)
                    def _(par=par, inner=inner, is_far=is_far, twin=twin):
                        pltpu.make_async_copy(sums[4 * is_far + 2 * par + twin].at[inner, q], gbuf.at[slot, par], gsem.at[par, slot]).start()

    for t in range(first, min(first + AHEAD, stop)):
        fetch(t, t % slots)
    h_out[...] = h_in[...].astype(F32)
    hb_ref[...] = hb_in[...]
    off = (piece // 128) * d

    def body(t, carry):
        slot = t % slots

        @pl.when(t % 4 == 0)
        def _():
            hb_ref[...] = h_out[...].astype(BF16)

        for copy in reads(t, slot):
            copy.wait()
        for par in range(2):
            pltpu.make_async_copy(sums[0].at[0, 0], gbuf.at[slot, par], gsem.at[par, slot]).wait()
            for cb in range(piece // 128):
                cols = slice(par * piece + cb * 128, par * piece + (cb + 1) * 128)
                mn = MOMENTUM * bm1[slot, :, cols] + gbuf[slot, par, cb * d:(cb + 1) * d, :].astype(F32)
                wn = bw1[slot, :, cols] - step_size * mn
                bm1[slot, :, cols] = mn
                bw1[slot, :, cols] = wn
                nb1[:, cols] = wn.astype(BF16)
            hid_rows = slice(par * piece, (par + 1) * piece)
            for lb in range(d // 128):
                cols = slice(lb * 128, (lb + 1) * 128)
                mn = MOMENTUM * bm2[slot, hid_rows, cols] + gbuf[slot, par, off + lb * piece:off + (lb + 1) * piece, :].astype(F32)
                wn = bw2[slot, hid_rows, cols] - step_size * mn
                bm2[slot, hid_rows, cols] = mn
                bw2[slot, hid_rows, cols] = wn
                nb2[hid_rows, cols] = wn.astype(BF16)
        for copy in writes(t, slot):
            copy.start()

        @pl.when(t + AHEAD < stop)
        def _():
            nslot = (t + AHEAD) % slots

            @pl.when(t + AHEAD >= first + slots)
            def _():
                for copy in writes(t + AHEAD - slots, nslot):
                    copy.wait()

            fetch(t + AHEAD, nslot)

        z = mm(hb_ref[...], nb1[...])
        h_out[...] += mm(gelu(z).astype(BF16), nb2[...])
        return carry

    lax.fori_loop(first, stop, body, 0)
    for t in range(max(first, stop - slots), stop):
        for copy in writes(t, t % slots):
            copy.wait()
    if last:
        diff = h_out[...] - y_ref[...].astype(F32)
        loss_ref[...] = jnp.sum(diff * diff, axis=-1) / (2 * d)


def update(group, first, stop, w_in, m_in, w_out, m_out, h, hb, sums, prev, y):
    layers, d, hid = w_in.shape
    rows = h.shape[0]
    piece = hid // 2 // QUARTERS
    chunk = 2 * piece
    last = group == layers // 4 - 1 and stop == TILES
    whole = pl.BlockSpec(memory_space=pltpu.VMEM)
    any_spec = pl.BlockSpec(memory_space=pl.ANY)
    args = [w_in, m_in, w_out, m_out, h, hb, *sums, *prev] + ([y] if last else [])
    in_specs = [any_spec] * 4 + [whole] * 2 + [any_spec] * (8 + len(prev)) + ([whole] if last else [])
    out_specs = [any_spec] * 4 + [whole] * 2
    out_shape = [jax.ShapeDtypeStruct(a.shape, F32) for a in (w_in, w_out, m_in, m_out, h)]
    out_shape.append(jax.ShapeDtypeStruct(hb.shape, BF16))
    if last:
        out_specs.append(whole)
        out_shape.append(jax.ShapeDtypeStruct((rows,), F32))
    n_el = 2 * w_in.size // 4 * (stop - first) // TILES
    slots = min(7, stop - first)
    return pl.pallas_call(
        functools.partial(update_kernel, (layers, rows, d, piece), group, first, stop, last),
        in_specs=in_specs,
        out_specs=out_specs,
        out_shape=out_shape,
        scratch_shapes=[
            pltpu.VMEM((slots, d, chunk), F32),
            pltpu.VMEM((slots, d, chunk), F32),
            pltpu.VMEM((slots, chunk, d), F32),
            pltpu.VMEM((slots, chunk, d), F32),
            pltpu.VMEM((slots, 2, *sums[0].shape[2:]), BF16),
            pltpu.SemaphoreType.DMA((4, slots)),
            pltpu.SemaphoreType.DMA((4, slots)),
            pltpu.SemaphoreType.DMA((2, slots)),
            pltpu.VMEM((d, chunk), BF16),
            pltpu.VMEM((chunk, d), BF16),
        ],
        input_output_aliases={14 + i: i for i in range(len(prev))},
        compiler_params=pltpu.CompilerParams(vmem_limit_bytes=VMEM_LIMIT),
        cost_estimate=pl.CostEstimate(flops=3 * 10**9 * (stop - first), bytes_accessed=18 * n_el, transcendentals=0),
    )(*args)


def solution(mesh):
    n_dev = mesh.shape["data"]
    rows_spec = P("data", None)
    swap = {axis: [(i, i ^ bit) for i in range(n_dev)] for axis, bit in (("core", 1), ("x", 2), ("y", 4))}

    def send(array, axis):
        return lax.ppermute(array, "data", swap[axis])

    def local_steps(w_in, w_out, mom_in, mom_out, x_first, y_first, x_second, y_second):
        groups = w_in.shape[0] // 4
        sums = local_grads(w_in, w_out, x_first, y_first, n_dev)
        near = [list(sums[4 * g:4 * g + 4]) for g in range(groups)]
        far = [list(sums[4 * (groups + g):4 * (groups + g) + 4]) for g in range(FIRST)]
        for g in range(FIRST, groups):
            from_y = send(near[g][0], "y")
            from_x = send(near[g][2], "x")
            far.append([from_y, send(from_y, "core"), from_x, send(from_x, "core")])
        prev, h, hb = [], x_second, x_second
        for g in range(groups):
            cuts = [0, HEAD, TILES] if g < groups - 1 else [0, TILES]
            for part in range(len(cuts) - 1):
                outs = update(g, cuts[part], cuts[part + 1], w_in, mom_in, w_out, mom_out, h, hb, near[g] + far[g], prev, y_second)
                prev, h, hb = list(outs[:4]), outs[4], outs[5]
        w_in_new, w_out_new, mom_in_new, mom_out_new = prev
        return w_in_new, w_out_new, mom_in_new, mom_out_new, outs[6], h

    return jax.shard_map(
        local_steps, mesh=mesh,
        in_specs=(P(), P(), P(), P(), rows_spec, rows_spec, rows_spec, rows_spec),
        out_specs=(P(), P(), P(), P(), P("data"), rows_spec), check_vma=False)
```

```python
import functools

import jax
import jax.numpy as jnp
from jax import lax
from jax.experimental import pallas as pl
from jax.experimental.pallas import tpu as pltpu
from jax.sharding import PartitionSpec as P


LR_SCALE = 1.0
MOMENTUM = 0.9
F32 = jnp.float32
BF16 = jnp.bfloat16
MESH = pl.DeviceIdType.MESH
GELU_C = 0.7978845608028654
GELU_K = 0.044715
SLOTS = 4
RING = 3
QUARTERS = 4
AHEAD = 4
CACHED = 6
FIRST = 1
RELAYS = (
    (
        (30000, 10000, 20000),
        (31000, 11000, 21000),
        (32000, 22000),
        (),
        (100, 10, 1, 10001, 1100, 1010, 1001, 33000, 12000, 21001, 101, 2010, 2, 10002, 20100, 2100, 1011, 1002, 13000,
         21002, 102, 110, 3, 10003, 23000, 3100, 1012, 1003, 11010, 21003, 103, 3010, 2003, 12003, 22100, 1110, 1013,
         3003, 13010, 23003, 2103, 2110, 2002, 12002, 3110, 3013, 3002, 23002, 2102, 2001, 12001, 3012, 3001, 23001,
         2101, 3011),
    ),
    (
        (30001, 40001, 10001),
        (21001, 31001, 41001),
        (12001,),
        (),
        (0, 101, 2, 20000, 30000, 40002, 10000, 1011, 1000, 1002, 21000, 2101, 31000, 41002, 10002, 10, 21002, 2000, 3,
         100, 32000, 40003, 10003, 1010, 3000, 1003, 21003, 102, 33000, 41003, 11000, 1012, 22000, 2003, 103, 32001,
         42003, 12003, 1013, 3003, 23003, 1100, 33001, 43003, 12000, 2010, 20100, 2002, 2103, 42002, 11010, 3013,
         23000, 3002, 2100, 43002, 13000, 110, 23002, 1110, 42001, 12002, 3010, 22100, 3100, 43001, 13010, 3012, 23001,
         2102, 2110, 3110, 3011),
    ),
    (
        (30002, 40002, 10002),
        (21002, 31002, 41002),
        (12002,),
        (),
        (1, 102, 3, 30001, 40003, 10001, 23002, 1012, 1001, 1003, 21001, 2102, 31001, 41003, 10003, 3012, 0, 2003,
         20000, 101, 30000, 42003, 10000, 1011, 1000, 3003, 21000, 103, 31000, 43003, 11000, 10, 2000, 22000, 100,
         32000, 42002, 12000, 1010, 20100, 3000, 1100, 33000, 43002, 11010, 2010, 23000, 2001, 2100, 32001, 13000, 110,
         22100, 3001, 1110, 33001, 3010, 13010, 21003, 3100, 32002, 12003, 2110, 23003, 3110, 33002, 12001, 1013,
         23001, 2103, 3013, 2101, 3011),
    ),
    (
        (40003, 10003),
        (21003, 41003),
        (12003, 42003),
        (),
        (2, 103, 10002, 23003, 1013, 1002, 21002, 2103, 43003, 3013, 1, 10001, 102, 1012, 1001, 21001, 101, 0, 10000,
         20000, 1011, 1000, 21000, 11000, 100, 10, 20100, 2000, 12000, 1100, 1010, 22000, 11010, 3000, 2100, 110,
         13000, 23000, 2001, 1110, 2010, 22100, 12001, 3001, 3100, 3010, 13010, 23001, 2002, 2110, 2101, 12002, 3002,
         23002, 3110, 3011, 3012, 2102),
    ),
)
VMEM_LIMIT = 67043328

NN = (((1,), (0,)), ((), ()))
NT = (((1,), (1,)), ((), ()))
TN = (((0,), (0,)), ((), ()))


def mm(a, b, dims=NN):
    return lax.dot_general(a, b, dims, preferred_element_type=F32)


def gelu(z):
    t = jnp.tanh(GELU_C * (z + GELU_K * (z * z * z)))
    return z * (0.5 * (1.0 + t))


def gelu_grad(z):
    zz = z * z
    t = jnp.tanh(GELU_C * (z + GELU_K * (zz * z)))
    cdf = 0.5 * (1.0 + t)
    slope = cdf + (0.5 * z) * (1.0 - t * t) * (GELU_C * (1.0 + (3.0 * GELU_K) * zz))
    return z * cdf, slope


def grads_kernel(dims, w1_hbm, w2_hbm, x_ref, y_ref, *rest):
    n_dev, layers, rows, d, hid = dims
    chips = n_dev // 2
    hc = hid // 2
    piece = hc // QUARTERS
    chips_z = chips // 4
    n_out = 4 * chips_z + 4 * FIRST
    outs, rest = rest[:n_out], rest[n_out:]
    (wb1, wb2, own2, far2, cw1, cw2, z_all, hb, eb, hcur, rh, re, ow1, ow2, acc1, acc2, own,
     w1_sem, w2_sem, x_send, x_recv, free_sem, hs_sem, hr_sem, es_sem, er_sem, px_send, px_recv,
     sp_send, sp_recv, tw_send, tw_recv, own_sem) = rest

    me = lax.axis_index("data")
    chip = me // 2
    core = me % 2
    partner = chip * 2 + (1 - core)

    cx, cy, cz = chip % 2, (chip // 2) % 2, chip // 4

    def greet(c, carry):
        @pl.when(c != chip)
        def _():
            pl.semaphore_signal(barrier, inc=1, device_id=(2 * c + core,), device_id_type=MESH)

        return carry

    barrier = pltpu.get_barrier_semaphore()
    lax.fori_loop(0, chips, greet, 0)
    pl.semaphore_signal(barrier, inc=1, device_id=(partner,), device_id_type=MESH)

    n_fwd, n_bwd = layers, layers - 1 - CACHED
    top = layers - 1 - CACHED
    n_steps = n_fwd + n_bwd

    def w1_copy(l, j, slot):
        return pltpu.make_async_copy(w1_hbm.at[l, :, pl.ds(pl.multiple_of(j * hc, 128), hc)], wb1.at[slot], w1_sem.at[slot])

    def w2_copy(l, slot):
        return pltpu.make_async_copy(w2_hbm.at[l, pl.ds(pl.multiple_of(core * hc, 128), hc), :], wb2.at[slot], w2_sem.at[slot])

    def pass_copy(step):
        at = step % RING
        return pltpu.make_async_remote_copy(
            src_ref=own2.at[at], dst_ref=far2.at[at], send_sem=x_send.at[at], recv_sem=x_recv.at[at],
            device_id=(partner,), device_id_type=MESH)

    def take_in(step):
        own2[step % RING] = wb2[step % 2].astype(BF16)

    def chunk(m):
        return (core + m) % 2

    for step in range(2):
        w2_copy(step, step).start()
        for m in range(2):
            w1_copy(step, chunk(m), 2 * step + m).start()
    pl.semaphore_wait(barrier, chips)
    for step in range(2):
        w2_copy(step, step).wait()
        take_in(step)
        pass_copy(step).start()
        w2_copy(step + 2, step).start()

    def h_copy(l):
        return pltpu.make_async_remote_copy(
            src_ref=hb.at[l], dst_ref=rh.at[core * chips + chip], send_sem=hs_sem.at[l], recv_sem=hr_sem.at[chip],
            device_id=(2 * l + core,), device_id_type=MESH)

    def e_copy(l):
        return pltpu.make_async_remote_copy(
            src_ref=eb.at[l], dst_ref=re.at[core * chips + chip], send_sem=es_sem.at[l], recv_sem=er_sem.at[chip],
            device_id=(2 * l + core,), device_id_type=MESH)

    def h_arrival(c):
        return pltpu.make_async_remote_copy(
            src_ref=hb.at[0], dst_ref=rh.at[core * chips + c], send_sem=hs_sem.at[0], recv_sem=hr_sem.at[c],
            device_id=(me,), device_id_type=MESH)

    def e_arrival(c):
        return pltpu.make_async_remote_copy(
            src_ref=eb.at[0], dst_ref=re.at[core * chips + c], send_sem=es_sem.at[0], recv_sem=er_sem.at[c],
            device_id=(me,), device_id_type=MESH)

    def send_h(l):
        @pl.when(l != chip)
        def _():
            h_copy(l).start()

        @pl.when(l == chip)
        def _():
            rh[core * chips + chip] = hb[l]

    def send_e(l):
        @pl.when(l != chip)
        def _():
            e_copy(l).start()

        @pl.when(l == chip)
        def _():
            re[core * chips + chip] = eb[l]

    hcur[...] = x_ref[...].astype(F32)

    def ahead(step):
        @pl.when(step >= 1)
        def _():
            pass_copy(step - 1).wait_send()
            pl.semaphore_wait(free_sem.at[(step + 2) % RING], 1)

        w2_copy(0, step % 2).wait()
        take_in(step + 2)

    def release(step):
        @pl.when(step <= n_steps - 1 - RING)
        def _():
            pl.semaphore_signal(free_sem.at[step % RING], inc=1, device_id=(partner,), device_id_type=MESH)

    def forward(step, carry):
        ahead(step)

        @pl.when(step + 4 < n_fwd)
        def _():
            w2_copy(step + 4, step % 2).start()

        @pl.when(step + 4 >= n_fwd)
        def _():
            w2_copy(top - (step + 4 - n_fwd), step % 2).start()

        hb[step] = hcur[...].astype(BF16)
        for m in range(2):
            j, slot = chunk(m), (2 * step + m) % SLOTS
            w1_copy(0, 0, slot).wait()
            if m == 1:
                pass_copy(step).wait_recv()
            w2 = own2 if m == 0 else far2
            z = mm(hb[step], wb1[slot].astype(BF16))
            z_all[2 * step + j] = z
            hcur[...] += mm(gelu(z).astype(BF16), w2[step % RING])
            if m == 0:
                pass_copy(step + 2).start()

            @pl.when(step >= layers - CACHED)
            def _(m=m, j=j, slot=slot, w2=w2):
                kept = 2 * (step - (layers - CACHED)) + j
                cw1[kept] = wb1[slot].astype(BF16)
                cw2[kept] = w2[step % RING]

            @pl.when(step + 2 < n_fwd)
            def _(j=j, slot=slot):
                w1_copy(step + 2, j, slot).start()

            @pl.when(step + 2 >= n_fwd)
            def _(j=j, slot=slot):
                w1_copy(top - (step + 2 - n_fwd), j, slot).start()
        release(step)
        send_h(step)
        return carry

    lax.fori_loop(0, n_fwd, forward, 0)

    scale = 1.0 / (rows * n_dev * d)
    hcur[...] = (hcur[...] - y_ref[...].astype(F32)) * scale

    h_swap = pltpu.make_async_remote_copy(
        src_ref=rh.at[pl.ds(core * chips, chips)], dst_ref=rh.at[pl.ds(core * chips, chips)],
        send_sem=px_send.at[0], recv_sem=px_recv.at[0], device_id=(partner,), device_id_type=MESH)
    e_swap = pltpu.make_async_remote_copy(
        src_ref=re.at[pl.ds(core * chips, chips)], dst_ref=re.at[pl.ds(core * chips, chips)],
        send_sem=px_send.at[1], recv_sem=px_recv.at[1], device_id=(partner,), device_id_type=MESH)

    def error_step(l, j, w1, w2):
        q = mm(eb[l], w2, NT)
        slope = gelu_grad(z_all[2 * l + j])[1]
        hcur[...] += mm((slope * q).astype(BF16), w1, NT)

    def backward_cached(i, carry):
        l = layers - 1 - i
        eb[l] = hcur[...].astype(BF16)
        for j in range(2):
            kept = 2 * (l - (layers - CACHED)) + j
            error_step(l, j, cw1[kept], cw2[kept])
        send_e(l)
        return carry

    def backward(i, carry):
        l, step = top - i, n_fwd + i

        @pl.when(step + 2 < n_steps)
        def _():
            ahead(step)

        @pl.when(step + 4 < n_steps)
        def _():
            w2_copy(l - 4, step % 2).start()

        @pl.when(step + 4 == n_steps)
        def _():
            w2_copy(chip, step % 2).start()

        eb[l] = hcur[...].astype(BF16)
        for m in range(2):
            j, slot = chunk(m), (2 * step + m) % SLOTS
            w1_copy(0, 0, slot).wait()
            if m == 1:
                pass_copy(step).wait_recv()
            error_step(l, j, wb1[slot].astype(BF16), (own2 if m == 0 else far2)[step % RING])

            @pl.when(step + 2 < n_steps)
            def _(m=m, j=j, slot=slot):
                if m == 0:
                    pass_copy(step + 2).start()
                w1_copy(l - 2, j, slot).start()

            if m == 0:
                @pl.when(step + 2 == n_steps)
                def _(j=j, slot=slot):
                    w1_copy(chip, j, slot).start()
        release(step)
        send_e(l)
        return carry

    lax.fori_loop(0, CACHED, backward_cached, 0)
    lax.fori_loop(0, n_bwd, backward, 0)
    eb[0] = hcur[...].astype(BF16)

    w1_copy(0, 0, (2 * n_steps) % SLOTS).wait()
    w2_copy(0, n_steps % 2).wait()
    ow1[...] = wb1[(2 * n_steps) % SLOTS].astype(BF16)
    ow2[...] = wb2[n_steps % 2].astype(BF16)
    send_e(0)

    def h_in(c, carry):
        @pl.when(c != chip)
        def _():
            h_arrival(c).wait_recv()

        return carry

    def e_in(c, carry):
        @pl.when(c != chip)
        def _():
            e_arrival(c).wait_recv()

        return carry

    lax.fori_loop(0, chips, h_in, 0)
    h_swap.start()
    lax.fori_loop(0, chips, e_in, 0)
    e_swap.start()

    def place(n, rx, ry, sz, twin):
        sx = 1 - cx if rx else cx
        sy = 1 - cy if ry else cy
        inner, far = (sx, ry) if n % 2 == 0 else (sy, rx)
        at = 4 * chips_z + 4 * sz + 2 * (n % 2) + twin if far else 4 * sz + 2 * (n % 2) + twin
        return outs[at].at[inner, n // 2]

    def source(rx, ry, sz):
        sx = 1 - cx if rx else cx
        sy = 1 - cy if ry else cy
        return sz * 4 + sy * 2 + sx

    hops = (chip + 1 - 2 * cx, chip + 2 - 4 * cy, chip + 4, chip - 4)

    def hop_copy(kind, n, rx, ry, sz, mine, part=None):
        src = source(rx, ry, sz)
        there = (n, 1 - rx if kind == 0 else rx, 1 - ry if kind == 1 else ry, sz, 0)
        tx, ty = there[1], there[2]
        inner = (1 - cx if rx else cx) if n % 2 == 0 else (1 - cy if ry else cy)
        far = ty if n % 2 == 0 else tx
        at = 4 * chips_z + 4 * sz + 2 * (n % 2) if far else 4 * sz + 2 * (n % 2)
        src_ref, dst_ref = own.at[n] if mine else place(n, rx, ry, sz, 0), outs[at].at[inner, n // 2]
        if part is not None:
            src_ref, dst_ref = src_ref.at[part], dst_ref.at[part]
        return pltpu.make_async_remote_copy(
            src_ref=src_ref, dst_ref=dst_ref, send_sem=sp_send.at[n, kind, src], recv_sem=sp_recv.at[n, src],
            device_id=(2 * hops[kind] + core,), device_id_type=MESH)

    def arrival(n, rx, ry, sz):
        return pltpu.make_async_remote_copy(
            src_ref=own.at[n], dst_ref=place(n, rx, ry, sz, 0), send_sem=sp_send.at[n, 0, source(rx, ry, sz)],
            recv_sem=sp_recv.at[n, source(rx, ry, sz)], device_id=(me,), device_id_type=MESH)

    def twin_copy(n, rx, ry, sz, mine):
        src = source(rx, ry, sz)
        return pltpu.make_async_remote_copy(
            src_ref=own.at[n] if mine else place(n, rx, ry, sz, 0), dst_ref=place(n, rx, ry, sz, 1),
            send_sem=tw_send.at[n, src], recv_sem=tw_recv.at[n, src], device_id=(partner,), device_id_type=MESH)

    def at_z(fn):
        for z in range(chips_z):
            pl.when(cz == z)(functools.partial(fn, z))

    def split(code):
        return code // 10000, (code // 1000 % 10, code // 100 % 10, code // 10 % 10, code % 10)

    def act(z, code):
        kind, block = split(code)
        mine = block[1:] == (0, 0, z)
        if kind:
            hop_copy(kind - 1, *block, mine).start()
        else:
            arrival(*block).wait_recv()
            twin_copy(*block, False).start()

    group = 4
    half_groups = chips // group

    def row_groups(body, wait=False):
        def step(gi, carry):
            if wait:
                @pl.when(gi == half_groups)
                def _():
                    h_swap.wait_recv()
                    e_swap.wait_recv()

            half = (core + gi // half_groups) % 2
            base = half * chips + (gi % half_groups) * group
            body(base, rh[pl.ds(base, group)].reshape(group * rows, d), re[pl.ds(base, group)].reshape(group * rows, d))
            return carry

        lax.fori_loop(0, 2 * half_groups, step, 0)

    def add_in(base, s):
        for b in range(group):
            acc1[...] += mm(rh[base + b], s[b * rows:(b + 1) * rows], TN).astype(BF16).astype(F32)

    def add_out(base, a):
        for b in range(group):
            acc2[...] += mm(a[b * rows:(b + 1) * rows], re[base + b], TN).astype(BF16).astype(F32)

    def store_in(n):
        for cb in range(piece // 128):
            own[n, 0, cb * d:(cb + 1) * d, :] = acc1[:, cb * 128:(cb + 1) * 128].astype(BF16)

    def store_out(n):
        for lb in range(d // 128):
            own[n, 1, lb * piece:(lb + 1) * piece, :] = acc2[:, lb * 128:(lb + 1) * 128].astype(BF16)

    def send_part(part):
        def start(z):
            for code in RELAYS[z][0]:
                kind, block = split(code)
                hop_copy(kind - 1, *block, True, part).start()

        at_z(start)

    acc1[...] = jnp.zeros_like(acc1)
    acc2[...] = jnp.zeros_like(acc2)

    def first_out(base, hg, eg):
        a, slope = gelu_grad(mm(hg, ow1[:, :piece]))
        z_all[pl.ds(base, group), :, :piece] = slope.reshape(group, rows, piece)
        add_out(base, a.astype(BF16))

    def first_in(base, hg, eg):
        q = mm(eg, ow2[:piece, :], NT)
        add_in(base, (z_all[pl.ds(base, group), :, :piece].reshape(group * rows, piece) * q).astype(BF16))

    row_groups(first_out, wait=True)
    store_out(0)
    send_part(1)
    row_groups(first_in)
    store_in(0)
    send_part(0)

    def start_rest(n):
        def start(z):
            for code in RELAYS[z][n] if n else ():
                act(z, code)
            twin_copy(n, 0, 0, z, True).start()
            pltpu.make_async_copy(own.at[n], place(n, 0, 0, z, 0), own_sem.at[n]).start()

        at_z(start)

    start_rest(0)
    for n in range(1, QUARTERS):
        cols = slice(n * piece, (n + 1) * piece)
        acc1[...] = jnp.zeros_like(acc1)
        acc2[...] = jnp.zeros_like(acc2)

        def both(base, hg, eg, cols=cols):
            a, slope = gelu_grad(mm(hg, ow1[:, cols]))
            q = mm(eg, ow2[cols, :], NT)
            a = a.astype(BF16)
            s = (slope * q).astype(BF16)
            for b in range(group):
                own_rows = slice(b * rows, (b + 1) * rows)
                acc1[...] += mm(rh[base + b], s[own_rows], TN).astype(BF16).astype(F32)
                acc2[...] += mm(a[own_rows], re[base + b], TN).astype(BF16).astype(F32)

        row_groups(both)
        store_in(n)
        store_out(n)
        start_rest(n)

    def relay(z):
        for code in RELAYS[z][QUARTERS]:
            act(z, code)

    at_z(relay)

    def sent(l, carry):
        @pl.when(l != chip)
        def _():
            h_copy(l).wait_send()
            e_copy(l).wait_send()

        return carry

    lax.fori_loop(0, layers, sent, 0)
    h_swap.wait_send()
    e_swap.wait_send()
    for step in range(n_steps - RING, n_steps):
        pass_copy(step).wait_send()

    def drain(z):
        for n in range(QUARTERS):
            twin_copy(n, 0, 0, z, True).wait()
            pltpu.make_async_copy(own.at[n], place(n, 0, 0, z, 0), own_sem.at[n]).wait()
        for code in sum(RELAYS[z], ()):
            kind, block = split(code)
            if kind:
                hop_copy(kind - 1, *block, block[1:] == (0, 0, z)).wait_send()
            else:
                twin_copy(*block, False).wait()

    at_z(drain)


def local_grads(w_in, w_out, x, y, n_dev):
    layers, d, hid = w_in.shape
    rows = x.shape[0]
    hc = hid // 2
    piece = hc // QUARTERS
    part_rows = piece * d // 128
    dims = (n_dev, layers, rows, d, hid)
    n_out = n_dev // 2 + 4 * FIRST
    flops = 2 * rows * d * hid * layers * 4 + 2 * rows * n_dev * d * hc * 4
    return pl.pallas_call(
        functools.partial(grads_kernel, dims),
        out_shape=[jax.ShapeDtypeStruct((2, QUARTERS // 2, 2, part_rows, 128), BF16)] * n_out,
        in_specs=[pl.BlockSpec(memory_space=pl.ANY)] * 2 + [pl.BlockSpec(memory_space=pltpu.VMEM)] * 2,
        out_specs=[pl.BlockSpec(memory_space=pl.ANY)] * n_out,
        scratch_shapes=[
            pltpu.VMEM((SLOTS, d, hc), F32),
            pltpu.VMEM((2, hc, d), F32),
            pltpu.VMEM((RING, hc, d), BF16),
            pltpu.VMEM((RING, hc, d), BF16),
            pltpu.VMEM((2 * CACHED, d, hc), BF16),
            pltpu.VMEM((2 * CACHED, hc, d), BF16),
            pltpu.VMEM((2 * layers, rows, hc), F32),
            pltpu.VMEM((layers, rows, d), BF16),
            pltpu.VMEM((layers, rows, d), BF16),
            pltpu.VMEM((rows, d), F32),
            pltpu.VMEM((n_dev, rows, d), BF16),
            pltpu.VMEM((n_dev, rows, d), BF16),
            pltpu.VMEM((d, hc), BF16),
            pltpu.VMEM((hc, d), BF16),
            pltpu.VMEM((d, piece), F32),
            pltpu.VMEM((piece, d), F32),
            pltpu.VMEM((QUARTERS, 2, part_rows, 128), BF16),
            pltpu.SemaphoreType.DMA((SLOTS,)),
            pltpu.SemaphoreType.DMA((2,)),
            pltpu.SemaphoreType.DMA((RING,)),
            pltpu.SemaphoreType.DMA((RING,)),
            pltpu.SemaphoreType.REGULAR((RING,)),
            pltpu.SemaphoreType.DMA((layers,)),
            pltpu.SemaphoreType.DMA((layers,)),
            pltpu.SemaphoreType.DMA((layers,)),
            pltpu.SemaphoreType.DMA((layers,)),
            pltpu.SemaphoreType.DMA((2,)),
            pltpu.SemaphoreType.DMA((2,)),
            pltpu.SemaphoreType.DMA((QUARTERS, 4, n_dev // 2)),
            pltpu.SemaphoreType.DMA((QUARTERS, n_dev // 2)),
            pltpu.SemaphoreType.DMA((QUARTERS, n_dev // 2)),
            pltpu.SemaphoreType.DMA((QUARTERS, n_dev // 2)),
            pltpu.SemaphoreType.DMA((QUARTERS,)),
        ],
        compiler_params=pltpu.CompilerParams(collective_id=0, has_side_effects=True, vmem_limit_bytes=VMEM_LIMIT),
        cost_estimate=pl.CostEstimate(flops=flops, bytes_accessed=4 * w_in.size * 4, transcendentals=0),
        name="local_grads",
    )(w_in, w_out, x, y)


def update_kernel(dims, group, last, *refs):
    layers, _, d, piece = dims
    step_size = LR_SCALE / layers
    chunk = 2 * piece
    steps = 16
    w1, m1, w2, m2, h_in = refs[:5]
    sums = refs[5:13]
    refs = refs[13:]
    if group:
        refs = refs[4:]
    if last:
        y_ref, refs = refs[0], refs[1:]
    w1o, w2o, m1o, m2o, h_out = refs[:5]
    if last:
        loss_ref = refs[5]
    bw1, bm1, bw2, bm2, gbuf, in_sem, out_sem, gsem, nb1, nb2, hb_ref = refs[-11:]
    slots = bw1.shape[0]

    me = lax.axis_index("data")
    chip, core = me // 2, me % 2
    cx, cy = chip % 2, (chip // 2) % 2

    def tile1(ref, t):
        return ref.at[4 * group + t // 4, :, pl.ds(pl.multiple_of((t % 4) * chunk, 128), chunk)]

    def tile2(ref, t):
        return ref.at[4 * group + t // 4, pl.ds(pl.multiple_of((t % 4) * chunk, 8), chunk), :]

    def reads(t, slot):
        return [pltpu.make_async_copy(src, buf.at[slot], in_sem.at[i, slot]) for i, (src, buf) in enumerate(
            ((tile1(w1, t), bw1), (tile1(m1, t), bm1), (tile2(w2, t), bw2), (tile2(m2, t), bm2)))]

    def writes(t, slot):
        return [pltpu.make_async_copy(buf.at[slot], dst, out_sem.at[i, slot]) for i, (dst, buf) in enumerate(
            ((tile1(w1o, t), bw1), (tile1(m1o, t), bm1), (tile2(w2o, t), bw2), (tile2(m2o, t), bm2)))]

    def fetch(t, slot):
        for copy in reads(t, slot):
            copy.start()
        layer, part = t // 4, t % 4
        sx, sy, half, q = layer % 2, layer // 2, part // 2, part % 2
        for par, inner, far in ((0, sx, sy != cy), (1, sy, sx != cx)):
            for is_far in (0, 1):
                for twin in (0, 1):
                    hit = jnp.logical_and(far == bool(is_far), (half != core) == bool(twin))

                    @pl.when(hit)
                    def _(par=par, inner=inner, is_far=is_far, twin=twin):
                        pltpu.make_async_copy(sums[4 * is_far + 2 * par + twin].at[inner, q], gbuf.at[slot, par], gsem.at[par, slot]).start()

    for t in range(AHEAD):
        fetch(t, t)
    h_out[...] = h_in[...].astype(F32)

    def body(t, carry):
        slot = t % slots

        @pl.when(t % 4 == 0)
        def _():
            hb_ref[...] = h_out[...].astype(BF16)

        for copy in reads(t, slot):
            copy.wait()
        for par in range(2):
            pltpu.make_async_copy(sums[0].at[0, 0], gbuf.at[slot, par], gsem.at[par, slot]).wait()
            for cb in range(piece // 128):
                cols = slice(par * piece + cb * 128, par * piece + (cb + 1) * 128)
                mn = MOMENTUM * bm1[slot, :, cols] + gbuf[slot, par, 0, cb * d:(cb + 1) * d, :].astype(F32)
                wn = bw1[slot, :, cols] - step_size * mn
                bm1[slot, :, cols] = mn
                bw1[slot, :, cols] = wn
                nb1[:, cols] = wn.astype(BF16)
            hid_rows = slice(par * piece, (par + 1) * piece)
            for lb in range(d // 128):
                cols = slice(lb * 128, (lb + 1) * 128)
                mn = MOMENTUM * bm2[slot, hid_rows, cols] + gbuf[slot, par, 1, lb * piece:(lb + 1) * piece, :].astype(F32)
                wn = bw2[slot, hid_rows, cols] - step_size * mn
                bm2[slot, hid_rows, cols] = mn
                bw2[slot, hid_rows, cols] = wn
                nb2[hid_rows, cols] = wn.astype(BF16)
        for copy in writes(t, slot):
            copy.start()

        @pl.when(t + AHEAD < steps)
        def _():
            nslot = (t + AHEAD) % slots

            @pl.when(t + AHEAD >= slots)
            def _():
                for copy in writes(t + AHEAD - slots, nslot):
                    copy.wait()

            fetch(t + AHEAD, nslot)

        z = mm(hb_ref[...], nb1[...])
        h_out[...] += mm(gelu(z).astype(BF16), nb2[...])
        return carry

    lax.fori_loop(0, steps, body, 0)
    for t in range(steps - slots, steps):
        for copy in writes(t, t % slots):
            copy.wait()
    if last:
        diff = h_out[...] - y_ref[...].astype(F32)
        loss_ref[...] = jnp.sum(diff * diff, axis=-1) / (2 * d)


def update(group, w_in, m_in, w_out, m_out, h, sums, prev, y):
    layers, d, hid = w_in.shape
    rows = h.shape[0]
    piece = hid // 2 // QUARTERS
    chunk = 2 * piece
    last = group == layers // 4 - 1
    whole = pl.BlockSpec(memory_space=pltpu.VMEM)
    any_spec = pl.BlockSpec(memory_space=pl.ANY)
    args = [w_in, m_in, w_out, m_out, h, *sums, *prev] + ([y] if last else [])
    in_specs = [any_spec] * 4 + [whole] + [any_spec] * (8 + len(prev)) + ([whole] if last else [])
    out_specs = [any_spec] * 4 + [whole]
    out_shape = [jax.ShapeDtypeStruct(a.shape, F32) for a in (w_in, w_out, m_in, m_out, h)]
    if last:
        out_specs.append(whole)
        out_shape.append(jax.ShapeDtypeStruct((rows,), F32))
    n_el = 2 * w_in.size // 4
    slots = 7
    return pl.pallas_call(
        functools.partial(update_kernel, (layers, rows, d, piece), group, last),
        in_specs=in_specs,
        out_specs=out_specs,
        out_shape=out_shape,
        scratch_shapes=[
            pltpu.VMEM((slots, d, chunk), F32),
            pltpu.VMEM((slots, d, chunk), F32),
            pltpu.VMEM((slots, chunk, d), F32),
            pltpu.VMEM((slots, chunk, d), F32),
            pltpu.VMEM((slots, 2, *sums[0].shape[2:]), BF16),
            pltpu.SemaphoreType.DMA((4, slots)),
            pltpu.SemaphoreType.DMA((4, slots)),
            pltpu.SemaphoreType.DMA((2, slots)),
            pltpu.VMEM((d, chunk), BF16),
            pltpu.VMEM((chunk, d), BF16),
            pltpu.VMEM((rows, d), BF16),
        ],
        input_output_aliases={13 + i: i for i in range(len(prev))},
        compiler_params=pltpu.CompilerParams(vmem_limit_bytes=VMEM_LIMIT),
        cost_estimate=pl.CostEstimate(flops=5 * 10**10, bytes_accessed=18 * n_el, transcendentals=0),
    )(*args)


def solution(mesh):
    n_dev = mesh.shape["data"]
    rows_spec = P("data", None)
    swap = {axis: [(i, i ^ bit) for i in range(n_dev)] for axis, bit in (("core", 1), ("x", 2), ("y", 4))}

    def send(array, axis):
        return lax.ppermute(array, "data", swap[axis])

    def local_steps(w_in, w_out, mom_in, mom_out, x_first, y_first, x_second, y_second):
        groups = w_in.shape[0] // 4
        sums = local_grads(w_in, w_out, x_first, y_first, n_dev)
        near = [list(sums[4 * g:4 * g + 4]) for g in range(groups)]
        far = [list(sums[4 * (groups + g):4 * (groups + g) + 4]) for g in range(FIRST)]
        for g in range(FIRST, groups):
            from_y = send(near[g][0], "y")
            from_x = send(near[g][2], "x")
            far.append([from_y, send(from_y, "core"), from_x, send(from_x, "core")])
        prev, h = [], x_second
        for g in range(groups):
            outs = update(g, w_in, mom_in, w_out, mom_out, h, near[g] + far[g], prev, y_second)
            prev, h = list(outs[:4]), outs[4]
        w_in_new, w_out_new, mom_in_new, mom_out_new = prev
        return w_in_new, w_out_new, mom_in_new, mom_out_new, outs[5], h

    return jax.shard_map(
        local_steps, mesh=mesh,
        in_specs=(P(), P(), P(), P(), rows_spec, rows_spec, rows_spec, rows_spec),
        out_specs=(P(), P(), P(), P(), P("data"), rows_spec), check_vma=False)
```

```python
import functools

import jax
import jax.numpy as jnp
from jax import lax
from jax.experimental import pallas as pl
from jax.experimental.pallas import tpu as pltpu
from jax.sharding import PartitionSpec as P


LR_SCALE = 1.0
MOMENTUM = 0.9
F32 = jnp.float32
BF16 = jnp.bfloat16
MESH = pl.DeviceIdType.MESH
GELU_C = 0.7978845608028654
GELU_K = 0.044715
SLOTS = 4
RING = 3
QUARTERS = 4
AHEAD = 4
CACHED = 6
FIRST = 1
RELAYS = (
    (
        (30000, 10000, 20000),
        (31000, 11000, 21000),
        (100, 10, 1, 10001, 20100, 32000),
        (),
        (33000, 12000, 1100, 1010, 1001, 21001, 22000, 101, 110, 2, 10002, 13000, 2100, 1011, 1002, 21002, 23000, 102,
         2010, 3, 10003, 11010, 3100, 1012, 1003, 21003, 22100, 103, 3010, 2003, 12003, 13010, 1110, 1013, 3003, 23003,
         2103, 2110, 2002, 12002, 3110, 3013, 3002, 23002, 2102, 2001, 12001, 3012, 3001, 23001, 2101, 3011),
    ),
    (
        (30001, 40001, 10001),
        (21001, 31001, 41001),
        (0, 101, 2, 10000, 20000, 30000, 40002, 10002),
        (),
        (1011, 1000, 1002, 21000, 31000, 41002, 11000, 100, 21002, 10, 2000, 3, 32000, 40003, 10003, 102, 1010, 3000,
         1003, 21003, 33000, 41003, 1100, 20100, 32001, 1012, 2003, 12003, 42003, 12000, 103, 33001, 1013, 3003, 23003,
         43003, 11010, 2103, 22000, 110, 2002, 42002, 13000, 2100, 23000, 3013, 3002, 43002, 12002, 1110, 22100, 42001,
         2010, 3100, 23002, 43001, 3010, 13010, 12001, 2102, 23001, 2110, 3110, 3012, 2101, 3011),
    ),
    (
        (30002, 40002, 10002),
        (21002, 31002, 41002),
        (1, 102, 3, 10001, 30001, 40003, 10003),
        (),
        (23002, 1012, 1001, 1003, 31001, 41003, 21001, 101, 0, 2003, 10000, 30000, 42003, 20000, 3012, 103, 1000, 3003,
         11000, 31000, 43003, 21000, 1011, 100, 42002, 2000, 12000, 32000, 20100, 10, 12003, 1100, 43002, 3000, 33000,
         22000, 1010, 13000, 2100, 2001, 32001, 23000, 110, 11010, 2103, 3001, 33001, 22100, 2010, 12001, 3100, 32002,
         21003, 3010, 13010, 1110, 33002, 23003, 2110, 12002, 2101, 23001, 1013, 3110, 3013, 2102, 3011),
    ),
    (
        (40003, 10003),
        (21003, 41003),
        (2, 103, 10002, 42003, 12003),
        (),
        (23003, 43003, 1013, 1002, 21002, 102, 1, 10001, 3013, 2103, 1001, 21001, 1012, 101, 0, 10000, 20000, 1011,
         1000, 21000, 11000, 100, 10, 20100, 2000, 12000, 22000, 1100, 1010, 11010, 3000, 13000, 23000, 2100, 110,
         2001, 22100, 12001, 1110, 2010, 3001, 23001, 3100, 3010, 13010, 2002, 12002, 2110, 2101, 3002, 23002, 3110,
         3011, 3012, 2102),
    ),
)
VMEM_LIMIT = 67043328

NN = (((1,), (0,)), ((), ()))
NT = (((1,), (1,)), ((), ()))
TN = (((0,), (0,)), ((), ()))


def mm(a, b, dims=NN):
    return lax.dot_general(a, b, dims, preferred_element_type=F32)


def gelu(z):
    t = jnp.tanh(GELU_C * (z + GELU_K * (z * z * z)))
    return z * (0.5 * (1.0 + t))


def gelu_grad(z):
    zz = z * z
    t = jnp.tanh(GELU_C * (z + GELU_K * (zz * z)))
    cdf = 0.5 * (1.0 + t)
    slope = cdf + (0.5 * z) * (1.0 - t * t) * (GELU_C * (1.0 + (3.0 * GELU_K) * zz))
    return z * cdf, slope


def grads_kernel(dims, w1_hbm, w2_hbm, x_hbm, y_hbm, *rest):
    n_dev, layers, rows, d, hid = dims
    chips = n_dev // 2
    hc = hid // 2
    piece = hc // QUARTERS
    chips_z = chips // 4
    n_out = 4 * chips_z + 4 * FIRST
    outs, rest = rest[:n_out], rest[n_out:]
    (x_ref, y_ref, xy_sem, wb1, wb2, own2, far2, cw1, cw2, z_all, hb, eb, hcur, rh, re, ow1, ow2, acc1, acc2, own,
     w1_sem, w2_sem, x_send, x_recv, free_sem, hs_sem, hr_sem, es_sem, er_sem, px_send, px_recv,
     sp_send, sp_recv, tw_send, tw_recv, own_sem) = rest

    me = lax.axis_index("data")
    chip = me // 2
    core = me % 2
    partner = chip * 2 + (1 - core)

    cx, cy, cz = chip % 2, (chip // 2) % 2, chip // 4

    def greet(c, carry):
        @pl.when(c != chip)
        def _():
            pl.semaphore_signal(barrier, inc=1, device_id=(2 * c + core,), device_id_type=MESH)

        return carry

    barrier = pltpu.get_barrier_semaphore()
    lax.fori_loop(0, chips, greet, 0)
    pl.semaphore_signal(barrier, inc=1, device_id=(partner,), device_id_type=MESH)

    n_fwd, n_bwd = layers, layers - 1 - CACHED
    top = layers - 1 - CACHED
    n_steps = n_fwd + n_bwd

    def w1_copy(l, j, slot):
        return pltpu.make_async_copy(w1_hbm.at[l, :, pl.ds(pl.multiple_of(j * hc, 128), hc)], wb1.at[slot], w1_sem.at[slot])

    def w2_copy(l, slot):
        return pltpu.make_async_copy(w2_hbm.at[l, pl.ds(pl.multiple_of(core * hc, 128), hc), :], wb2.at[slot], w2_sem.at[slot])

    def pass_copy(step):
        at = step % RING
        return pltpu.make_async_remote_copy(
            src_ref=own2.at[at], dst_ref=far2.at[at], send_sem=x_send.at[at], recv_sem=x_recv.at[at],
            device_id=(partner,), device_id_type=MESH)

    def take_in(step):
        own2[step % RING] = wb2[step % 2].astype(BF16)

    def chunk(m):
        return (core + m) % 2

    takes = [pltpu.make_async_copy(src, dst, xy_sem.at[i]) for i, (src, dst) in enumerate(((x_hbm, x_ref), (y_hbm, y_ref)))]
    for step in range(2):
        w2_copy(step, step).start()
        if step == 0:
            for copy in takes:
                copy.start()
        for m in range(2):
            w1_copy(step, chunk(m), 2 * step + m).start()
    pl.semaphore_wait(barrier, chips)
    for step in range(2):
        w2_copy(step, step).wait()
        take_in(step)
        pass_copy(step).start()
        w2_copy(step + 2, step).start()

    def h_copy(l):
        return pltpu.make_async_remote_copy(
            src_ref=hb.at[l], dst_ref=rh.at[core * chips + chip], send_sem=hs_sem.at[l], recv_sem=hr_sem.at[chip],
            device_id=(2 * l + core,), device_id_type=MESH)

    def e_copy(l):
        return pltpu.make_async_remote_copy(
            src_ref=eb.at[l], dst_ref=re.at[core * chips + chip], send_sem=es_sem.at[l], recv_sem=er_sem.at[chip],
            device_id=(2 * l + core,), device_id_type=MESH)

    def h_arrival(c):
        return pltpu.make_async_remote_copy(
            src_ref=hb.at[0], dst_ref=rh.at[core * chips + c], send_sem=hs_sem.at[0], recv_sem=hr_sem.at[c],
            device_id=(me,), device_id_type=MESH)

    def e_arrival(c):
        return pltpu.make_async_remote_copy(
            src_ref=eb.at[0], dst_ref=re.at[core * chips + c], send_sem=es_sem.at[0], recv_sem=er_sem.at[c],
            device_id=(me,), device_id_type=MESH)

    def send_h(l):
        @pl.when(l != chip)
        def _():
            h_copy(l).start()

        @pl.when(l == chip)
        def _():
            rh[core * chips + chip] = hb[l]

    def send_e(l):
        @pl.when(l != chip)
        def _():
            e_copy(l).start()

        @pl.when(l == chip)
        def _():
            re[core * chips + chip] = eb[l]

    for copy in takes:
        copy.wait()
    hcur[...] = x_ref[...].astype(F32)

    def ahead(step):
        @pl.when(step >= 1)
        def _():
            pass_copy(step - 1).wait_send()
            pl.semaphore_wait(free_sem.at[(step + 2) % RING], 1)

        w2_copy(0, step % 2).wait()
        take_in(step + 2)

    def release(step):
        @pl.when(step <= n_steps - 1 - RING)
        def _():
            pl.semaphore_signal(free_sem.at[step % RING], inc=1, device_id=(partner,), device_id_type=MESH)

    def forward(step, carry):
        ahead(step)

        @pl.when(step + 4 < n_fwd)
        def _():
            w2_copy(step + 4, step % 2).start()

        @pl.when(step + 4 >= n_fwd)
        def _():
            w2_copy(top - (step + 4 - n_fwd), step % 2).start()

        hb[step] = hcur[...].astype(BF16)
        for m in range(2):
            j, slot = chunk(m), (2 * step + m) % SLOTS
            w1_copy(0, 0, slot).wait()
            if m == 1:
                pass_copy(step).wait_recv()
            w2 = own2 if m == 0 else far2
            z = mm(hb[step], wb1[slot].astype(BF16))
            z_all[2 * step + j] = z
            hcur[...] += mm(gelu(z).astype(BF16), w2[step % RING])
            if m == 0:
                pass_copy(step + 2).start()

            @pl.when(step >= layers - CACHED)
            def _(m=m, j=j, slot=slot, w2=w2):
                kept = 2 * (step - (layers - CACHED)) + j
                cw1[kept] = wb1[slot].astype(BF16)
                cw2[kept] = w2[step % RING]

            @pl.when(step + 2 < n_fwd)
            def _(j=j, slot=slot):
                w1_copy(step + 2, j, slot).start()

            @pl.when(step + 2 >= n_fwd)
            def _(j=j, slot=slot):
                w1_copy(top - (step + 2 - n_fwd), j, slot).start()
        release(step)
        send_h(step)
        return carry

    lax.fori_loop(0, n_fwd, forward, 0)

    scale = 1.0 / (rows * n_dev * d)
    hcur[...] = (hcur[...] - y_ref[...].astype(F32)) * scale

    h_swap = pltpu.make_async_remote_copy(
        src_ref=rh.at[pl.ds(core * chips, chips)], dst_ref=rh.at[pl.ds(core * chips, chips)],
        send_sem=px_send.at[0], recv_sem=px_recv.at[0], device_id=(partner,), device_id_type=MESH)
    e_swap = pltpu.make_async_remote_copy(
        src_ref=re.at[pl.ds(core * chips, chips)], dst_ref=re.at[pl.ds(core * chips, chips)],
        send_sem=px_send.at[1], recv_sem=px_recv.at[1], device_id=(partner,), device_id_type=MESH)

    def error_step(l, j, w1, w2):
        q = mm(eb[l], w2, NT)
        slope = gelu_grad(z_all[2 * l + j])[1]
        hcur[...] += mm((slope * q).astype(BF16), w1, NT)

    def backward_cached(i, carry):
        l = layers - 1 - i
        eb[l] = hcur[...].astype(BF16)
        for j in range(2):
            kept = 2 * (l - (layers - CACHED)) + j
            error_step(l, j, cw1[kept], cw2[kept])
        send_e(l)
        return carry

    def backward(i, carry):
        l, step = top - i, n_fwd + i

        @pl.when(step + 2 < n_steps)
        def _():
            ahead(step)

        @pl.when(step + 4 < n_steps)
        def _():
            w2_copy(l - 4, step % 2).start()

        @pl.when(step + 4 == n_steps)
        def _():
            w2_copy(chip, step % 2).start()

        eb[l] = hcur[...].astype(BF16)
        for m in range(2):
            j, slot = chunk(m), (2 * step + m) % SLOTS
            w1_copy(0, 0, slot).wait()
            if m == 1:
                pass_copy(step).wait_recv()
            error_step(l, j, wb1[slot].astype(BF16), (own2 if m == 0 else far2)[step % RING])

            @pl.when(step + 2 < n_steps)
            def _(m=m, j=j, slot=slot):
                if m == 0:
                    pass_copy(step + 2).start()
                w1_copy(l - 2, j, slot).start()

            if m == 0:
                @pl.when(step + 2 == n_steps)
                def _(j=j, slot=slot):
                    w1_copy(chip, j, slot).start()
        release(step)
        send_e(l)
        return carry

    lax.fori_loop(0, CACHED, backward_cached, 0)
    lax.fori_loop(0, n_bwd, backward, 0)
    eb[0] = hcur[...].astype(BF16)

    w1_copy(0, 0, (2 * n_steps) % SLOTS).wait()
    w2_copy(0, n_steps % 2).wait()
    ow1[...] = wb1[(2 * n_steps) % SLOTS].astype(BF16)
    ow2[...] = wb2[n_steps % 2].astype(BF16)
    send_e(0)

    def h_in(c, carry):
        @pl.when(c != chip)
        def _():
            h_arrival(c).wait_recv()

        return carry

    def e_in(c, carry):
        @pl.when(c != chip)
        def _():
            e_arrival(c).wait_recv()

        return carry

    lax.fori_loop(0, chips, h_in, 0)
    h_swap.start()
    lax.fori_loop(0, chips, e_in, 0)
    e_swap.start()

    def place(n, rx, ry, sz, twin):
        sx = 1 - cx if rx else cx
        sy = 1 - cy if ry else cy
        inner, far = (sx, ry) if n % 2 == 0 else (sy, rx)
        at = 4 * chips_z + 4 * sz + 2 * (n % 2) + twin if far else 4 * sz + 2 * (n % 2) + twin
        return outs[at].at[inner, n // 2]

    def source(rx, ry, sz):
        sx = 1 - cx if rx else cx
        sy = 1 - cy if ry else cy
        return sz * 4 + sy * 2 + sx

    hops = (chip + 1 - 2 * cx, chip + 2 - 4 * cy, chip + 4, chip - 4)

    def hop_copy(kind, n, rx, ry, sz, mine, part=None):
        src = source(rx, ry, sz)
        there = (n, 1 - rx if kind == 0 else rx, 1 - ry if kind == 1 else ry, sz, 0)
        tx, ty = there[1], there[2]
        inner = (1 - cx if rx else cx) if n % 2 == 0 else (1 - cy if ry else cy)
        far = ty if n % 2 == 0 else tx
        at = 4 * chips_z + 4 * sz + 2 * (n % 2) if far else 4 * sz + 2 * (n % 2)
        src_ref, dst_ref = own.at[n] if mine else place(n, rx, ry, sz, 0), outs[at].at[inner, n // 2]
        if part is not None:
            src_ref, dst_ref = src_ref.at[part], dst_ref.at[part]
        return pltpu.make_async_remote_copy(
            src_ref=src_ref, dst_ref=dst_ref, send_sem=sp_send.at[n, kind, src], recv_sem=sp_recv.at[n, src],
            device_id=(2 * hops[kind] + core,), device_id_type=MESH)

    def arrival(n, rx, ry, sz):
        return pltpu.make_async_remote_copy(
            src_ref=own.at[n], dst_ref=place(n, rx, ry, sz, 0), send_sem=sp_send.at[n, 0, source(rx, ry, sz)],
            recv_sem=sp_recv.at[n, source(rx, ry, sz)], device_id=(me,), device_id_type=MESH)

    def twin_copy(n, rx, ry, sz, mine):
        src = source(rx, ry, sz)
        return pltpu.make_async_remote_copy(
            src_ref=own.at[n] if mine else place(n, rx, ry, sz, 0), dst_ref=place(n, rx, ry, sz, 1),
            send_sem=tw_send.at[n, src], recv_sem=tw_recv.at[n, src], device_id=(partner,), device_id_type=MESH)

    def at_z(fn):
        for z in range(chips_z):
            pl.when(cz == z)(functools.partial(fn, z))

    def split(code):
        return code // 10000, (code // 1000 % 10, code // 100 % 10, code // 10 % 10, code % 10)

    def act(z, code):
        kind, block = split(code)
        mine = block[1:] == (0, 0, z)
        if kind:
            hop_copy(kind - 1, *block, mine).start()
        else:
            arrival(*block).wait_recv()
            twin_copy(*block, False).start()

    group = 4
    half_groups = chips // group

    def row_groups(body, wait=False):
        def step(gi, carry):
            if wait:
                @pl.when(gi == half_groups)
                def _():
                    h_swap.wait_recv()
                    e_swap.wait_recv()

            half = (core + gi // half_groups) % 2
            base = half * chips + (gi % half_groups) * group
            body(base, rh[pl.ds(base, group)].reshape(group * rows, d), re[pl.ds(base, group)].reshape(group * rows, d))
            return carry

        lax.fori_loop(0, 2 * half_groups, step, 0)

    def add_in(base, s):
        for b in range(group):
            acc1[...] += mm(rh[base + b], s[b * rows:(b + 1) * rows], TN).astype(BF16).astype(F32)

    def add_out(base, a):
        for b in range(group):
            acc2[...] += mm(a[b * rows:(b + 1) * rows], re[base + b], TN).astype(BF16).astype(F32)

    def store_in(n):
        for cb in range(piece // 128):
            own[n, 0, cb * d:(cb + 1) * d, :] = acc1[:, cb * 128:(cb + 1) * 128].astype(BF16)

    def store_out(n):
        for lb in range(d // 128):
            own[n, 1, lb * piece:(lb + 1) * piece, :] = acc2[:, lb * 128:(lb + 1) * 128].astype(BF16)

    def send_part(part):
        def start(z):
            for code in RELAYS[z][0]:
                kind, block = split(code)
                hop_copy(kind - 1, *block, True, part).start()

        at_z(start)

    acc1[...] = jnp.zeros_like(acc1)
    acc2[...] = jnp.zeros_like(acc2)

    def first_out(base, hg, eg):
        a, slope = gelu_grad(mm(hg, ow1[:, :piece]))
        z_all[pl.ds(base, group), :, :piece] = slope.reshape(group, rows, piece)
        add_out(base, a.astype(BF16))

    def first_in(base, hg, eg):
        q = mm(eg, ow2[:piece, :], NT)
        add_in(base, (z_all[pl.ds(base, group), :, :piece].reshape(group * rows, piece) * q).astype(BF16))

    row_groups(first_out, wait=True)
    store_out(0)
    send_part(1)
    row_groups(first_in)
    store_in(0)
    send_part(0)

    def start_rest(n):
        def start(z):
            for code in RELAYS[z][n] if n else ():
                act(z, code)
            twin_copy(n, 0, 0, z, True).start()
            pltpu.make_async_copy(own.at[n], place(n, 0, 0, z, 0), own_sem.at[n]).start()

        at_z(start)

    start_rest(0)
    for n in range(1, QUARTERS):
        cols = slice(n * piece, (n + 1) * piece)
        acc1[...] = jnp.zeros_like(acc1)
        acc2[...] = jnp.zeros_like(acc2)

        def both(base, hg, eg, cols=cols):
            a, slope = gelu_grad(mm(hg, ow1[:, cols]))
            q = mm(eg, ow2[cols, :], NT)
            a = a.astype(BF16)
            s = (slope * q).astype(BF16)
            for b in range(group):
                own_rows = slice(b * rows, (b + 1) * rows)
                acc1[...] += mm(rh[base + b], s[own_rows], TN).astype(BF16).astype(F32)
                acc2[...] += mm(a[own_rows], re[base + b], TN).astype(BF16).astype(F32)

        row_groups(both)
        store_in(n)
        store_out(n)
        start_rest(n)

    def relay(z):
        for code in RELAYS[z][QUARTERS]:
            act(z, code)

    at_z(relay)

    def sent(l, carry):
        @pl.when(l != chip)
        def _():
            h_copy(l).wait_send()
            e_copy(l).wait_send()

        return carry

    lax.fori_loop(0, layers, sent, 0)
    h_swap.wait_send()
    e_swap.wait_send()
    for step in range(n_steps - RING, n_steps):
        pass_copy(step).wait_send()

    def drain(z):
        for n in range(QUARTERS):
            twin_copy(n, 0, 0, z, True).wait()
            pltpu.make_async_copy(own.at[n], place(n, 0, 0, z, 0), own_sem.at[n]).wait()
        for code in sum(RELAYS[z], ()):
            kind, block = split(code)
            if kind:
                hop_copy(kind - 1, *block, block[1:] == (0, 0, z)).wait_send()
            else:
                twin_copy(*block, False).wait()

    at_z(drain)


def local_grads(w_in, w_out, x, y, n_dev):
    layers, d, hid = w_in.shape
    rows = x.shape[0]
    hc = hid // 2
    piece = hc // QUARTERS
    part_rows = piece * d // 128
    dims = (n_dev, layers, rows, d, hid)
    n_out = n_dev // 2 + 4 * FIRST
    flops = 2 * rows * d * hid * layers * 4 + 2 * rows * n_dev * d * hc * 4
    return pl.pallas_call(
        functools.partial(grads_kernel, dims),
        out_shape=[jax.ShapeDtypeStruct((2, QUARTERS // 2, 2, part_rows, 128), BF16)] * n_out,
        in_specs=[pl.BlockSpec(memory_space=pl.ANY)] * 4,
        out_specs=[pl.BlockSpec(memory_space=pl.ANY)] * n_out,
        scratch_shapes=[
            pltpu.VMEM((rows, d), BF16),
            pltpu.VMEM((rows, d), BF16),
            pltpu.SemaphoreType.DMA((2,)),
            pltpu.VMEM((SLOTS, d, hc), F32),
            pltpu.VMEM((2, hc, d), F32),
            pltpu.VMEM((RING, hc, d), BF16),
            pltpu.VMEM((RING, hc, d), BF16),
            pltpu.VMEM((2 * CACHED, d, hc), BF16),
            pltpu.VMEM((2 * CACHED, hc, d), BF16),
            pltpu.VMEM((2 * layers, rows, hc), F32),
            pltpu.VMEM((layers, rows, d), BF16),
            pltpu.VMEM((layers, rows, d), BF16),
            pltpu.VMEM((rows, d), F32),
            pltpu.VMEM((n_dev, rows, d), BF16),
            pltpu.VMEM((n_dev, rows, d), BF16),
            pltpu.VMEM((d, hc), BF16),
            pltpu.VMEM((hc, d), BF16),
            pltpu.VMEM((d, piece), F32),
            pltpu.VMEM((piece, d), F32),
            pltpu.VMEM((QUARTERS, 2, part_rows, 128), BF16),
            pltpu.SemaphoreType.DMA((SLOTS,)),
            pltpu.SemaphoreType.DMA((2,)),
            pltpu.SemaphoreType.DMA((RING,)),
            pltpu.SemaphoreType.DMA((RING,)),
            pltpu.SemaphoreType.REGULAR((RING,)),
            pltpu.SemaphoreType.DMA((layers,)),
            pltpu.SemaphoreType.DMA((layers,)),
            pltpu.SemaphoreType.DMA((layers,)),
            pltpu.SemaphoreType.DMA((layers,)),
            pltpu.SemaphoreType.DMA((2,)),
            pltpu.SemaphoreType.DMA((2,)),
            pltpu.SemaphoreType.DMA((QUARTERS, 4, n_dev // 2)),
            pltpu.SemaphoreType.DMA((QUARTERS, n_dev // 2)),
            pltpu.SemaphoreType.DMA((QUARTERS, n_dev // 2)),
            pltpu.SemaphoreType.DMA((QUARTERS, n_dev // 2)),
            pltpu.SemaphoreType.DMA((QUARTERS,)),
        ],
        compiler_params=pltpu.CompilerParams(collective_id=0, has_side_effects=True, vmem_limit_bytes=VMEM_LIMIT),
        cost_estimate=pl.CostEstimate(flops=flops, bytes_accessed=4 * w_in.size * 4, transcendentals=0),
        name="local_grads",
    )(w_in, w_out, x, y)


def update_kernel(dims, group, last, *refs):
    layers, _, d, piece = dims
    step_size = LR_SCALE / layers
    chunk = 2 * piece
    steps = 16
    w1, m1, w2, m2, h_hbm = refs[:5]
    sums = refs[5:13]
    refs = refs[13:]
    if group:
        refs = refs[4:]
    if last:
        y_hbm, refs = refs[0], refs[1:]
    w1o, w2o, m1o, m2o, h_done = refs[:5]
    if last:
        loss_ref = refs[5]
    bw1, bm1, bw2, bm2, gbuf, in_sem, out_sem, gsem, nb1, nb2, hb_ref, y_ref, h_out, h_sem = refs[-14:]
    slots = bw1.shape[0]

    me = lax.axis_index("data")
    chip, core = me // 2, me % 2
    cx, cy = chip % 2, (chip // 2) % 2

    def tile1(ref, t):
        return ref.at[4 * group + t // 4, :, pl.ds(pl.multiple_of((t % 4) * chunk, 128), chunk)]

    def tile2(ref, t):
        return ref.at[4 * group + t // 4, pl.ds(pl.multiple_of((t % 4) * chunk, 8), chunk), :]

    def reads(t, slot):
        return [pltpu.make_async_copy(src, buf.at[slot], in_sem.at[i, slot]) for i, (src, buf) in enumerate(
            ((tile1(w1, t), bw1), (tile1(m1, t), bm1), (tile2(w2, t), bw2), (tile2(m2, t), bm2)))]

    def writes(t, slot):
        return [pltpu.make_async_copy(buf.at[slot], dst, out_sem.at[i, slot]) for i, (dst, buf) in enumerate(
            ((tile1(w1o, t), bw1), (tile1(m1o, t), bm1), (tile2(w2o, t), bw2), (tile2(m2o, t), bm2)))]

    def fetch(t, slot):
        for copy in reads(t, slot):
            copy.start()
        layer, part = t // 4, t % 4
        sx, sy, half, q = layer % 2, layer // 2, part // 2, part % 2
        for par, inner, far in ((0, sx, sy != cy), (1, sy, sx != cx)):
            for is_far in (0, 1):
                for twin in (0, 1):
                    hit = jnp.logical_and(far == bool(is_far), (half != core) == bool(twin))

                    @pl.when(hit)
                    def _(par=par, inner=inner, is_far=is_far, twin=twin):
                        pltpu.make_async_copy(sums[4 * is_far + 2 * par + twin].at[inner, q], gbuf.at[slot, par], gsem.at[par, slot]).start()

    takes = [pltpu.make_async_copy(h_hbm, h_out if group else hb_ref, h_sem.at[0])]
    if last:
        takes.append(pltpu.make_async_copy(y_hbm, y_ref, h_sem.at[1]))
    fetch(0, 0)
    for copy in takes:
        copy.start()
    for t in range(1, AHEAD):
        fetch(t, t)
    for copy in takes:
        copy.wait()
    if not group:
        h_out[...] = hb_ref[...].astype(F32)

    def body(t, carry):
        slot = t % slots

        @pl.when(t % 4 == 0)
        def _():
            hb_ref[...] = h_out[...].astype(BF16)

        for copy in reads(t, slot):
            copy.wait()
        done = writes(t, slot)
        for par in range(2):
            pltpu.make_async_copy(sums[0].at[0, 0], gbuf.at[slot, par], gsem.at[par, slot]).wait()
            for cb in range(piece // 128):
                cols = slice(par * piece + cb * 128, par * piece + (cb + 1) * 128)
                mn = MOMENTUM * bm1[slot, :, cols] + gbuf[slot, par, 0, cb * d:(cb + 1) * d, :].astype(F32)
                wn = bw1[slot, :, cols] - step_size * mn
                bm1[slot, :, cols] = mn
                bw1[slot, :, cols] = wn
                nb1[:, cols] = wn.astype(BF16)
        for copy in done[:2]:
            copy.start()
        for par in range(2):
            hid_rows = slice(par * piece, (par + 1) * piece)
            for lb in range(d // 128):
                cols = slice(lb * 128, (lb + 1) * 128)
                mn = MOMENTUM * bm2[slot, hid_rows, cols] + gbuf[slot, par, 1, lb * piece:(lb + 1) * piece, :].astype(F32)
                wn = bw2[slot, hid_rows, cols] - step_size * mn
                bm2[slot, hid_rows, cols] = mn
                bw2[slot, hid_rows, cols] = wn
                nb2[hid_rows, cols] = wn.astype(BF16)
        for copy in done[2:]:
            copy.start()

        @pl.when(t + AHEAD < steps)
        def _():
            nslot = (t + AHEAD) % slots

            @pl.when(t + AHEAD >= slots)
            def _():
                for copy in writes(t + AHEAD - slots, nslot):
                    copy.wait()

            fetch(t + AHEAD, nslot)

        z = mm(hb_ref[...], nb1[...])
        h_out[...] += mm(gelu(z).astype(BF16), nb2[...])
        return carry

    lax.fori_loop(0, steps, body, 0)
    give = pltpu.make_async_copy(h_out, h_done, h_sem.at[0])
    give.start()
    if last:
        diff = h_out[...] - y_ref[...].astype(F32)
        loss_ref[...] = jnp.sum(diff * diff, axis=-1) / (2 * d)
    for t in range(steps - slots, steps):
        for copy in writes(t, t % slots):
            copy.wait()
    give.wait()


def update(group, w_in, m_in, w_out, m_out, h, sums, prev, y):
    layers, d, hid = w_in.shape
    rows = h.shape[0]
    piece = hid // 2 // QUARTERS
    chunk = 2 * piece
    last = group == layers // 4 - 1
    whole = pl.BlockSpec(memory_space=pltpu.VMEM)
    any_spec = pl.BlockSpec(memory_space=pl.ANY)
    args = [w_in, m_in, w_out, m_out, h, *sums, *prev] + ([y] if last else [])
    in_specs = [any_spec] * len(args)
    out_specs = [any_spec] * 5
    out_shape = [jax.ShapeDtypeStruct(a.shape, F32) for a in (w_in, w_out, m_in, m_out, h)]
    if last:
        out_specs.append(whole)
        out_shape.append(jax.ShapeDtypeStruct((rows,), F32))
    n_el = 2 * w_in.size // 4
    slots = 7
    return pl.pallas_call(
        functools.partial(update_kernel, (layers, rows, d, piece), group, last),
        in_specs=in_specs,
        out_specs=out_specs,
        out_shape=out_shape,
        scratch_shapes=[
            pltpu.VMEM((slots, d, chunk), F32),
            pltpu.VMEM((slots, d, chunk), F32),
            pltpu.VMEM((slots, chunk, d), F32),
            pltpu.VMEM((slots, chunk, d), F32),
            pltpu.VMEM((slots, 2, *sums[0].shape[2:]), BF16),
            pltpu.SemaphoreType.DMA((4, slots)),
            pltpu.SemaphoreType.DMA((4, slots)),
            pltpu.SemaphoreType.DMA((2, slots)),
            pltpu.VMEM((d, chunk), BF16),
            pltpu.VMEM((chunk, d), BF16),
            pltpu.VMEM((rows, d), BF16),
            pltpu.VMEM((rows, d), BF16),
            pltpu.VMEM((rows, d), F32),
            pltpu.SemaphoreType.DMA((2,)),
        ],
        input_output_aliases={13 + i: i for i in range(len(prev))},
        compiler_params=pltpu.CompilerParams(vmem_limit_bytes=VMEM_LIMIT),
        cost_estimate=pl.CostEstimate(flops=5 * 10**10, bytes_accessed=18 * n_el, transcendentals=0),
    )(*args)


def solution(mesh):
    n_dev = mesh.shape["data"]
    rows_spec = P("data", None)
    swap = {axis: [(i, i ^ bit) for i in range(n_dev)] for axis, bit in (("core", 1), ("x", 2), ("y", 4))}

    def send(array, axis):
        return lax.ppermute(array, "data", swap[axis])

    def local_steps(w_in, w_out, mom_in, mom_out, x_first, y_first, x_second, y_second):
        groups = w_in.shape[0] // 4
        sums = local_grads(w_in, w_out, x_first, y_first, n_dev)
        near = [list(sums[4 * g:4 * g + 4]) for g in range(groups)]
        far = [list(sums[4 * (groups + g):4 * (groups + g) + 4]) for g in range(FIRST)]
        for g in range(FIRST, groups):
            from_y = send(near[g][0], "y")
            from_x = send(near[g][2], "x")
            far.append([from_y, send(from_y, "core"), from_x, send(from_x, "core")])
        prev, h = [], x_second
        for g in range(groups):
            outs = update(g, w_in, mom_in, w_out, mom_out, h, near[g] + far[g], prev, y_second)
            prev, h = list(outs[:4]), outs[4]
        w_in_new, w_out_new, mom_in_new, mom_out_new = prev
        return w_in_new, w_out_new, mom_in_new, mom_out_new, outs[5], h

    return jax.shard_map(
        local_steps, mesh=mesh,
        in_specs=(P(), P(), P(), P(), rows_spec, rows_spec, rows_spec, rows_spec),
        out_specs=(P(), P(), P(), P(), P("data"), rows_spec), check_vma=False)
```

```python
import functools

import jax
import jax.numpy as jnp
from jax import lax
from jax.experimental import pallas as pl
from jax.experimental.pallas import tpu as pltpu
from jax.sharding import PartitionSpec as P


LR_SCALE = 1.0
MOMENTUM = 0.9
F32 = jnp.float32
BF16 = jnp.bfloat16
MESH = pl.DeviceIdType.MESH
GELU_C = 0.7978845608028654
GELU_K = 0.044715
SLOTS = 4
RING = 3
QUARTERS = 4
AHEAD = 4
CACHED = 6
FIRST = 1
RELAYS = (
    (
        (30000, 10000, 20000),
        (31000, 11000, 21000),
        (100, 10, 1, 10001, 20100, 32000),
        (),
        (33000, 12000, 1100, 1010, 1001, 21001, 22000, 101, 110, 2, 10002, 13000, 2100, 1011, 1002, 21002, 23000, 102,
         2010, 3, 10003, 11010, 3100, 1012, 1003, 21003, 22100, 103, 3010, 2003, 12003, 13010, 1110, 1013, 3003, 23003,
         2103, 2110, 2002, 12002, 3110, 3013, 3002, 23002, 2102, 2001, 12001, 3012, 3001, 23001, 2101, 3011),
    ),
    (
        (30001, 40001, 10001),
        (21001, 31001, 41001),
        (0, 101, 2, 10000, 20000, 30000, 40002, 10002),
        (),
        (1011, 1000, 1002, 21000, 31000, 41002, 11000, 100, 21002, 10, 2000, 3, 32000, 40003, 10003, 102, 1010, 3000,
         1003, 21003, 33000, 41003, 1100, 20100, 32001, 1012, 2003, 12003, 42003, 12000, 103, 33001, 1013, 3003, 23003,
         43003, 11010, 2103, 22000, 110, 2002, 42002, 13000, 2100, 23000, 3013, 3002, 43002, 12002, 1110, 22100, 42001,
         2010, 3100, 23002, 43001, 3010, 13010, 12001, 2102, 23001, 2110, 3110, 3012, 2101, 3011),
    ),
    (
        (30002, 40002, 10002),
        (21002, 31002, 41002),
        (1, 102, 3, 10001, 30001, 40003, 10003),
        (),
        (23002, 1012, 1001, 1003, 31001, 41003, 21001, 101, 0, 2003, 10000, 30000, 42003, 20000, 3012, 103, 1000, 3003,
         11000, 31000, 43003, 21000, 1011, 100, 42002, 2000, 12000, 32000, 20100, 10, 12003, 1100, 43002, 3000, 33000,
         22000, 1010, 13000, 2100, 2001, 32001, 23000, 110, 11010, 2103, 3001, 33001, 22100, 2010, 12001, 3100, 32002,
         21003, 3010, 13010, 1110, 33002, 23003, 2110, 12002, 2101, 23001, 1013, 3110, 3013, 2102, 3011),
    ),
    (
        (40003, 10003),
        (21003, 41003),
        (2, 103, 10002, 42003, 12003),
        (),
        (23003, 43003, 1013, 1002, 21002, 102, 1, 10001, 3013, 2103, 1001, 21001, 1012, 101, 0, 10000, 20000, 1011,
         1000, 21000, 11000, 100, 10, 20100, 2000, 12000, 22000, 1100, 1010, 11010, 3000, 13000, 23000, 2100, 110,
         2001, 22100, 12001, 1110, 2010, 3001, 23001, 3100, 3010, 13010, 2002, 12002, 2110, 2101, 3002, 23002, 3110,
         3011, 3012, 2102),
    ),
)
VMEM_LIMIT = 67043328

NN = (((1,), (0,)), ((), ()))
NT = (((1,), (1,)), ((), ()))
TN = (((0,), (0,)), ((), ()))


def mm(a, b, dims=NN):
    return lax.dot_general(a, b, dims, preferred_element_type=F32)


def gelu(z):
    t = jnp.tanh(GELU_C * (z + GELU_K * (z * z * z)))
    return z * (0.5 * (1.0 + t))


def gelu_grad(z):
    zz = z * z
    t = jnp.tanh(GELU_C * (z + GELU_K * (zz * z)))
    cdf = 0.5 * (1.0 + t)
    slope = cdf + (0.5 * z) * (1.0 - t * t) * (GELU_C * (1.0 + (3.0 * GELU_K) * zz))
    return z * cdf, slope


def grads_kernel(dims, w1_hbm, w2_hbm, x_hbm, y_hbm, *rest):
    n_dev, layers, rows, d, hid = dims
    chips = n_dev // 2
    hc = hid // 2
    piece = hc // QUARTERS
    chips_z = chips // 4
    n_out = 4 * chips_z + 4 * FIRST
    outs, rest = rest[:n_out], rest[n_out:]
    (x_ref, y_ref, xy_sem, wb1, wb2, own2, far2, cw1, cw2, z_all, hb, eb, hcur, rh, re, ow1, ow2, acc1, acc2, own,
     w1_sem, w2_sem, x_send, x_recv, free_sem, hs_sem, hr_sem, es_sem, er_sem, px_send, px_recv,
     sp_send, sp_recv, tw_send, tw_recv, own_sem) = rest

    me = lax.axis_index("data")
    chip = me // 2
    core = me % 2
    partner = chip * 2 + (1 - core)

    cx, cy, cz = chip % 2, (chip // 2) % 2, chip // 4

    def greet(c, carry):
        @pl.when(c != chip)
        def _():
            pl.semaphore_signal(barrier, inc=1, device_id=(2 * c + core,), device_id_type=MESH)

        return carry

    barrier = pltpu.get_barrier_semaphore()
    lax.fori_loop(0, chips, greet, 0)
    pl.semaphore_signal(barrier, inc=1, device_id=(partner,), device_id_type=MESH)

    n_fwd, n_bwd = layers, layers - 1 - CACHED
    top = layers - 1 - CACHED
    n_steps = n_fwd + n_bwd

    def w1_copy(l, j, slot):
        return pltpu.make_async_copy(w1_hbm.at[l, :, pl.ds(pl.multiple_of(j * hc, 128), hc)], wb1.at[slot], w1_sem.at[slot])

    def w2_copy(l, slot):
        return pltpu.make_async_copy(w2_hbm.at[l, pl.ds(pl.multiple_of(core * hc, 128), hc), :], wb2.at[slot], w2_sem.at[slot])

    def pass_copy(step):
        at = step % RING
        return pltpu.make_async_remote_copy(
            src_ref=own2.at[at], dst_ref=far2.at[at], send_sem=x_send.at[at], recv_sem=x_recv.at[at],
            device_id=(partner,), device_id_type=MESH)

    def take_in(step):
        own2[step % RING] = wb2[step % 2].astype(BF16)

    def chunk(m):
        return (core + m) % 2

    takes = [pltpu.make_async_copy(src, dst, xy_sem.at[i]) for i, (src, dst) in enumerate(((x_hbm, x_ref), (y_hbm, y_ref)))]
    for step in range(2):
        w2_copy(step, step).start()
        if step == 0:
            for copy in takes:
                copy.start()
        for m in range(2):
            w1_copy(step, chunk(m), 2 * step + m).start()
    pl.semaphore_wait(barrier, chips)
    for step in range(2):
        w2_copy(step, step).wait()
        take_in(step)
        pass_copy(step).start()
        w2_copy(step + 2, step).start()

    def h_copy(l):
        return pltpu.make_async_remote_copy(
            src_ref=hb.at[l], dst_ref=rh.at[core * chips + chip], send_sem=hs_sem.at[l], recv_sem=hr_sem.at[chip],
            device_id=(2 * l + core,), device_id_type=MESH)

    def e_copy(l):
        return pltpu.make_async_remote_copy(
            src_ref=eb.at[l], dst_ref=re.at[core * chips + chip], send_sem=es_sem.at[l], recv_sem=er_sem.at[chip],
            device_id=(2 * l + core,), device_id_type=MESH)

    def h_arrival(c):
        return pltpu.make_async_remote_copy(
            src_ref=hb.at[0], dst_ref=rh.at[core * chips + c], send_sem=hs_sem.at[0], recv_sem=hr_sem.at[c],
            device_id=(me,), device_id_type=MESH)

    def e_arrival(c):
        return pltpu.make_async_remote_copy(
            src_ref=eb.at[0], dst_ref=re.at[core * chips + c], send_sem=es_sem.at[0], recv_sem=er_sem.at[c],
            device_id=(me,), device_id_type=MESH)

    def send_h(l):
        @pl.when(l != chip)
        def _():
            h_copy(l).start()

        @pl.when(l == chip)
        def _():
            rh[core * chips + chip] = hb[l]

    def send_e(l):
        @pl.when(l != chip)
        def _():
            e_copy(l).start()

        @pl.when(l == chip)
        def _():
            re[core * chips + chip] = eb[l]

    for copy in takes:
        copy.wait()
    hcur[...] = x_ref[...].astype(F32)

    def ahead(step):
        @pl.when(step >= 1)
        def _():
            pass_copy(step - 1).wait_send()
            pl.semaphore_wait(free_sem.at[(step + 2) % RING], 1)

        w2_copy(0, step % 2).wait()
        take_in(step + 2)

    def release(step):
        @pl.when(step <= n_steps - 1 - RING)
        def _():
            pl.semaphore_signal(free_sem.at[step % RING], inc=1, device_id=(partner,), device_id_type=MESH)

    def forward(step, carry):
        ahead(step)

        @pl.when(step + 4 < n_fwd)
        def _():
            w2_copy(step + 4, step % 2).start()

        @pl.when(step + 4 >= n_fwd)
        def _():
            w2_copy(top - (step + 4 - n_fwd), step % 2).start()

        hb[step] = hcur[...].astype(BF16)
        for m in range(2):
            j, slot = chunk(m), (2 * step + m) % SLOTS
            w1_copy(0, 0, slot).wait()
            if m == 1:
                pass_copy(step).wait_recv()
            w2 = own2 if m == 0 else far2
            z = mm(hb[step], wb1[slot].astype(BF16))
            z_all[2 * step + j] = z
            hcur[...] += mm(gelu(z).astype(BF16), w2[step % RING])
            if m == 0:
                pass_copy(step + 2).start()

            @pl.when(step >= layers - CACHED)
            def _(m=m, j=j, slot=slot, w2=w2):
                kept = 2 * (step - (layers - CACHED)) + j
                cw1[kept] = wb1[slot].astype(BF16)
                cw2[kept] = w2[step % RING]

            @pl.when(step + 2 < n_fwd)
            def _(j=j, slot=slot):
                w1_copy(step + 2, j, slot).start()

            @pl.when(step + 2 >= n_fwd)
            def _(j=j, slot=slot):
                w1_copy(top - (step + 2 - n_fwd), j, slot).start()
        release(step)
        send_h(step)
        return carry

    lax.fori_loop(0, n_fwd, forward, 0)

    scale = 1.0 / (rows * n_dev * d)
    hcur[...] = (hcur[...] - y_ref[...].astype(F32)) * scale

    h_swap = pltpu.make_async_remote_copy(
        src_ref=rh.at[pl.ds(core * chips, chips)], dst_ref=rh.at[pl.ds(core * chips, chips)],
        send_sem=px_send.at[0], recv_sem=px_recv.at[0], device_id=(partner,), device_id_type=MESH)
    e_swap = pltpu.make_async_remote_copy(
        src_ref=re.at[pl.ds(core * chips, chips)], dst_ref=re.at[pl.ds(core * chips, chips)],
        send_sem=px_send.at[1], recv_sem=px_recv.at[1], device_id=(partner,), device_id_type=MESH)

    def error_step(l, j, w1, w2):
        q = mm(eb[l], w2, NT)
        slope = gelu_grad(z_all[2 * l + j])[1]
        hcur[...] += mm((slope * q).astype(BF16), w1, NT)

    def backward_cached(i, carry):
        l = layers - 1 - i
        eb[l] = hcur[...].astype(BF16)
        for j in range(2):
            kept = 2 * (l - (layers - CACHED)) + j
            error_step(l, j, cw1[kept], cw2[kept])
        send_e(l)
        return carry

    def backward(i, carry):
        l, step = top - i, n_fwd + i

        @pl.when(step + 2 < n_steps)
        def _():
            ahead(step)

        @pl.when(step + 4 < n_steps)
        def _():
            w2_copy(l - 4, step % 2).start()

        @pl.when(step + 4 == n_steps)
        def _():
            w2_copy(chip, step % 2).start()

        eb[l] = hcur[...].astype(BF16)
        for m in range(2):
            j, slot = chunk(m), (2 * step + m) % SLOTS
            w1_copy(0, 0, slot).wait()
            if m == 1:
                pass_copy(step).wait_recv()
            error_step(l, j, wb1[slot].astype(BF16), (own2 if m == 0 else far2)[step % RING])

            @pl.when(step + 2 < n_steps)
            def _(m=m, j=j, slot=slot):
                if m == 0:
                    pass_copy(step + 2).start()
                w1_copy(l - 2, j, slot).start()

            if m == 0:
                @pl.when(step + 2 == n_steps)
                def _(j=j, slot=slot):
                    w1_copy(chip, j, slot).start()
        release(step)
        send_e(l)
        return carry

    lax.fori_loop(0, CACHED, backward_cached, 0)
    lax.fori_loop(0, n_bwd, backward, 0)
    eb[0] = hcur[...].astype(BF16)

    w1_copy(0, 0, (2 * n_steps) % SLOTS).wait()
    w2_copy(0, n_steps % 2).wait()
    ow1[...] = wb1[(2 * n_steps) % SLOTS].astype(BF16)
    ow2[...] = wb2[n_steps % 2].astype(BF16)
    send_e(0)

    def h_in(c, carry):
        @pl.when(c != chip)
        def _():
            h_arrival(c).wait_recv()

        return carry

    def e_in(c, carry):
        @pl.when(c != chip)
        def _():
            e_arrival(c).wait_recv()

        return carry

    lax.fori_loop(0, chips, h_in, 0)
    h_swap.start()
    lax.fori_loop(0, chips, e_in, 0)
    e_swap.start()

    def place(n, rx, ry, sz, twin):
        sx = 1 - cx if rx else cx
        sy = 1 - cy if ry else cy
        inner, far = (sx, ry) if n % 2 == 0 else (sy, rx)
        at = 4 * chips_z + 4 * sz + 2 * (n % 2) + twin if far else 4 * sz + 2 * (n % 2) + twin
        return outs[at].at[inner, n // 2]

    def source(rx, ry, sz):
        sx = 1 - cx if rx else cx
        sy = 1 - cy if ry else cy
        return sz * 4 + sy * 2 + sx

    hops = (chip + 1 - 2 * cx, chip + 2 - 4 * cy, chip + 4, chip - 4)

    def hop_copy(kind, n, rx, ry, sz, mine, part=None):
        src = source(rx, ry, sz)
        there = (n, 1 - rx if kind == 0 else rx, 1 - ry if kind == 1 else ry, sz, 0)
        tx, ty = there[1], there[2]
        inner = (1 - cx if rx else cx) if n % 2 == 0 else (1 - cy if ry else cy)
        far = ty if n % 2 == 0 else tx
        at = 4 * chips_z + 4 * sz + 2 * (n % 2) if far else 4 * sz + 2 * (n % 2)
        src_ref, dst_ref = own.at[n] if mine else place(n, rx, ry, sz, 0), outs[at].at[inner, n // 2]
        if part is not None:
            src_ref, dst_ref = src_ref.at[part], dst_ref.at[part]
        return pltpu.make_async_remote_copy(
            src_ref=src_ref, dst_ref=dst_ref, send_sem=sp_send.at[n, kind, src], recv_sem=sp_recv.at[n, src],
            device_id=(2 * hops[kind] + core,), device_id_type=MESH)

    def arrival(n, rx, ry, sz):
        return pltpu.make_async_remote_copy(
            src_ref=own.at[n], dst_ref=place(n, rx, ry, sz, 0), send_sem=sp_send.at[n, 0, source(rx, ry, sz)],
            recv_sem=sp_recv.at[n, source(rx, ry, sz)], device_id=(me,), device_id_type=MESH)

    def twin_copy(n, rx, ry, sz, mine):
        src = source(rx, ry, sz)
        return pltpu.make_async_remote_copy(
            src_ref=own.at[n] if mine else place(n, rx, ry, sz, 0), dst_ref=place(n, rx, ry, sz, 1),
            send_sem=tw_send.at[n, src], recv_sem=tw_recv.at[n, src], device_id=(partner,), device_id_type=MESH)

    def at_z(fn):
        for z in range(chips_z):
            pl.when(cz == z)(functools.partial(fn, z))

    def split(code):
        return code // 10000, (code // 1000 % 10, code // 100 % 10, code // 10 % 10, code % 10)

    def act(z, code):
        kind, block = split(code)
        mine = block[1:] == (0, 0, z)
        if kind:
            hop_copy(kind - 1, *block, mine).start()
        else:
            arrival(*block).wait_recv()
            twin_copy(*block, False).start()

    group = 4
    half_groups = chips // group

    def row_groups(body, wait=False):
        def step(gi, carry):
            if wait:
                @pl.when(gi == half_groups)
                def _():
                    h_swap.wait_recv()
                    e_swap.wait_recv()

            half = (core + gi // half_groups) % 2
            base = half * chips + (gi % half_groups) * group
            body(base, rh[pl.ds(base, group)].reshape(group * rows, d), re[pl.ds(base, group)].reshape(group * rows, d))
            return carry

        lax.fori_loop(0, 2 * half_groups, step, 0)

    def add_in(base, s):
        for b in range(group):
            acc1[...] += mm(rh[base + b], s[b * rows:(b + 1) * rows], TN).astype(BF16).astype(F32)

    def add_out(base, a):
        for b in range(group):
            acc2[...] += mm(a[b * rows:(b + 1) * rows], re[base + b], TN).astype(BF16).astype(F32)

    def store_in(n):
        for cb in range(piece // 128):
            own[n, 0, cb * d:(cb + 1) * d, :] = acc1[:, cb * 128:(cb + 1) * 128].astype(BF16)

    def store_out(n):
        for lb in range(d // 128):
            own[n, 1, lb * piece:(lb + 1) * piece, :] = acc2[:, lb * 128:(lb + 1) * 128].astype(BF16)

    def send_part(part):
        def start(z):
            for code in RELAYS[z][0]:
                kind, block = split(code)
                hop_copy(kind - 1, *block, True, part).start()

        at_z(start)

    acc1[...] = jnp.zeros_like(acc1)
    acc2[...] = jnp.zeros_like(acc2)

    def first_out(base, hg, eg):
        a, slope = gelu_grad(mm(hg, ow1[:, :piece]))
        z_all[pl.ds(base, group), :, :piece] = slope.reshape(group, rows, piece)
        add_out(base, a.astype(BF16))

    def first_in(base, hg, eg):
        q = mm(eg, ow2[:piece, :], NT)
        add_in(base, (z_all[pl.ds(base, group), :, :piece].reshape(group * rows, piece) * q).astype(BF16))

    row_groups(first_out, wait=True)
    store_out(0)
    send_part(1)
    row_groups(first_in)
    store_in(0)
    send_part(0)

    def start_rest(n):
        def start(z):
            for code in RELAYS[z][n] if n else ():
                act(z, code)
            twin_copy(n, 0, 0, z, True).start()
            pltpu.make_async_copy(own.at[n], place(n, 0, 0, z, 0), own_sem.at[n]).start()

        at_z(start)

    start_rest(0)
    for n in range(1, QUARTERS):
        cols = slice(n * piece, (n + 1) * piece)
        acc1[...] = jnp.zeros_like(acc1)
        acc2[...] = jnp.zeros_like(acc2)

        def both(base, hg, eg, cols=cols):
            a, slope = gelu_grad(mm(hg, ow1[:, cols]))
            q = mm(eg, ow2[cols, :], NT)
            a = a.astype(BF16)
            s = (slope * q).astype(BF16)
            for b in range(group):
                own_rows = slice(b * rows, (b + 1) * rows)
                acc1[...] += mm(rh[base + b], s[own_rows], TN).astype(BF16).astype(F32)
                acc2[...] += mm(a[own_rows], re[base + b], TN).astype(BF16).astype(F32)

        row_groups(both)
        store_in(n)
        store_out(n)
        start_rest(n)

    def relay(z):
        for code in RELAYS[z][QUARTERS]:
            act(z, code)

    at_z(relay)

    def sent(l, carry):
        @pl.when(l != chip)
        def _():
            h_copy(l).wait_send()
            e_copy(l).wait_send()

        return carry

    lax.fori_loop(0, layers, sent, 0)
    h_swap.wait_send()
    e_swap.wait_send()
    for step in range(n_steps - RING, n_steps):
        pass_copy(step).wait_send()

    def drain(z):
        for n in range(QUARTERS):
            twin_copy(n, 0, 0, z, True).wait()
            pltpu.make_async_copy(own.at[n], place(n, 0, 0, z, 0), own_sem.at[n]).wait()
        for code in sum(RELAYS[z], ()):
            kind, block = split(code)
            if kind:
                hop_copy(kind - 1, *block, block[1:] == (0, 0, z)).wait_send()
            else:
                twin_copy(*block, False).wait()

    at_z(drain)


def local_grads(w_in, w_out, x, y, n_dev):
    layers, d, hid = w_in.shape
    rows = x.shape[0]
    hc = hid // 2
    piece = hc // QUARTERS
    part_rows = piece * d // 128
    dims = (n_dev, layers, rows, d, hid)
    n_out = n_dev // 2 + 4 * FIRST
    flops = 2 * rows * d * hid * layers * 4 + 2 * rows * n_dev * d * hc * 4
    return pl.pallas_call(
        functools.partial(grads_kernel, dims),
        out_shape=[jax.ShapeDtypeStruct((2, QUARTERS // 2, 2, part_rows, 128), BF16)] * n_out,
        in_specs=[pl.BlockSpec(memory_space=pl.ANY)] * 4,
        out_specs=[pl.BlockSpec(memory_space=pl.ANY)] * n_out,
        scratch_shapes=[
            pltpu.VMEM((rows, d), BF16),
            pltpu.VMEM((rows, d), BF16),
            pltpu.SemaphoreType.DMA((2,)),
            pltpu.VMEM((SLOTS, d, hc), F32),
            pltpu.VMEM((2, hc, d), F32),
            pltpu.VMEM((RING, hc, d), BF16),
            pltpu.VMEM((RING, hc, d), BF16),
            pltpu.VMEM((2 * CACHED, d, hc), BF16),
            pltpu.VMEM((2 * CACHED, hc, d), BF16),
            pltpu.VMEM((2 * layers, rows, hc), F32),
            pltpu.VMEM((layers, rows, d), BF16),
            pltpu.VMEM((layers, rows, d), BF16),
            pltpu.VMEM((rows, d), F32),
            pltpu.VMEM((n_dev, rows, d), BF16),
            pltpu.VMEM((n_dev, rows, d), BF16),
            pltpu.VMEM((d, hc), BF16),
            pltpu.VMEM((hc, d), BF16),
            pltpu.VMEM((d, piece), F32),
            pltpu.VMEM((piece, d), F32),
            pltpu.VMEM((QUARTERS, 2, part_rows, 128), BF16),
            pltpu.SemaphoreType.DMA((SLOTS,)),
            pltpu.SemaphoreType.DMA((2,)),
            pltpu.SemaphoreType.DMA((RING,)),
            pltpu.SemaphoreType.DMA((RING,)),
            pltpu.SemaphoreType.REGULAR((RING,)),
            pltpu.SemaphoreType.DMA((layers,)),
            pltpu.SemaphoreType.DMA((layers,)),
            pltpu.SemaphoreType.DMA((layers,)),
            pltpu.SemaphoreType.DMA((layers,)),
            pltpu.SemaphoreType.DMA((2,)),
            pltpu.SemaphoreType.DMA((2,)),
            pltpu.SemaphoreType.DMA((QUARTERS, 4, n_dev // 2)),
            pltpu.SemaphoreType.DMA((QUARTERS, n_dev // 2)),
            pltpu.SemaphoreType.DMA((QUARTERS, n_dev // 2)),
            pltpu.SemaphoreType.DMA((QUARTERS, n_dev // 2)),
            pltpu.SemaphoreType.DMA((QUARTERS,)),
        ],
        compiler_params=pltpu.CompilerParams(collective_id=0, has_side_effects=True, vmem_limit_bytes=VMEM_LIMIT),
        cost_estimate=pl.CostEstimate(flops=flops, bytes_accessed=4 * w_in.size * 4, transcendentals=0),
        name="local_grads",
    )(w_in, w_out, x, y)


def update_kernel(dims, group, last, *refs):
    layers, _, d, piece = dims
    step_size = LR_SCALE / layers
    chunk = 2 * piece
    steps = 16
    w1, m1, w2, m2, h_in = refs[:5]
    sums = refs[5:13]
    refs = refs[13:]
    if group:
        refs = refs[4:]
    if last:
        y_ref, refs = refs[0], refs[1:]
    w1o, w2o, m1o, m2o, h_out = refs[:5]
    if last:
        loss_ref = refs[5]
    bw1, bm1, bw2, bm2, gbuf, in_sem, out_sem, gsem, nb1, nb2, hb_ref = refs[-11:]
    slots = bw1.shape[0]

    me = lax.axis_index("data")
    chip, core = me // 2, me % 2
    cx, cy = chip % 2, (chip // 2) % 2

    def tile1(ref, t):
        return ref.at[4 * group + t // 4, :, pl.ds(pl.multiple_of((t % 4) * chunk, 128), chunk)]

    def tile2(ref, t):
        return ref.at[4 * group + t // 4, pl.ds(pl.multiple_of((t % 4) * chunk, 8), chunk), :]

    def reads(t, slot):
        return [pltpu.make_async_copy(src, buf.at[slot], in_sem.at[i, slot]) for i, (src, buf) in enumerate(
            ((tile1(w1, t), bw1), (tile1(m1, t), bm1), (tile2(w2, t), bw2), (tile2(m2, t), bm2)))]

    def writes(t, slot):
        return [pltpu.make_async_copy(buf.at[slot], dst, out_sem.at[i, slot]) for i, (dst, buf) in enumerate(
            ((tile1(w1o, t), bw1), (tile1(m1o, t), bm1), (tile2(w2o, t), bw2), (tile2(m2o, t), bm2)))]

    def fetch(t, slot):
        for copy in reads(t, slot):
            copy.start()
        layer, part = t // 4, t % 4
        sx, sy, half, q = layer % 2, layer // 2, part // 2, part % 2
        for par, inner, far in ((0, sx, sy != cy), (1, sy, sx != cx)):
            for is_far in (0, 1):
                for twin in (0, 1):
                    hit = jnp.logical_and(far == bool(is_far), (half != core) == bool(twin))

                    @pl.when(hit)
                    def _(par=par, inner=inner, is_far=is_far, twin=twin):
                        pltpu.make_async_copy(sums[4 * is_far + 2 * par + twin].at[inner, q], gbuf.at[slot, par], gsem.at[par, slot]).start()

    for t in range(AHEAD):
        fetch(t, t)
    h_out[...] = h_in[...].astype(F32)

    def body(t, carry):
        slot = t % slots

        @pl.when(t % 4 == 0)
        def _():
            hb_ref[...] = h_out[...].astype(BF16)

        for copy in reads(t, slot):
            copy.wait()
        for par in range(2):
            pltpu.make_async_copy(sums[0].at[0, 0], gbuf.at[slot, par], gsem.at[par, slot]).wait()
            for cb in range(piece // 128):
                cols = slice(par * piece + cb * 128, par * piece + (cb + 1) * 128)
                mn = MOMENTUM * bm1[slot, :, cols] + gbuf[slot, par, 0, cb * d:(cb + 1) * d, :].astype(F32)
                wn = bw1[slot, :, cols] - step_size * mn
                bm1[slot, :, cols] = mn
                bw1[slot, :, cols] = wn
                nb1[:, cols] = wn.astype(BF16)
            hid_rows = slice(par * piece, (par + 1) * piece)
            for lb in range(d // 128):
                cols = slice(lb * 128, (lb + 1) * 128)
                mn = MOMENTUM * bm2[slot, hid_rows, cols] + gbuf[slot, par, 1, lb * piece:(lb + 1) * piece, :].astype(F32)
                wn = bw2[slot, hid_rows, cols] - step_size * mn
                bm2[slot, hid_rows, cols] = mn
                bw2[slot, hid_rows, cols] = wn
                nb2[hid_rows, cols] = wn.astype(BF16)
        for copy in writes(t, slot):
            copy.start()

        @pl.when(t + AHEAD < steps)
        def _():
            nslot = (t + AHEAD) % slots

            @pl.when(t + AHEAD >= slots)
            def _():
                for copy in writes(t + AHEAD - slots, nslot):
                    copy.wait()

            fetch(t + AHEAD, nslot)

        z = mm(hb_ref[...], nb1[...])
        h_out[...] += mm(gelu(z).astype(BF16), nb2[...])
        return carry

    lax.fori_loop(0, steps, body, 0)
    for t in range(steps - slots, steps):
        for copy in writes(t, t % slots):
            copy.wait()
    if last:
        diff = h_out[...] - y_ref[...].astype(F32)
        loss_ref[...] = jnp.sum(diff * diff, axis=-1) / (2 * d)


def update(group, w_in, m_in, w_out, m_out, h, sums, prev, y):
    layers, d, hid = w_in.shape
    rows = h.shape[0]
    piece = hid // 2 // QUARTERS
    chunk = 2 * piece
    last = group == layers // 4 - 1
    whole = pl.BlockSpec(memory_space=pltpu.VMEM)
    any_spec = pl.BlockSpec(memory_space=pl.ANY)
    args = [w_in, m_in, w_out, m_out, h, *sums, *prev] + ([y] if last else [])
    in_specs = [any_spec] * 4 + [whole] + [any_spec] * (8 + len(prev)) + ([whole] if last else [])
    out_specs = [any_spec] * 4 + [whole]
    out_shape = [jax.ShapeDtypeStruct(a.shape, F32) for a in (w_in, w_out, m_in, m_out, h)]
    if last:
        out_specs.append(whole)
        out_shape.append(jax.ShapeDtypeStruct((rows,), F32))
    n_el = 2 * w_in.size // 4
    slots = 7
    return pl.pallas_call(
        functools.partial(update_kernel, (layers, rows, d, piece), group, last),
        in_specs=in_specs,
        out_specs=out_specs,
        out_shape=out_shape,
        scratch_shapes=[
            pltpu.VMEM((slots, d, chunk), F32),
            pltpu.VMEM((slots, d, chunk), F32),
            pltpu.VMEM((slots, chunk, d), F32),
            pltpu.VMEM((slots, chunk, d), F32),
            pltpu.VMEM((slots, 2, *sums[0].shape[2:]), BF16),
            pltpu.SemaphoreType.DMA((4, slots)),
            pltpu.SemaphoreType.DMA((4, slots)),
            pltpu.SemaphoreType.DMA((2, slots)),
            pltpu.VMEM((d, chunk), BF16),
            pltpu.VMEM((chunk, d), BF16),
            pltpu.VMEM((rows, d), BF16),
        ],
        input_output_aliases={13 + i: i for i in range(len(prev))},
        compiler_params=pltpu.CompilerParams(vmem_limit_bytes=VMEM_LIMIT),
        cost_estimate=pl.CostEstimate(flops=5 * 10**10, bytes_accessed=18 * n_el, transcendentals=0),
    )(*args)


def solution(mesh):
    n_dev = mesh.shape["data"]
    rows_spec = P("data", None)
    swap = {axis: [(i, i ^ bit) for i in range(n_dev)] for axis, bit in (("core", 1), ("x", 2), ("y", 4))}

    def send(array, axis):
        return lax.ppermute(array, "data", swap[axis])

    def local_steps(w_in, w_out, mom_in, mom_out, x_first, y_first, x_second, y_second):
        groups = w_in.shape[0] // 4
        sums = local_grads(w_in, w_out, x_first, y_first, n_dev)
        near = [list(sums[4 * g:4 * g + 4]) for g in range(groups)]
        far = [list(sums[4 * (groups + g):4 * (groups + g) + 4]) for g in range(FIRST)]
        for g in range(FIRST, groups):
            from_y = send(near[g][0], "y")
            from_x = send(near[g][2], "x")
            far.append([from_y, send(from_y, "core"), from_x, send(from_x, "core")])
        prev, h = [], x_second
        for g in range(groups):
            outs = update(g, w_in, mom_in, w_out, mom_out, h, near[g] + far[g], prev, y_second)
            prev, h = list(outs[:4]), outs[4]
        w_in_new, w_out_new, mom_in_new, mom_out_new = prev
        return w_in_new, w_out_new, mom_in_new, mom_out_new, outs[5], h

    return jax.shard_map(
        local_steps, mesh=mesh,
        in_specs=(P(), P(), P(), P(), rows_spec, rows_spec, rows_spec, rows_spec),
        out_specs=(P(), P(), P(), P(), P("data"), rows_spec), check_vma=False)
```

```python
import functools

import jax
import jax.numpy as jnp
from jax import lax
from jax.experimental import pallas as pl
from jax.experimental.pallas import tpu as pltpu
from jax.sharding import PartitionSpec as P


LR_SCALE = 1.0
MOMENTUM = 0.9
F32 = jnp.float32
BF16 = jnp.bfloat16
MESH = pl.DeviceIdType.MESH
GELU_C = 0.7978845608028654
GELU_K = 0.044715
SLOTS = 4
RING = 3
QUARTERS = 4
AHEAD = 4
CACHED = 7
FIRST = 1
RELAYS = (
    (
        (30000, 10000, 20000),
        (31000, 11000, 21000),
        (100, 10, 1, 10001, 20100, 32000),
        (),
        (33000, 12000, 1100, 1010, 1001, 21001, 22000, 101, 110, 2, 10002, 13000, 2100, 1011, 1002, 21002, 23000, 102,
         2010, 3, 10003, 11010, 3100, 1012, 1003, 21003, 22100, 103, 3010, 2003, 12003, 13010, 1110, 1013, 3003, 23003,
         2103, 2110, 2002, 12002, 3110, 3013, 3002, 23002, 2102, 2001, 12001, 3012, 3001, 23001, 2101, 3011),
    ),
    (
        (30001, 40001, 10001),
        (21001, 31001, 41001),
        (0, 101, 2, 10000, 20000, 30000, 40002, 10002),
        (),
        (1011, 1000, 1002, 21000, 31000, 41002, 11000, 100, 21002, 10, 2000, 3, 32000, 40003, 10003, 102, 1010, 3000,
         1003, 21003, 33000, 41003, 1100, 20100, 32001, 1012, 2003, 12003, 42003, 12000, 103, 33001, 1013, 3003, 23003,
         43003, 11010, 2103, 22000, 110, 2002, 42002, 13000, 2100, 23000, 3013, 3002, 43002, 12002, 1110, 22100, 42001,
         2010, 3100, 23002, 43001, 3010, 13010, 12001, 2102, 23001, 2110, 3110, 3012, 2101, 3011),
    ),
    (
        (30002, 40002, 10002),
        (21002, 31002, 41002),
        (1, 102, 3, 10001, 30001, 40003, 10003),
        (),
        (23002, 1012, 1001, 1003, 31001, 41003, 21001, 101, 0, 2003, 10000, 30000, 42003, 20000, 3012, 103, 1000, 3003,
         11000, 31000, 43003, 21000, 1011, 100, 42002, 2000, 12000, 32000, 20100, 10, 12003, 1100, 43002, 3000, 33000,
         22000, 1010, 13000, 2100, 2001, 32001, 23000, 110, 11010, 2103, 3001, 33001, 22100, 2010, 12001, 3100, 32002,
         21003, 3010, 13010, 1110, 33002, 23003, 2110, 12002, 2101, 23001, 1013, 3110, 3013, 2102, 3011),
    ),
    (
        (40003, 10003),
        (21003, 41003),
        (2, 103, 10002, 42003, 12003),
        (),
        (23003, 43003, 1013, 1002, 21002, 102, 1, 10001, 3013, 2103, 1001, 21001, 1012, 101, 0, 10000, 20000, 1011,
         1000, 21000, 11000, 100, 10, 20100, 2000, 12000, 22000, 1100, 1010, 11010, 3000, 13000, 23000, 2100, 110,
         2001, 22100, 12001, 1110, 2010, 3001, 23001, 3100, 3010, 13010, 2002, 12002, 2110, 2101, 3002, 23002, 3110,
         3011, 3012, 2102),
    ),
)
VMEM_LIMIT = 67043328

NN = (((1,), (0,)), ((), ()))
NT = (((1,), (1,)), ((), ()))
TN = (((0,), (0,)), ((), ()))


def mm(a, b, dims=NN):
    return lax.dot_general(a, b, dims, preferred_element_type=F32)


def gelu(z):
    t = jnp.tanh(GELU_C * (z + GELU_K * (z * z * z)))
    return z * (0.5 * (1.0 + t))


def gelu_grad(z):
    zz = z * z
    t = jnp.tanh(GELU_C * (z + GELU_K * (zz * z)))
    cdf = 0.5 * (1.0 + t)
    slope = cdf + (0.5 * z) * (1.0 - t * t) * (GELU_C * (1.0 + (3.0 * GELU_K) * zz))
    return z * cdf, slope


def grads_kernel(dims, w1_hbm, w2_hbm, x_hbm, y_hbm, *rest):
    n_dev, layers, rows, d, hid = dims
    chips = n_dev // 2
    hc = hid // 2
    piece = hc // QUARTERS
    chips_z = chips // 4
    n_out = 4 * chips_z + 4 * FIRST
    outs, rest = rest[:n_out], rest[n_out:]
    (x_ref, y_ref, xy_sem, wb1, wb2, own2, far2, cw1, cw2, z_kept, hb, eb, hcur, rh, re, ow1, ow2, acc1, acc2, own,
     w1_sem, w2_sem, x_send, x_recv, free_sem, hs_sem, hr_sem, es_sem, er_sem, px_send, px_recv,
     sp_send, sp_recv, tw_send, tw_recv, own_sem) = rest

    me = lax.axis_index("data")
    chip = me // 2
    core = me % 2
    partner = chip * 2 + (1 - core)

    cx, cy, cz = chip % 2, (chip // 2) % 2, chip // 4

    def greet(c, carry):
        @pl.when(c != chip)
        def _():
            pl.semaphore_signal(barrier, inc=1, device_id=(2 * c + core,), device_id_type=MESH)

        return carry

    barrier = pltpu.get_barrier_semaphore()
    lax.fori_loop(0, chips, greet, 0)
    pl.semaphore_signal(barrier, inc=1, device_id=(partner,), device_id_type=MESH)

    n_fwd, n_bwd = layers, layers - 1 - CACHED
    top = layers - 1 - CACHED
    n_steps = n_fwd + n_bwd

    def w1_copy(l, j, slot):
        return pltpu.make_async_copy(w1_hbm.at[l, :, pl.ds(pl.multiple_of(j * hc, 128), hc)], wb1.at[slot], w1_sem.at[slot])

    def w2_copy(l, slot):
        return pltpu.make_async_copy(w2_hbm.at[l, pl.ds(pl.multiple_of(core * hc, 128), hc), :], wb2.at[slot], w2_sem.at[slot])

    def pass_copy(step):
        at = step % RING
        return pltpu.make_async_remote_copy(
            src_ref=own2.at[at], dst_ref=far2.at[at], send_sem=x_send.at[at], recv_sem=x_recv.at[at],
            device_id=(partner,), device_id_type=MESH)

    def take_in(step):
        own2[step % RING] = wb2[step % 2].astype(BF16)

    def chunk(m):
        return (core + m) % 2

    takes = [pltpu.make_async_copy(src, dst, xy_sem.at[i]) for i, (src, dst) in enumerate(((x_hbm, x_ref), (y_hbm, y_ref)))]
    for step in range(2):
        w2_copy(step, step).start()
        if step == 0:
            for copy in takes:
                copy.start()
        for m in range(2):
            w1_copy(step, chunk(m), 2 * step + m).start()
    pl.semaphore_wait(barrier, chips)
    for step in range(2):
        w2_copy(step, step).wait()
        take_in(step)
        pass_copy(step).start()
        w2_copy(step + 2, step).start()

    def h_copy(l):
        return pltpu.make_async_remote_copy(
            src_ref=hb.at[l], dst_ref=rh.at[core * chips + chip], send_sem=hs_sem.at[l], recv_sem=hr_sem.at[chip],
            device_id=(2 * l + core,), device_id_type=MESH)

    def e_copy(l):
        return pltpu.make_async_remote_copy(
            src_ref=eb.at[l], dst_ref=re.at[core * chips + chip], send_sem=es_sem.at[l], recv_sem=er_sem.at[chip],
            device_id=(2 * l + core,), device_id_type=MESH)

    def h_arrival(c):
        return pltpu.make_async_remote_copy(
            src_ref=hb.at[0], dst_ref=rh.at[core * chips + c], send_sem=hs_sem.at[0], recv_sem=hr_sem.at[c],
            device_id=(me,), device_id_type=MESH)

    def e_arrival(c):
        return pltpu.make_async_remote_copy(
            src_ref=eb.at[0], dst_ref=re.at[core * chips + c], send_sem=es_sem.at[0], recv_sem=er_sem.at[c],
            device_id=(me,), device_id_type=MESH)

    def send_h(l):
        @pl.when(l != chip)
        def _():
            h_copy(l).start()

        @pl.when(l == chip)
        def _():
            rh[core * chips + chip] = hb[l]

    def send_e(l):
        @pl.when(l != chip)
        def _():
            e_copy(l).start()

        @pl.when(l == chip)
        def _():
            re[core * chips + chip] = eb[l]

    for copy in takes:
        copy.wait()
    hcur[...] = x_ref[...].astype(F32)

    def ahead(step):
        @pl.when(step >= 1)
        def _():
            pass_copy(step - 1).wait_send()
            pl.semaphore_wait(free_sem.at[(step + 2) % RING], 1)

        w2_copy(0, step % 2).wait()
        take_in(step + 2)

    def release(step):
        @pl.when(step <= n_steps - 1 - RING)
        def _():
            pl.semaphore_signal(free_sem.at[step % RING], inc=1, device_id=(partner,), device_id_type=MESH)

    def forward(step, carry):
        ahead(step)

        @pl.when(step + 4 < n_fwd)
        def _():
            w2_copy(step + 4, step % 2).start()

        @pl.when(step + 4 >= n_fwd)
        def _():
            w2_copy(top - (step + 4 - n_fwd), step % 2).start()

        hb[step] = hcur[...].astype(BF16)
        for m in range(2):
            j, slot = chunk(m), (2 * step + m) % SLOTS
            w1_copy(0, 0, slot).wait()
            if m == 1:
                pass_copy(step).wait_recv()
            w2 = own2 if m == 0 else far2
            z = mm(hb[step], wb1[slot].astype(BF16))
            hcur[...] += mm(gelu(z).astype(BF16), w2[step % RING])
            if m == 0:
                pass_copy(step + 2).start()

            @pl.when(step >= layers - CACHED)
            def _(m=m, j=j, slot=slot, w2=w2, z=z):
                kept = 2 * (step - (layers - CACHED)) + j
                z_kept[kept] = z
                cw1[kept] = wb1[slot].astype(BF16)
                cw2[kept] = w2[step % RING]

            @pl.when(step + 2 < n_fwd)
            def _(j=j, slot=slot):
                w1_copy(step + 2, j, slot).start()

            @pl.when(step + 2 >= n_fwd)
            def _(j=j, slot=slot):
                w1_copy(top - (step + 2 - n_fwd), j, slot).start()
        release(step)
        send_h(step)
        return carry

    lax.fori_loop(0, n_fwd, forward, 0)

    scale = 1.0 / (rows * n_dev * d)
    hcur[...] = (hcur[...] - y_ref[...].astype(F32)) * scale

    h_swap = pltpu.make_async_remote_copy(
        src_ref=rh.at[pl.ds(core * chips, chips)], dst_ref=rh.at[pl.ds(core * chips, chips)],
        send_sem=px_send.at[0], recv_sem=px_recv.at[0], device_id=(partner,), device_id_type=MESH)
    e_swap = pltpu.make_async_remote_copy(
        src_ref=re.at[pl.ds(core * chips, chips)], dst_ref=re.at[pl.ds(core * chips, chips)],
        send_sem=px_send.at[1], recv_sem=px_recv.at[1], device_id=(partner,), device_id_type=MESH)

    def error_step(l, z, w1, w2):
        q = mm(eb[l], w2, NT)
        slope = gelu_grad(z)[1]
        hcur[...] += mm((slope * q).astype(BF16), w1, NT)

    def backward_cached(i, carry):
        l = layers - 1 - i
        eb[l] = hcur[...].astype(BF16)
        for j in range(2):
            kept = 2 * (l - (layers - CACHED)) + j
            error_step(l, z_kept[kept], cw1[kept], cw2[kept])
        send_e(l)
        return carry

    def backward(i, carry):
        l, step = top - i, n_fwd + i

        @pl.when(step + 2 < n_steps)
        def _():
            ahead(step)

        @pl.when(step + 4 < n_steps)
        def _():
            w2_copy(l - 4, step % 2).start()

        @pl.when(step + 4 == n_steps)
        def _():
            w2_copy(chip, step % 2).start()

        eb[l] = hcur[...].astype(BF16)
        for m in range(2):
            j, slot = chunk(m), (2 * step + m) % SLOTS
            w1_copy(0, 0, slot).wait()
            if m == 1:
                pass_copy(step).wait_recv()
            w1 = wb1[slot].astype(BF16)
            error_step(l, mm(hb[l], w1), w1, (own2 if m == 0 else far2)[step % RING])

            @pl.when(step + 2 < n_steps)
            def _(m=m, j=j, slot=slot):
                if m == 0:
                    pass_copy(step + 2).start()
                w1_copy(l - 2, j, slot).start()

            if m == 0:
                @pl.when(step + 2 == n_steps)
                def _(j=j, slot=slot):
                    w1_copy(chip, j, slot).start()
        release(step)
        send_e(l)
        return carry

    def h_in(c, carry):
        @pl.when(c != chip)
        def _():
            h_arrival(c).wait_recv()

        return carry

    def e_in(c, carry):
        @pl.when(c != chip)
        def _():
            e_arrival(c).wait_recv()

        return carry

    lax.fori_loop(0, CACHED, backward_cached, 0)
    lax.fori_loop(0, n_bwd, backward, 0)
    eb[0] = hcur[...].astype(BF16)
    send_e(0)
    lax.fori_loop(0, chips, h_in, 0)
    h_swap.start()
    lax.fori_loop(0, chips, e_in, 0)
    e_swap.start()
    w1_copy(0, 0, (2 * n_steps) % SLOTS).wait()
    w2_copy(0, n_steps % 2).wait()
    ow1[...] = wb1[(2 * n_steps) % SLOTS].astype(BF16)
    ow2[...] = wb2[n_steps % 2].astype(BF16)

    def place(n, rx, ry, sz, twin):
        sx = 1 - cx if rx else cx
        sy = 1 - cy if ry else cy
        inner, far = (sx, ry) if n % 2 == 0 else (sy, rx)
        at = 4 * chips_z + 4 * sz + 2 * (n % 2) + twin if far else 4 * sz + 2 * (n % 2) + twin
        return outs[at].at[inner, n // 2]

    def source(rx, ry, sz):
        sx = 1 - cx if rx else cx
        sy = 1 - cy if ry else cy
        return sz * 4 + sy * 2 + sx

    hops = (chip + 1 - 2 * cx, chip + 2 - 4 * cy, chip + 4, chip - 4)

    def hop_copy(kind, n, rx, ry, sz, mine, part=None):
        src = source(rx, ry, sz)
        there = (n, 1 - rx if kind == 0 else rx, 1 - ry if kind == 1 else ry, sz, 0)
        tx, ty = there[1], there[2]
        inner = (1 - cx if rx else cx) if n % 2 == 0 else (1 - cy if ry else cy)
        far = ty if n % 2 == 0 else tx
        at = 4 * chips_z + 4 * sz + 2 * (n % 2) if far else 4 * sz + 2 * (n % 2)
        src_ref, dst_ref = own.at[n] if mine else place(n, rx, ry, sz, 0), outs[at].at[inner, n // 2]
        if part is not None:
            src_ref, dst_ref = src_ref.at[part], dst_ref.at[part]
        return pltpu.make_async_remote_copy(
            src_ref=src_ref, dst_ref=dst_ref, send_sem=sp_send.at[n, kind, src], recv_sem=sp_recv.at[n, src],
            device_id=(2 * hops[kind] + core,), device_id_type=MESH)

    def arrival(n, rx, ry, sz):
        return pltpu.make_async_remote_copy(
            src_ref=own.at[n], dst_ref=place(n, rx, ry, sz, 0), send_sem=sp_send.at[n, 0, source(rx, ry, sz)],
            recv_sem=sp_recv.at[n, source(rx, ry, sz)], device_id=(me,), device_id_type=MESH)

    def twin_copy(n, rx, ry, sz, mine):
        src = source(rx, ry, sz)
        return pltpu.make_async_remote_copy(
            src_ref=own.at[n] if mine else place(n, rx, ry, sz, 0), dst_ref=place(n, rx, ry, sz, 1),
            send_sem=tw_send.at[n, src], recv_sem=tw_recv.at[n, src], device_id=(partner,), device_id_type=MESH)

    def at_z(fn):
        for z in range(chips_z):
            pl.when(cz == z)(functools.partial(fn, z))

    def split(code):
        return code // 10000, (code // 1000 % 10, code // 100 % 10, code // 10 % 10, code % 10)

    def act(z, code):
        kind, block = split(code)
        mine = block[1:] == (0, 0, z)
        if kind:
            hop_copy(kind - 1, *block, mine).start()
        else:
            arrival(*block).wait_recv()
            twin_copy(*block, False).start()

    group = 4
    half_groups = chips // group

    def row_groups(body, wait=False):
        def step(gi, carry):
            if wait:
                @pl.when(gi == half_groups)
                def _():
                    h_swap.wait_recv()
                    e_swap.wait_recv()

            half = (core + gi // half_groups) % 2
            base = half * chips + (gi % half_groups) * group
            body(base, rh[pl.ds(base, group)].reshape(group * rows, d), re[pl.ds(base, group)].reshape(group * rows, d))
            return carry

        lax.fori_loop(0, 2 * half_groups, step, 0)

    def add_in(base, s):
        for b in range(group):
            acc1[...] += mm(rh[base + b], s[b * rows:(b + 1) * rows], TN).astype(BF16).astype(F32)

    def add_out(base, a):
        for b in range(group):
            acc2[...] += mm(a[b * rows:(b + 1) * rows], re[base + b], TN).astype(BF16).astype(F32)

    def store_in(n):
        for cb in range(piece // 128):
            own[n, 0, cb * d:(cb + 1) * d, :] = acc1[:, cb * 128:(cb + 1) * 128].astype(BF16)

    def store_out(n):
        for lb in range(d // 128):
            own[n, 1, lb * piece:(lb + 1) * piece, :] = acc2[:, lb * 128:(lb + 1) * 128].astype(BF16)

    def send_part(part):
        def start(z):
            for code in RELAYS[z][0]:
                kind, block = split(code)
                hop_copy(kind - 1, *block, True, part).start()

        at_z(start)

    acc1[...] = jnp.zeros_like(acc1)
    acc2[...] = jnp.zeros_like(acc2)

    def first_out(base, hg, eg):
        a, slope = gelu_grad(mm(hg, ow1[:, :piece]))
        for b in range(group):
            z_kept[base // group, :, b * piece:(b + 1) * piece] = slope[b * rows:(b + 1) * rows]
        add_out(base, a.astype(BF16))

    def first_in(base, hg, eg):
        q = mm(eg, ow2[:piece, :], NT)
        slope = jnp.concatenate([z_kept[base // group, :, b * piece:(b + 1) * piece] for b in range(group)], axis=0)
        add_in(base, (slope * q).astype(BF16))

    row_groups(first_out, wait=True)
    store_out(0)
    send_part(1)
    row_groups(first_in)
    store_in(0)
    send_part(0)

    def start_rest(n):
        def start(z):
            for code in RELAYS[z][n] if n else ():
                act(z, code)
            twin_copy(n, 0, 0, z, True).start()
            pltpu.make_async_copy(own.at[n], place(n, 0, 0, z, 0), own_sem.at[n]).start()

        at_z(start)

    start_rest(0)
    for n in range(1, QUARTERS):
        cols = slice(n * piece, (n + 1) * piece)
        acc1[...] = jnp.zeros_like(acc1)
        acc2[...] = jnp.zeros_like(acc2)

        def both(base, hg, eg, cols=cols):
            a, slope = gelu_grad(mm(hg, ow1[:, cols]))
            q = mm(eg, ow2[cols, :], NT)
            a = a.astype(BF16)
            s = (slope * q).astype(BF16)
            for b in range(group):
                own_rows = slice(b * rows, (b + 1) * rows)
                acc1[...] += mm(rh[base + b], s[own_rows], TN).astype(BF16).astype(F32)
                acc2[...] += mm(a[own_rows], re[base + b], TN).astype(BF16).astype(F32)

        row_groups(both)
        store_in(n)
        store_out(n)
        start_rest(n)

    def relay(z):
        for code in RELAYS[z][QUARTERS]:
            act(z, code)

    at_z(relay)

    def sent(l, carry):
        @pl.when(l != chip)
        def _():
            h_copy(l).wait_send()
            e_copy(l).wait_send()

        return carry

    lax.fori_loop(0, layers, sent, 0)
    h_swap.wait_send()
    e_swap.wait_send()
    for step in range(n_steps - RING, n_steps):
        pass_copy(step).wait_send()

    def drain(z):
        for n in range(QUARTERS):
            twin_copy(n, 0, 0, z, True).wait()
            pltpu.make_async_copy(own.at[n], place(n, 0, 0, z, 0), own_sem.at[n]).wait()
        for code in sum(RELAYS[z], ()):
            kind, block = split(code)
            if kind:
                hop_copy(kind - 1, *block, block[1:] == (0, 0, z)).wait_send()
            else:
                twin_copy(*block, False).wait()

    at_z(drain)


def local_grads(w_in, w_out, x, y, n_dev):
    layers, d, hid = w_in.shape
    rows = x.shape[0]
    hc = hid // 2
    piece = hc // QUARTERS
    part_rows = piece * d // 128
    dims = (n_dev, layers, rows, d, hid)
    n_out = n_dev // 2 + 4 * FIRST
    flops = 2 * rows * d * hid * layers * 4 + 2 * rows * n_dev * d * hc * 4
    return pl.pallas_call(
        functools.partial(grads_kernel, dims),
        out_shape=[jax.ShapeDtypeStruct((2, QUARTERS // 2, 2, part_rows, 128), BF16)] * n_out,
        in_specs=[pl.BlockSpec(memory_space=pl.ANY)] * 4,
        out_specs=[pl.BlockSpec(memory_space=pl.ANY)] * n_out,
        scratch_shapes=[
            pltpu.VMEM((rows, d), BF16),
            pltpu.VMEM((rows, d), BF16),
            pltpu.SemaphoreType.DMA((2,)),
            pltpu.VMEM((SLOTS, d, hc), F32),
            pltpu.VMEM((2, hc, d), F32),
            pltpu.VMEM((RING, hc, d), BF16),
            pltpu.VMEM((RING, hc, d), BF16),
            pltpu.VMEM((2 * CACHED, d, hc), BF16),
            pltpu.VMEM((2 * CACHED, hc, d), BF16),
            pltpu.VMEM((2 * CACHED, rows, hc), F32),
            pltpu.VMEM((layers, rows, d), BF16),
            pltpu.VMEM((layers, rows, d), BF16),
            pltpu.VMEM((rows, d), F32),
            pltpu.VMEM((n_dev, rows, d), BF16),
            pltpu.VMEM((n_dev, rows, d), BF16),
            pltpu.VMEM((d, hc), BF16),
            pltpu.VMEM((hc, d), BF16),
            pltpu.VMEM((d, piece), F32),
            pltpu.VMEM((piece, d), F32),
            pltpu.VMEM((QUARTERS, 2, part_rows, 128), BF16),
            pltpu.SemaphoreType.DMA((SLOTS,)),
            pltpu.SemaphoreType.DMA((2,)),
            pltpu.SemaphoreType.DMA((RING,)),
            pltpu.SemaphoreType.DMA((RING,)),
            pltpu.SemaphoreType.REGULAR((RING,)),
            pltpu.SemaphoreType.DMA((layers,)),
            pltpu.SemaphoreType.DMA((layers,)),
            pltpu.SemaphoreType.DMA((layers,)),
            pltpu.SemaphoreType.DMA((layers,)),
            pltpu.SemaphoreType.DMA((2,)),
            pltpu.SemaphoreType.DMA((2,)),
            pltpu.SemaphoreType.DMA((QUARTERS, 4, n_dev // 2)),
            pltpu.SemaphoreType.DMA((QUARTERS, n_dev // 2)),
            pltpu.SemaphoreType.DMA((QUARTERS, n_dev // 2)),
            pltpu.SemaphoreType.DMA((QUARTERS, n_dev // 2)),
            pltpu.SemaphoreType.DMA((QUARTERS,)),
        ],
        compiler_params=pltpu.CompilerParams(collective_id=0, has_side_effects=True, vmem_limit_bytes=VMEM_LIMIT),
        cost_estimate=pl.CostEstimate(flops=flops, bytes_accessed=4 * w_in.size * 4, transcendentals=0),
        name="local_grads",
    )(w_in, w_out, x, y)


def update_kernel(dims, group, last, *refs):
    layers, _, d, piece = dims
    step_size = LR_SCALE / layers
    chunk = 2 * piece
    steps = 16
    w1, m1, w2, m2, h_in = refs[:5]
    sums = refs[5:13]
    refs = refs[13:]
    if group:
        refs = refs[4:]
    if last:
        y_ref, refs = refs[0], refs[1:]
    w1o, w2o, m1o, m2o, h_out = refs[:5]
    if last:
        loss_ref = refs[5]
    bw1, bm1, bw2, bm2, gbuf, in_sem, out_sem, gsem, nb1, nb2, hb_ref = refs[-11:]
    slots = bw1.shape[0]

    me = lax.axis_index("data")
    chip, core = me // 2, me % 2
    cx, cy = chip % 2, (chip // 2) % 2

    def tile1(ref, t):
        return ref.at[4 * group + t // 4, :, pl.ds(pl.multiple_of((t % 4) * chunk, 128), chunk)]

    def tile2(ref, t):
        return ref.at[4 * group + t // 4, pl.ds(pl.multiple_of((t % 4) * chunk, 8), chunk), :]

    def reads(t, slot):
        return [pltpu.make_async_copy(src, buf.at[slot], in_sem.at[i, slot]) for i, (src, buf) in enumerate(
            ((tile1(w1, t), bw1), (tile1(m1, t), bm1), (tile2(w2, t), bw2), (tile2(m2, t), bm2)))]

    def writes(t, slot):
        return [pltpu.make_async_copy(buf.at[slot], dst, out_sem.at[i, slot]) for i, (dst, buf) in enumerate(
            ((tile1(w1o, t), bw1), (tile1(m1o, t), bm1), (tile2(w2o, t), bw2), (tile2(m2o, t), bm2)))]

    def fetch(t, slot):
        for copy in reads(t, slot):
            copy.start()
        layer, part = t // 4, t % 4
        sx, sy, half, q = layer % 2, layer // 2, part // 2, part % 2
        for par, inner, far in ((0, sx, sy != cy), (1, sy, sx != cx)):
            for is_far in (0, 1):
                for twin in (0, 1):
                    hit = jnp.logical_and(far == bool(is_far), (half != core) == bool(twin))

                    @pl.when(hit)
                    def _(par=par, inner=inner, is_far=is_far, twin=twin):
                        pltpu.make_async_copy(sums[4 * is_far + 2 * par + twin].at[inner, q], gbuf.at[slot, par], gsem.at[par, slot]).start()

    for t in range(AHEAD):
        fetch(t, t)
    h_out[...] = h_in[...].astype(F32)

    def body(t, carry):
        slot = t % slots

        @pl.when(t % 4 == 0)
        def _():
            hb_ref[...] = h_out[...].astype(BF16)

        for copy in reads(t, slot):
            copy.wait()
        for par in range(2):
            pltpu.make_async_copy(sums[0].at[0, 0], gbuf.at[slot, par], gsem.at[par, slot]).wait()
            for cb in range(piece // 128):
                cols = slice(par * piece + cb * 128, par * piece + (cb + 1) * 128)
                mn = MOMENTUM * bm1[slot, :, cols] + gbuf[slot, par, 0, cb * d:(cb + 1) * d, :].astype(F32)
                wn = bw1[slot, :, cols] - step_size * mn
                bm1[slot, :, cols] = mn
                bw1[slot, :, cols] = wn
                nb1[:, cols] = wn.astype(BF16)
            hid_rows = slice(par * piece, (par + 1) * piece)
            for lb in range(d // 128):
                cols = slice(lb * 128, (lb + 1) * 128)
                mn = MOMENTUM * bm2[slot, hid_rows, cols] + gbuf[slot, par, 1, lb * piece:(lb + 1) * piece, :].astype(F32)
                wn = bw2[slot, hid_rows, cols] - step_size * mn
                bm2[slot, hid_rows, cols] = mn
                bw2[slot, hid_rows, cols] = wn
                nb2[hid_rows, cols] = wn.astype(BF16)
        for copy in writes(t, slot):
            copy.start()

        @pl.when(t + AHEAD < steps)
        def _():
            nslot = (t + AHEAD) % slots

            @pl.when(t + AHEAD >= slots)
            def _():
                for copy in writes(t + AHEAD - slots, nslot):
                    copy.wait()

            fetch(t + AHEAD, nslot)

        z = mm(hb_ref[...], nb1[...])
        h_out[...] += mm(gelu(z).astype(BF16), nb2[...])
        return carry

    lax.fori_loop(0, steps, body, 0)
    for t in range(steps - slots, steps):
        for copy in writes(t, t % slots):
            copy.wait()
    if last:
        diff = h_out[...] - y_ref[...].astype(F32)
        loss_ref[...] = jnp.sum(diff * diff, axis=-1) / (2 * d)


def update(group, w_in, m_in, w_out, m_out, h, sums, prev, y):
    layers, d, hid = w_in.shape
    rows = h.shape[0]
    piece = hid // 2 // QUARTERS
    chunk = 2 * piece
    last = group == layers // 4 - 1
    whole = pl.BlockSpec(memory_space=pltpu.VMEM)
    any_spec = pl.BlockSpec(memory_space=pl.ANY)
    args = [w_in, m_in, w_out, m_out, h, *sums, *prev] + ([y] if last else [])
    in_specs = [any_spec] * 4 + [whole] + [any_spec] * (8 + len(prev)) + ([whole] if last else [])
    out_specs = [any_spec] * 4 + [whole]
    out_shape = [jax.ShapeDtypeStruct(a.shape, F32) for a in (w_in, w_out, m_in, m_out, h)]
    if last:
        out_specs.append(whole)
        out_shape.append(jax.ShapeDtypeStruct((rows,), F32))
    n_el = 2 * w_in.size // 4
    slots = 7
    return pl.pallas_call(
        functools.partial(update_kernel, (layers, rows, d, piece), group, last),
        in_specs=in_specs,
        out_specs=out_specs,
        out_shape=out_shape,
        scratch_shapes=[
            pltpu.VMEM((slots, d, chunk), F32),
            pltpu.VMEM((slots, d, chunk), F32),
            pltpu.VMEM((slots, chunk, d), F32),
            pltpu.VMEM((slots, chunk, d), F32),
            pltpu.VMEM((slots, 2, *sums[0].shape[2:]), BF16),
            pltpu.SemaphoreType.DMA((4, slots)),
            pltpu.SemaphoreType.DMA((4, slots)),
            pltpu.SemaphoreType.DMA((2, slots)),
            pltpu.VMEM((d, chunk), BF16),
            pltpu.VMEM((chunk, d), BF16),
            pltpu.VMEM((rows, d), BF16),
        ],
        input_output_aliases={13 + i: i for i in range(len(prev))},
        compiler_params=pltpu.CompilerParams(vmem_limit_bytes=VMEM_LIMIT),
        cost_estimate=pl.CostEstimate(flops=5 * 10**10, bytes_accessed=18 * n_el, transcendentals=0),
    )(*args)


def solution(mesh):
    n_dev = mesh.shape["data"]
    rows_spec = P("data", None)
    swap = {axis: [(i, i ^ bit) for i in range(n_dev)] for axis, bit in (("core", 1), ("x", 2), ("y", 4))}

    def send(array, axis):
        return lax.ppermute(array, "data", swap[axis])

    def local_steps(w_in, w_out, mom_in, mom_out, x_first, y_first, x_second, y_second):
        groups = w_in.shape[0] // 4
        sums = local_grads(w_in, w_out, x_first, y_first, n_dev)
        near = [list(sums[4 * g:4 * g + 4]) for g in range(groups)]
        far = [list(sums[4 * (groups + g):4 * (groups + g) + 4]) for g in range(FIRST)]
        for g in range(FIRST, groups):
            from_y = send(near[g][0], "y")
            from_x = send(near[g][2], "x")
            far.append([from_y, send(from_y, "core"), from_x, send(from_x, "core")])
        prev, h = [], x_second
        for g in range(groups):
            outs = update(g, w_in, mom_in, w_out, mom_out, h, near[g] + far[g], prev, y_second)
            prev, h = list(outs[:4]), outs[4]
        w_in_new, w_out_new, mom_in_new, mom_out_new = prev
        return w_in_new, w_out_new, mom_in_new, mom_out_new, outs[5], h

    return jax.shard_map(
        local_steps, mesh=mesh,
        in_specs=(P(), P(), P(), P(), rows_spec, rows_spec, rows_spec, rows_spec),
        out_specs=(P(), P(), P(), P(), P("data"), rows_spec), check_vma=False)
```
